32 devices in a mesh: groups: 2 (over y), expert: 8 (over z, x), tensor: 2 (over core).
Axes of the slice: x: 2, y: 2, z: 4, core: 2. Of those that a mesh axis runs over, the one named last changes fastest.
Arguments:
- tokens: bfloat16 [1024, 1536], P(('groups', 'expert')), parts along dimension 0, may hold values from -12 to 12
- gain: float32 [1536], replicated, may hold values from 0.25 to 1.75
- route_ids: int32 [1024, 4], P(('groups', 'expert')), parts along dimension 0, may hold values from 0 to 3, as said below
- route_weights: float32 [1024, 4], P(('groups', 'expert')), parts along dimension 0, may hold values from 0.05 to 0.5
- w_gate: bfloat16 [8, 1536, 768], P('expert', None, 'tensor'), may hold values from -0.15625 to 0.15625
- w_up: bfloat16 [8, 1536, 768], P('expert', None, 'tensor'), may hold values from -0.15625 to 0.15625
- w_down: bfloat16 [8, 768, 1536], P('expert', 'tensor'), may hold values from -0.15625 to 0.15625
Outputs:
- mixed: bfloat16 [1024, 1536], P(('groups', 'expert')), parts along dimension 0
The draws below stay inside these ranges and needn't reach their ends.
There are 2 independent parts, one for each index of `groups`. The reference program is written for one: setup_inputs(seed, part) draws one part's arguments, and reference() takes and returns one part's arrays. A program takes and returns all parts, laid end to end along the dimension named above; an argument that names none is the same for every part. Nothing has to cross between parts.
Inputs may be any that keep to these rules, and one draw needn't show every extreme that they name: `route_ids`: each row names 4 different experts. In each aligned block of 32 rows no expert is named more than 32 times; one expert, the same in every block, is named exactly 32 times in every block, and the other experts' counts within a block differ by at most one.
All inputs are finite; a program needn't handle non-finite values.
Results may differ from the reference program's by a relative error of at most 0.0045.
Values may be sent and summed in bfloat16 or wider, within the bound.
A program may use at most 64 MiB of HBM per device.

```python
import math
import jax
import jax.numpy as jnp
from jax import lax

D = 1536
FF = 1536
TOP = 4
EXPERTS = 4
TOK_DEV = 32
CAP = 32
TOKENS = 512


def draw_tokens(key, part):
    key_base = jax.random.fold_in(key, 0)
    values = jax.random.normal(key_base, (TOKENS, D), jnp.float32)
    return jnp.clip(values, -12.0, 12.0).astype(jnp.bfloat16)


def draw_route_ids(key, part):
    blocks = TOKENS // TOK_DEV
    slot_total = TOK_DEV * TOP
    others = EXPERTS - 1
    key_hot, key_rank, key_rows, key_cols = jax.random.split(key, 4)
    hot_expert = jax.random.randint(key_hot, (), 0, EXPERTS, dtype=jnp.int32)
    spare = slot_total - CAP
    floor_count = spare // others
    surplus = spare - floor_count * others
    rank_keys = jax.random.split(key_rank, blocks)
    ranking = jax.vmap(lambda sub_key: jax.random.permutation(sub_key, others))(rank_keys)
    counts = floor_count + (ranking < surplus).astype(jnp.int32)
    run_ends = CAP + jnp.cumsum(counts, axis=1, dtype=jnp.int32)
    places = jnp.arange(slot_total, dtype=jnp.int32)
    owner_index = jnp.sum((places[None, :, None] >= run_ends[:, None, :]).astype(jnp.int32), axis=2, dtype=jnp.int32)
    other_ids = (hot_expert + 1 + owner_index) % EXPERTS
    listed = jnp.where(places[None, :] < CAP, hot_expert, other_ids)
    id_grid = listed.reshape(blocks, TOP, TOK_DEV).transpose(0, 2, 1)
    row_keys = jax.random.split(key_rows, blocks)
    row_order = jax.vmap(lambda sub_key: jax.random.permutation(sub_key, TOK_DEV))(row_keys)
    id_grid = jnp.take_along_axis(id_grid, row_order[:, :, None], axis=1)
    scores = jax.random.randint(key_cols, (blocks, TOK_DEV, TOP), 0, 1 << 20, dtype=jnp.int32) * TOP + jnp.arange(TOP, dtype=jnp.int32)
    col_order = jnp.argsort(scores, axis=2)
    id_grid = jnp.take_along_axis(id_grid, col_order, axis=2)
    return id_grid.reshape(TOKENS, TOP).astype(jnp.int32)


def steps_of(own_key, dims, pieces, least, top_value):
    factor_of = 1.0
    for axis_at, parts in pieces:
        draws = jax.random.uniform(jax.random.fold_in(jax.random.fold_in(own_key, 6), axis_at), (parts,), jnp.float32, least / len(pieces), top_value / len(pieces))
        factor_of = factor_of * jnp.repeat(jnp.exp(draws), dims[axis_at] // parts).reshape((-1,) + (1,) * (len(dims) - 1 - axis_at))
    return factor_of


def normal_values(key, extent, deviation, limit, shards=(), held_as=jnp.bfloat16):
    level = steps_of(key, extent, shards, -0.22, 0.18) if shards else 1.0
    entries = jax.random.normal(key, extent, jnp.float32) * deviation * level
    return jnp.minimum(jnp.maximum(entries, -limit), limit).astype(held_as)


def setup_inputs(seed: int = 0, part: int = 0) -> dict:
    arg_keys = jax.random.split(jax.random.key(seed), 8)
    part_splits = jax.random.split(jax.random.fold_in(arg_keys[7], part), 8)
    tokens = draw_tokens(jax.random.fold_in(jax.random.fold_in(arg_keys[7], part), 71), part)
    gain = jnp.clip(1.0 + 0.15 * jax.random.normal(arg_keys[1], (D,), jnp.float32), 0.25, 1.75)
    route_ids = draw_route_ids(jax.random.fold_in(jax.random.fold_in(arg_keys[7], part), 71), part)
    route_weights = jnp.clip(jnp.exp(math.log(0.5) - 2.3025851 * jax.random.uniform(part_splits[3], (TOKENS, TOP), jnp.float32) ** steps_of(part_splits[3], (TOKENS, TOP), ((0, 8),), -0.2, 0.2)), 0.05, 0.5)
    w_gate = normal_values(arg_keys[4], (2 * EXPERTS, D, FF // 2), D ** -0.5, 0.15625, ((0, 8), (2, 2)))
    w_up = normal_values(arg_keys[5], (2 * EXPERTS, D, FF // 2), D ** -0.5, 0.15625, ((0, 8), (2, 2)))
    w_down = normal_values(arg_keys[6], (2 * EXPERTS, FF // 2, D), FF ** -0.5, 0.15625, ((0, 8), (1, 2)))
    return {"tokens": tokens, "gain": gain, "route_ids": route_ids, "route_weights": route_weights, "w_gate": w_gate, "w_up": w_up, "w_down": w_down}


def gated_unit(gate_val, up_val):
    return gate_val * jax.nn.sigmoid(1.702 * gate_val) * (up_val + 1.0)

def reference(tokens, gain, route_ids, route_weights, w_gate, w_up, w_down):
    resident = tokens.astype(jnp.float32)
    inv_rms = lax.rsqrt(lax.optimization_barrier(jnp.mean(resident * resident, axis=1, keepdims=True)) + 1e-05)
    normed = (resident * inv_rms * gain).astype(jnp.bfloat16)
    flat_ids = route_ids.reshape(-1)
    flat_weight = route_weights.reshape(-1)
    slot_total = flat_ids.shape[0]
    most_rows = TOKENS // TOK_DEV * CAP
    slot_range = jnp.arange(slot_total, dtype=jnp.int32)
    row_range = jnp.arange(most_rows, dtype=jnp.int32)

    def one_expert(summed, expert):
        chosen = flat_ids == expert
        rank_in = jnp.cumsum(chosen.astype(jnp.int32), dtype=jnp.int32) - 1
        target = jnp.where(chosen, rank_in, most_rows).astype(jnp.int32)
        picked = jnp.zeros((most_rows,), jnp.int32).at[target].set(slot_range, mode='drop')
        is_live = row_range < jnp.sum(chosen.astype(jnp.int32), dtype=jnp.int32)
        token_row = picked // TOP
        inputs = normed[token_row]
        first = (2 * expert).astype(jnp.int32)
        pair_gate = lax.dynamic_slice_in_dim(w_gate, first, 2, 0)
        pair_up = lax.dynamic_slice_in_dim(w_up, first, 2, 0)
        pair_down = lax.dynamic_slice_in_dim(w_down, first, 2, 0)
        full_gate = jnp.concatenate([pair_gate[0], pair_gate[1]], axis=1)
        full_up = jnp.concatenate([pair_up[0], pair_up[1]], axis=1)
        full_down = pair_down.reshape(-1, pair_down.shape[2])
        gate_val = jnp.dot(inputs, full_gate, preferred_element_type=jnp.float32)
        up_val = jnp.dot(inputs, full_up, preferred_element_type=jnp.float32)
        hidden = gated_unit(gate_val, up_val).astype(jnp.bfloat16)
        expert_out = jnp.dot(hidden, full_down, preferred_element_type=jnp.float32)
        weight = jnp.where(is_live, flat_weight[picked], 0.0)
        summed = summed.at[token_row].add(weight[:, None] * expert_out)
        return (summed, None)
    empty_sum = jnp.zeros(resident.shape, jnp.float32)
    summed, unused = lax.scan(one_expert, empty_sum, jnp.arange(EXPERTS, dtype=jnp.int32))
    return (resident + summed).astype(jnp.bfloat16)
```

```python
import jax
import jax.numpy as jnp
from jax import lax
from jax.experimental import pallas as pl
from jax.experimental.pallas import tpu as pltpu
from jax.sharding import PartitionSpec as P

MESH = pl.DeviceIdType.MESH


def gated_unit(gate_val, up_val):
    return gate_val * jax.nn.sigmoid(1.702 * gate_val) * (up_val + 1.0)


def dense_kernel(
    tokens_ref,
    gain_ref,
    ids_ref,
    weights_ref,
    gate_ref,
    up_ref,
    down_ref,
    out_ref,
    held,
    gain,
    ids,
    weights,
    wg,
    wu,
    wd,
    own,
    slots,
    keep,
    first_out,
    first_in,
    second_out,
    second_in,
    near_out,
    near_in,
    final,
    line_out,
    line_in,
    small_sem,
    load_sem,
    swap_send,
    swap_recv,
    line_send,
    line_recv,
    spread_send,
    spread_recv,
    back_send,
    back_recv,
    near_send,
    near_recv,
    give_send,
    give_recv,
    keep_sem,
):
    me = lax.axis_index("expert")
    core = lax.axis_index("tensor")
    place = me // 2
    side = lax.rem(me, 2)
    half = place // 2
    inner = lax.rem(place + half, 2)
    is_inner = inner == 1

    def at(where, which):
        return {"expert": where * 2 + which}

    pair = place + 1 - 2 * lax.rem(place, 2)
    far_inner = 2 - half
    far_outer = 3 - 3 * half
    across = at(place, 1 - side)
    beside = at(pair, side)
    corner = at(pair, 1 - side)
    sibling = {"tensor": 1 - core}
    far_spots = (far_inner, far_outer)
    far = [at(spot, side) for spot in far_spots]
    my_far_slot = 1 - inner

    rows, features = own.shape
    cols = gate_ref.shape[2]
    batches = spread_send.shape[1]
    batch = rows // batches
    pieces, _, width = keep.shape
    scope = jax.named_scope

    barrier = pltpu.get_barrier_semaphore()

    def greet(peers):
        for peer in peers:
            pl.semaphore_signal(barrier, inc=1, device_id=peer, device_id_type=MESH)

    near_peers = [across, beside, corner, sibling]
    far_peers = [across, beside, *far, sibling]

    @pl.when(core == 0)
    def _():
        greet(near_peers)

    @pl.when(core == 1)
    def _():
        greet(far_peers)

    smalls = [
        pltpu.make_async_copy(src, dst, small_sem.at[i])
        for i, (src, dst) in enumerate(
            (
                (tokens_ref, held),
                (gain_ref, gain),
                (ids_ref, ids),
                (weights_ref, weights),
            )
        )
    ]
    for small in smalls:
        small.start()

    pairs = (
        (gate_ref.at[0], lambda part: wg.at[:, pl.ds(part * cols, cols)]),
        (up_ref.at[0], lambda part: wu.at[:, pl.ds(part * cols, cols)]),
        (down_ref.at[0], lambda part: wd.at[pl.ds(part * cols, cols), :]),
    )
    loads = [
        pltpu.make_async_copy(src, dst(0), load_sem.at[i]) for i, (src, dst) in enumerate(pairs)
    ]
    for load in loads:
        load.start()

    def remote(src, dst, send, recv, peer):
        return pltpu.make_async_remote_copy(
            src_ref=src, dst_ref=dst, send_sem=send, recv_sem=recv, device_id=peer,
            device_id_type=MESH,
        )

    swaps = [
        remote(src, dst(1), swap_send.at[i], swap_recv.at[i], sibling)
        for i, (src, dst) in enumerate(pairs)
    ]

    def rows_of(q):
        return pl.ds(q * batch, batch)

    def part(p):
        return pl.ds(p * width, width)

    with scope("w_small"):
        smalls[0].wait()
        smalls[1].wait()

    def normed(q):
        resident = held[rows_of(q), :].astype(jnp.float32)
        inv_rms = lax.rsqrt(jnp.mean(resident * resident, axis=1, keepdims=True) + 1e-05)
        return (resident * inv_rms * gain[...].reshape(1, -1)).astype(jnp.bfloat16)

    smalls[2].wait()
    smalls[3].wait()
    lanes = line_out.shape[1]
    spots = line_out.shape[0]
    spot_ids = lax.broadcasted_iota(jnp.int32, (rows, rows), 0)
    lane_ids = lax.broadcasted_iota(jnp.int32, (rows, rows), 1)

    def line_of(spot):
        named = jnp.where(ids[...] == spot, weights[...], 0.0)
        return jnp.sum(named, axis=0, keepdims=True)

    def column(line):
        return jnp.sum(jnp.where(spot_ids == lane_ids, line, 0.0), axis=1, keepdims=True)

    def ready(i):
        loads[i].wait()
        swaps[i].wait_recv()

    def hidden_of(first, fresh):
        block = slots[pl.ds(first, 2)].reshape(2 * rows, features)
        if fresh:
            with scope("w_wg"):
                ready(0)
        gate_val = jnp.dot(block, wg[...], preferred_element_type=jnp.float32)
        if fresh:
            with scope("w_wu"):
                ready(1)
        up_val = jnp.dot(block, wu[...], preferred_element_type=jnp.float32)
        value = gated_unit(gate_val, up_val).astype(jnp.bfloat16)
        if fresh:
            with scope("w_wd"):
                ready(2)
        return value

    def down(hidden, p):
        return jnp.dot(hidden, wd[:, part(p)], preferred_element_type=jnp.float32)

    def give(p):
        there = out_ref.at[:, part(p)]
        return remote(final.at[:, part(p)], there, give_send.at[p], give_recv.at[p], sibling)

    def stay(p):
        return pltpu.make_async_copy(final.at[:, part(p)], out_ref.at[:, part(p)], keep_sem.at[p])

    def hand(p):
        return remote(near_out.at[p], near_in.at[p], near_send.at[p], near_recv.at[p], sibling)

    def spread(lane, slot, q, src, peer):
        return remote(
            src.at[rows_of(q), :], slots.at[slot, rows_of(q), :], spread_send.at[lane, q],
            spread_recv.at[slot, q], peer,
        )

    lower, upper = pl.ds(0, rows), pl.ds(rows, rows)

    @pl.when(core == 0)
    def _():
        def to_across(q):
            return spread(0, 1, q, slots.at[0], across)

        def to_beside(q):
            return spread(1, 2, q, slots.at[0], beside)

        def on_to_beside(q):
            return spread(2, 3, q, slots.at[1], beside)

        def line_to(i):
            return remote(
                line_out, line_in.at[i], line_send.at[i], line_recv.at[i],
                (across, beside, corner)[i],
            )

        def back_z(p):
            return remote(
                first_out.at[p], first_in.at[p], back_send.at[0, p], back_recv.at[0, p], beside
            )

        def back_x(p):
            return remote(
                second_out.at[p, lower, :], second_in.at[p, lower, :], back_send.at[1, p],
                back_recv.at[1, p], across,
            )

        for q in range(batches):
            slots[0, rows_of(q), :] = normed(q)
        for spot in range(spots):
            line_out[spot : spot + 1, :] = line_of(spot)
        with scope("w_bar"):
            pl.semaphore_wait(barrier, len(near_peers))
        for q in range(batches):
            to_across(q).start()
            to_beside(q).start()
        for i in range(3):
            line_to(i).start()
        for swap in swaps:
            swap.start()
        for q in range(batches):
            with scope(f"w_A{q}"):
                to_across(q).wait_recv()
            on_to_beside(q).start()
        for i in range(3):
            line_to(i).wait_recv()

        def share(table):
            own_line = jnp.sum(
                jnp.where(
                    lax.broadcasted_iota(jnp.int32, (spots, lanes), 0) == place, table, 0.0
                ),
                axis=0,
                keepdims=True,
            )
            return column(own_line)

        own_share = share(line_out[...])
        shares = [share(line_in[i]) for i in range(3)]
        hidden = hidden_of(0, True)
        scales = jnp.concatenate([own_share, shares[0]], axis=0)
        for p in range(pieces):
            keep[p] = down(hidden, p) * scales
        for q in range(batches):
            with scope(f"w_P{q}"):
                to_beside(q).wait_recv()
        for q in range(batches):
            with scope(f"w_D{q}"):
                on_to_beside(q).wait_recv()
        hidden = hidden_of(2, False)
        scales = jnp.concatenate([shares[1], shares[2]], axis=0)
        for p in range(pieces):
            first_out[p] = (down(hidden, p) * scales).astype(jnp.bfloat16)
            back_z(p).start()
        for p in range(pieces):
            with scope(f"w_bz{p}"):
                back_z(p).wait_recv()
            both = keep[p] + first_in[p].astype(jnp.float32)
            second_out[p, lower, :] = both[rows:].astype(jnp.bfloat16)
            back_x(p).start()
            keep[p, lower, :] = both[:rows] + held[:, part(p)].astype(jnp.float32)
        for p in range(pieces):
            with scope(f"w_bx{p}"):
                back_x(p).wait_recv()
            near_out[p] = keep[p, lower, :] + second_in[p, lower, :].astype(jnp.float32)
            hand(p).start()
        for q in range(batches):
            to_across(q).wait_send()
            to_beside(q).wait_send()
            on_to_beside(q).wait_send()
        for i in range(3):
            line_to(i).wait_send()
        for p in range(pieces):
            back_z(p).wait_send()
            back_x(p).wait_send()
            hand(p).wait_send()
        for swap in swaps:
            swap.wait_send()
        with scope("w_give"):
            for p in range(pieces):
                give(p).wait_recv()

    @pl.when(core == 1)
    def _():
        def outward(q):
            return remote(
                own.at[rows_of(q), :], slots.at[my_far_slot, rows_of(q), :], spread_send.at[0, q],
                spread_recv.at[my_far_slot, q], far[0],
            )

        def arrived(s, q):
            return spread(1 + s, s, q, slots.at[s], beside)

        def sideways(s, q):
            return spread(3 + s, 2 + s, q, slots.at[s], across)

        def back_x(p):
            return remote(
                first_out.at[p], first_in.at[p], back_send.at[0, p], back_recv.at[0, p], across
            )

        def back_z(s, p):
            return remote(
                second_out.at[p, (lower, upper)[s], :],
                second_in.at[p, pl.ds(pl.multiple_of(my_far_slot * rows, rows), rows), :],
                back_send.at[1 + s, p],
                back_recv.at[1 + my_far_slot, p],
                far[s],
            )

        def came_z(s, p):
            return remote(
                second_out.at[p, (lower, upper)[s], :], second_in.at[p, (lower, upper)[s], :],
                back_send.at[1 + s, p], back_recv.at[1 + s, p], far[s],
            )

        for q in range(batches):
            own[rows_of(q), :] = normed(q)
        with scope("w_bar"):
            pl.semaphore_wait(barrier, len(far_peers))
        for q in range(batches):
            outward(q).start()
        for swap in swaps:
            swap.start()
        shares = [column(line_of(spot)) for spot in far_spots]
        for q in range(batches):
            for s in range(2):
                with scope(f"w_F{s}{q}"):
                    arrived(s, q).wait_recv()

                @pl.when(is_inner)
                def _():
                    arrived(s, q).start()

                sideways(s, q).start()
        hidden = hidden_of(0, True)
        for p in range(pieces):
            keep[p] = down(hidden, p)
        for q in range(batches):
            for s in range(2):
                with scope(f"w_G{s}{q}"):
                    sideways(s, q).wait_recv()
        hidden = hidden_of(2, False)
        for p in range(pieces):
            first_out[p] = down(hidden, p).astype(jnp.bfloat16)
            back_x(p).start()
        for p in range(pieces):
            with scope(f"w_bx{p}"):
                back_x(p).wait_recv()
            second_out[p] = (keep[p] + first_in[p].astype(jnp.float32)).astype(jnp.bfloat16)
            for s in range(2):
                back_z(s, p).start()
        for p in range(pieces):
            with scope(f"w_near{p}"):
                hand(p).wait_recv()
            total = near_in[p]
            for s in range(2):
                with scope(f"w_bz{s}{p}"):
                    came_z(s, p).wait_recv()
                total = total + shares[s] * second_in[p, (lower, upper)[s], :].astype(jnp.float32)
            final[:, part(p)] = total.astype(jnp.bfloat16)
            give(p).start()
            stay(p).start()
        for q in range(batches):
            outward(q).wait_send()
            for s in range(2):
                sideways(s, q).wait_send()

                @pl.when(is_inner)
                def _():
                    arrived(s, q).wait_send()

        for p in range(pieces):
            back_x(p).wait_send()
            for s in range(2):
                back_z(s, p).wait_send()
        for swap in swaps:
            swap.wait_send()
        with scope("w_end"):
            for p in range(pieces):
                give(p).wait_send()
                stay(p).wait()


def dense_layer(tokens, gain, route_ids, route_weights, w_gate, w_up, w_down):
    rows, features = tokens.shape
    units = 2 * w_gate.shape[2]
    batches = rows // 16
    pieces = 3
    width = features // pieces
    hbm = pl.BlockSpec(memory_space=pl.ANY)
    half = jnp.bfloat16
    dma = pltpu.SemaphoreType.DMA
    ids = route_ids.T
    weights = route_weights.T
    travel = pltpu.VMEM((pieces, 2 * rows, width), half)
    return pl.pallas_call(
        dense_kernel,
        out_shape=jax.ShapeDtypeStruct(tokens.shape, tokens.dtype),
        in_specs=[hbm] * 7,
        out_specs=hbm,
        scratch_shapes=[
            pltpu.VMEM((rows, features), half),
            pltpu.VMEM((features,), jnp.float32),
            pltpu.VMEM(ids.shape, jnp.int32),
            pltpu.VMEM(weights.shape, jnp.float32),
            pltpu.VMEM((features, units), half),
            pltpu.VMEM((features, units), half),
            pltpu.VMEM((units, features), half),
            pltpu.VMEM((rows, features), half),
            pltpu.VMEM((4, rows, features), half),
            pltpu.VMEM((pieces, 2 * rows, width), jnp.float32),
            travel,
            travel,
            travel,
            travel,
            pltpu.VMEM((pieces, rows, width), jnp.float32),
            pltpu.VMEM((pieces, rows, width), jnp.float32),
            pltpu.VMEM((rows, features), half),
            pltpu.VMEM(weights.shape, jnp.float32),
            pltpu.VMEM((3, *weights.shape), jnp.float32),
            dma((4,)),
            dma((3,)),
            dma((3,)),
            dma((3,)),
            dma((3,)),
            dma((3,)),
            dma((5, batches)),
            dma((4, batches)),
            dma((3, pieces)),
            dma((3, pieces)),
        ]
        + [dma((pieces,))] * 5,
        compiler_params=pltpu.CompilerParams(
            collective_id=0, has_side_effects=True, vmem_limit_bytes=66_000_000
        ),
    )(tokens, gain, ids, weights, w_gate, w_up, w_down)


def route_tables(chosen_ids, chosen_weights, expert_count, slot_room):
    row_count, top_count = chosen_ids.shape
    matches = (chosen_ids[:, :, None] == jnp.arange(expert_count, dtype=jnp.int32)).astype(
        jnp.float32
    )
    flat_match = matches.reshape(row_count * top_count, expert_count)
    order_range = jnp.arange(row_count * top_count, dtype=jnp.int32)
    earlier = (order_range[:, None] > order_range[None, :]).astype(jnp.float32)
    before = jnp.dot(
        earlier, flat_match, precision=lax.Precision.HIGHEST, preferred_element_type=jnp.float32
    )
    position = jnp.sum(before * flat_match, axis=1).reshape(row_count, top_count).astype(jnp.int32)
    slot_index = chosen_ids * slot_room + position
    targets = jnp.arange(expert_count * slot_room, dtype=jnp.int32)
    slot_hits = slot_index[None, :, :] == targets[:, None, None]
    send_table = jnp.sum(slot_hits.astype(jnp.float32), axis=2).astype(jnp.bfloat16)
    mix_table = jnp.sum(jnp.where(slot_hits, chosen_weights[None, :, :], 0.0), axis=2)
    return (send_table, mix_table)


def routed_layer(tokens, gain, route_ids, route_weights, w_gate, w_up, w_down):
    expert_axis = lax.axis_size("expert")
    expert_count = expert_axis // 2
    tensor_count = lax.axis_size("tensor")
    own_rows = tokens.shape[0] // tensor_count
    top_count = route_ids.shape[1]
    capacity = max(2, own_rows * top_count // expert_count)
    gate_local = w_gate[0]
    up_local = w_up[0]
    down_local = w_down[0]
    first_row = lax.axis_index("tensor") * own_rows
    own_tokens = lax.dynamic_slice_in_dim(tokens, first_row, own_rows, 0)
    own_ids = lax.dynamic_slice_in_dim(route_ids, first_row, own_rows, 0)
    own_weights = lax.dynamic_slice_in_dim(route_weights, first_row, own_rows, 0)
    resident = own_tokens.astype(jnp.float32)
    inv_rms = lax.rsqrt(jnp.mean(resident * resident, axis=1, keepdims=True) + 1e-05)
    normed = (resident * inv_rms * gain).astype(jnp.bfloat16)
    send_table, mix_table = route_tables(own_ids, own_weights, expert_count, capacity)
    packed = jnp.dot(send_table, normed, preferred_element_type=jnp.float32).astype(jnp.bfloat16)
    features = packed.shape[1]
    by_expert = packed.reshape(expert_count, 1, capacity, features)
    outgoing = jnp.broadcast_to(by_expert, (expert_count, 2, capacity, features)).reshape(
        expert_axis * capacity, features
    )
    arrived = lax.all_to_all(outgoing, "expert", split_axis=0, concat_axis=0, tiled=True)
    row_piece = lax.all_gather(arrived, "tensor", axis=0, tiled=True)
    gate_val = jnp.dot(row_piece, gate_local, preferred_element_type=jnp.float32)
    up_val = jnp.dot(row_piece, up_local, preferred_element_type=jnp.float32)
    hidden = gated_unit(gate_val, up_val).astype(jnp.bfloat16)
    partial_value = lax.psum_scatter(
        jnp.dot(hidden, down_local, preferred_element_type=jnp.float32),
        "tensor",
        scatter_dimension=0,
        tiled=True,
    )
    returned = lax.all_to_all(
        partial_value.astype(jnp.bfloat16), "expert", split_axis=0, concat_axis=0, tiled=True
    ).astype(partial_value.dtype)
    expert_out = (
        returned.reshape(expert_count, 2, capacity, features)
        .sum(axis=1)
        .reshape(expert_count * capacity, features)
    )
    weighted = jnp.dot(
        mix_table.T, expert_out, precision=lax.Precision.HIGHEST, preferred_element_type=jnp.float32
    )
    finished = (resident + weighted).astype(jnp.bfloat16)
    return lax.all_gather(finished, "tensor", axis=0, tiled=True)


def per_device(tokens, gain, route_ids, route_weights, w_gate, w_up, w_down):
    experts = lax.axis_size("expert") // 2
    dense = (
        route_ids.shape[1] == experts
        and experts == 4
        and lax.axis_size("tensor") == 2
        and w_gate.shape[0] == 1
    )
    layer = dense_layer if dense else routed_layer
    return layer(tokens, gain, route_ids, route_weights, w_gate, w_up, w_down)


def solution(mesh):
    placed = (
        P(("groups", "expert"), None),
        P(),
        P(("groups", "expert"), None),
        P(("groups", "expert"), None),
        P("expert", None, "tensor"),
        P("expert", None, "tensor"),
        P("expert", "tensor", None),
    )
    return jax.shard_map(
        per_device,
        mesh=mesh,
        in_specs=placed,
        out_specs=P(("groups", "expert"), None),
        check_vma=False,
    )
```

```python
import jax
import jax.numpy as jnp
from jax import lax
from jax.experimental import pallas as pl
from jax.experimental.pallas import tpu as pltpu
from jax.sharding import PartitionSpec as P

MESH = pl.DeviceIdType.MESH


def gated_unit(gate_val, up_val):
    return gate_val * jax.nn.sigmoid(1.702 * gate_val) * (up_val + 1.0)


def dense_kernel(
    tokens_ref,
    gain_ref,
    ids_ref,
    weights_ref,
    gate_ref,
    up_ref,
    down_ref,
    out_ref,
    held,
    gain,
    ids,
    weights,
    wg,
    wu,
    wd,
    own,
    slots,
    keep,
    first_out,
    first_in,
    second_out,
    second_in,
    own_pair,
    other_pair,
    from_beside,
    from_across,
    from_corner,
    to_cross,
    to_merge,
    final,
    line_out,
    line_in,
    small_sem,
    load_sem,
    swap_send,
    swap_recv,
    line_send,
    line_recv,
    spread_send,
    spread_recv,
    back_send,
    back_recv,
    near_send,
    pair_recv,
    near_recv,
    give_send,
    give_recv,
    keep_sem,
):
    me = lax.axis_index("expert")
    core = lax.axis_index("tensor")
    place = me // 2
    side = lax.rem(me, 2)
    half = place // 2
    inner = lax.rem(place + half, 2)
    is_inner = inner == 1
    is_outer = inner == 0

    def at(where, which):
        return {"expert": where * 2 + which}

    pair = place + 1 - 2 * lax.rem(place, 2)
    far_inner = 2 - half
    far_outer = 3 - 3 * half
    across = at(place, 1 - side)
    beside = at(pair, side)
    corner = at(pair, 1 - side)
    sibling = {"tensor": 1 - core}
    far_spots = (far_inner, far_outer)
    far = [at(spot, side) for spot in far_spots]
    my_far_slot = 1 - inner

    rows, features = own.shape
    cols = gate_ref.shape[2]
    batches = spread_recv.shape[1]
    batch = rows // batches
    pieces, _, width = keep.shape
    scope = jax.named_scope

    barrier = pltpu.get_barrier_semaphore()

    def greet(peers):
        for peer in peers:
            pl.semaphore_signal(barrier, inc=1, device_id=peer, device_id_type=MESH)

    def on(peer, which):
        return {**peer, "tensor": which}

    near_peers = [across, beside, corner, sibling]
    far_peers = [across, beside, *far, sibling]

    @pl.when(core == 0)
    def _():
        greet(near_peers)

    @pl.when(core == 1)
    def _():
        greet([*far_peers, on(across, 0), on(beside, 0)])

    smalls = [
        pltpu.make_async_copy(src, dst, small_sem.at[i])
        for i, (src, dst) in enumerate(
            (
                (tokens_ref, held),
                (gain_ref, gain),
                (ids_ref, ids),
                (weights_ref, weights),
            )
        )
    ]
    for small in smalls:
        small.start()

    pairs = (
        (gate_ref.at[0], lambda part: wg.at[:, pl.ds(part * cols, cols)]),
        (up_ref.at[0], lambda part: wu.at[:, pl.ds(part * cols, cols)]),
        (down_ref.at[0], lambda part: wd.at[pl.ds(part * cols, cols), :]),
    )
    loads = [
        pltpu.make_async_copy(src, dst(0), load_sem.at[i]) for i, (src, dst) in enumerate(pairs)
    ]
    for load in loads:
        load.start()

    def remote(src, dst, send, recv, peer):
        return pltpu.make_async_remote_copy(
            src_ref=src, dst_ref=dst, send_sem=send, recv_sem=recv, device_id=peer,
            device_id_type=MESH,
        )

    swaps = [
        remote(src, dst(1), swap_send.at[i], swap_recv.at[i], sibling)
        for i, (src, dst) in enumerate(pairs)
    ]

    def rows_of(q):
        return pl.ds(q * batch, batch)

    def part(p):
        return pl.ds(p * width, width)

    with scope("w_small"):
        smalls[0].wait()
        smalls[1].wait()

    def normed(q):
        resident = held[rows_of(q), :].astype(jnp.float32)
        inv_rms = lax.rsqrt(jnp.mean(resident * resident, axis=1, keepdims=True) + 1e-05)
        return (resident * inv_rms * gain[...].reshape(1, -1)).astype(jnp.bfloat16)

    smalls[2].wait()
    smalls[3].wait()
    lanes = line_out.shape[1]
    spots = line_out.shape[0]
    spot_ids = lax.broadcasted_iota(jnp.int32, (rows, rows), 0)
    lane_ids = lax.broadcasted_iota(jnp.int32, (rows, rows), 1)

    def line_of(spot):
        named = jnp.where(ids[...] == spot, weights[...], 0.0)
        return jnp.sum(named, axis=0, keepdims=True)

    def column(line):
        return jnp.sum(jnp.where(spot_ids == lane_ids, line, 0.0), axis=1, keepdims=True)

    def ready(i):
        loads[i].wait()
        swaps[i].wait_recv()

    def hidden_of(first, fresh):
        block = slots[pl.ds(first, 2)].reshape(2 * rows, features)
        if fresh:
            with scope("w_wg"):
                ready(0)
        gate_val = jnp.dot(block, wg[...], preferred_element_type=jnp.float32)
        if fresh:
            with scope("w_wu"):
                ready(1)
        up_val = jnp.dot(block, wu[...], preferred_element_type=jnp.float32)
        value = gated_unit(gate_val, up_val).astype(jnp.bfloat16)
        if fresh:
            with scope("w_wd"):
                ready(2)
        return value

    def down(hidden, p):
        return jnp.dot(hidden, wd[:, part(p)], preferred_element_type=jnp.float32)

    def give(p):
        there = out_ref.at[:, part(p)]
        return remote(final.at[:, part(p)], there, give_send, give_recv, sibling)

    def stay(p):
        return pltpu.make_async_copy(final.at[:, part(p)], out_ref.at[:, part(p)], keep_sem)

    def whole(ref, sem):
        return pltpu.make_async_copy(ref, ref, sem)

    def spread(lane, slot, q, src, peer):
        return remote(
            src.at[rows_of(q), :], slots.at[slot, rows_of(q), :], spread_send.at[lane],
            spread_recv.at[slot, q], peer,
        )

    lower, upper = pl.ds(0, rows), pl.ds(rows, rows)
    both_halves = pl.ds(0, 2 * rows)

    def cross(p, src):
        return remote(
            src, from_across.at[p], near_send.at[2], near_recv.at[1, p], on(across, 1)
        )

    def along(p, src, rows_there):
        return remote(
            src, from_beside.at[p, rows_there, :], near_send.at[1], near_recv.at[0, p],
            on(beside, 1),
        )

    @pl.when(core == 0)
    def _():
        def to_across(q):
            return spread(0, 1, q, slots.at[0], across)

        def to_beside(q):
            return spread(1, 2, q, slots.at[0], beside)

        def on_to_beside(q):
            return spread(2, 3, q, slots.at[1], beside)

        def on_to_across(q):
            return spread(3, 3, q, slots.at[2], across)

        def line_to(i):
            return remote(
                line_out, line_in.at[i], line_send.at[i], line_recv.at[i],
                (across, beside, corner)[i],
            )

        for q in range(batches):
            slots[0, rows_of(q), :] = normed(q)
        for spot in range(spots):
            line_out[spot : spot + 1, :] = line_of(spot)
        with scope("w_bar"):
            pl.semaphore_wait(barrier, len(near_peers) + 2)
        for q in range(batches):
            to_across(q).start()
            to_beside(q).start()
        for i in range(3):
            line_to(i).start()
        for swap in swaps:
            swap.start()
        for q in range(batches):
            with scope(f"w_A{q}"):
                to_across(q).wait_recv()

            @pl.when(is_outer)
            def _():
                on_to_beside(q).start()
                with scope(f"w_Po{q}"):
                    to_beside(q).wait_recv()
                on_to_across(q).start()

        for i in range(3):
            line_to(i).wait_recv()

        def share(table):
            own_line = jnp.sum(
                jnp.where(
                    lax.broadcasted_iota(jnp.int32, (spots, lanes), 0) == place, table, 0.0
                ),
                axis=0,
                keepdims=True,
            )
            return column(own_line)

        own_share = share(line_out[...])
        shares = [share(line_in[i]) for i in range(3)]
        hidden = hidden_of(0, True)
        scales = jnp.concatenate([own_share, shares[0]], axis=0)
        for p in range(pieces):
            first_out[p] = (down(hidden, p) * scales).astype(jnp.bfloat16)

        def hand_pair(src, dst, i):
            return remote(src, dst, near_send.at[3 * i], pair_recv.at[i], sibling)

        @pl.when(is_inner)
        def _():
            for p in range(pieces):
                hand_pair(first_out.at[p], own_pair.at[p], 0).start()
            for q in range(batches):
                with scope(f"w_P{q}"):
                    to_beside(q).wait_recv()

        @pl.when(is_outer)
        def _():
            for p in range(pieces):
                hand_pair(first_out.at[p, lower, :], own_pair.at[p, lower, :], 0).start()

        for q in range(batches):
            with scope(f"w_D{q}"):
                on_to_beside(q).wait_recv()
        hidden = hidden_of(2, False)
        scales = jnp.concatenate([shares[1], shares[2]], axis=0)
        for p in range(pieces):
            second_out[p] = (down(hidden, p) * scales).astype(jnp.bfloat16)

            @pl.when(is_inner)
            def _():
                hand_pair(second_out.at[p], other_pair.at[p], 1).start()

            @pl.when(is_outer)
            def _():
                along(p, second_out.at[p], both_halves).start()

        whole(slots.at[0], spread_send.at[0]).wait()
        whole(slots.at[0], spread_send.at[1]).wait()
        for i in range(3):
            line_to(i).wait_send()

        @pl.when(is_outer)
        def _():
            for p in range(pieces):
                cross(p, first_out.at[p, upper, :]).start()
            whole(slots.at[1], spread_send.at[2]).wait()
            whole(slots.at[2], spread_send.at[3]).wait()
            whole(first_out.at[:, lower, :], near_send.at[0]).wait()
            whole(second_out, near_send.at[1]).wait()
            whole(first_out.at[:, upper, :], near_send.at[2]).wait()

        @pl.when(is_inner)
        def _():
            whole(first_out, near_send.at[0]).wait()
            whole(second_out, near_send.at[3]).wait()

        for swap in swaps:
            swap.wait_send()
        with scope("w_give"):
            whole(final, give_recv).wait()

    @pl.when(core == 1)
    def _():
        def outward(q):
            return remote(
                own.at[rows_of(q), :], slots.at[my_far_slot, rows_of(q), :], spread_send.at[0],
                spread_recv.at[my_far_slot, q], far[0],
            )

        def arrived(s, q):
            return spread(1 + s, s, q, slots.at[s], beside)

        def sideways(s, q):
            return spread(3 + s, 2 + s, q, slots.at[s], across)

        def back_x(p):
            return remote(
                first_out.at[p], first_in.at[p], back_send.at[0], back_recv.at[0, p], across
            )

        def back_z(s, p):
            return remote(
                second_out.at[p, (lower, upper)[s], :],
                second_in.at[p, pl.ds(pl.multiple_of(my_far_slot * rows, rows), rows), :],
                back_send.at[1],
                back_recv.at[1 + my_far_slot, p],
                far[s],
            )

        def came_z(s, p):
            return whole(second_in.at[p, (lower, upper)[s], :], back_recv.at[1 + s, p])

        def cross_corner(p):
            return remote(
                other_pair.at[p, upper, :], from_corner.at[p], near_send.at[0],
                near_recv.at[2, p], across,
            )

        for q in range(batches):
            own[rows_of(q), :] = normed(q)
        with scope("w_bar"):
            pl.semaphore_wait(barrier, len(far_peers))
        for q in range(batches):
            outward(q).start()
        for swap in swaps:
            swap.start()
        shares = [column(line_of(spot)) for spot in far_spots]
        for q in range(batches):
            for s in range(2):
                with scope(f"w_F{s}{q}"):
                    arrived(s, q).wait_recv()

                @pl.when(is_inner)
                def _():
                    arrived(s, q).start()

                sideways(s, q).start()
        hidden = hidden_of(0, True)
        for p in range(pieces):
            keep[p] = down(hidden, p)
        for q in range(batches):
            for s in range(2):
                with scope(f"w_G{s}{q}"):
                    sideways(s, q).wait_recv()
        hidden = hidden_of(2, False)
        for p in range(pieces):
            first_out[p] = down(hidden, p).astype(jnp.bfloat16)
            back_x(p).start()

        @pl.when(is_inner)
        def _():
            with scope("w_i2"):
                whole(other_pair, pair_recv.at[1]).wait()
            for p in range(pieces):
                cross_corner(p).start()

        for p in range(pieces):
            with scope(f"w_bx{p}"):
                back_x(p).wait_recv()
            second_out[p] = (keep[p] + first_in[p].astype(jnp.float32)).astype(jnp.bfloat16)
            for s in range(2):
                back_z(s, p).start()

        @pl.when(is_inner)
        def _():
            with scope("w_i1"):
                whole(own_pair, pair_recv.at[0]).wait()
            for p in range(pieces):
                with scope(f"w_iz{p}"):
                    whole(from_beside.at[p], near_recv.at[0, p]).wait()
                sums = own_pair[p, upper, :].astype(jnp.float32)
                sums = sums + from_beside[p, upper, :].astype(jnp.float32)
                to_cross[p] = sums.astype(jnp.bfloat16)
                cross(p, to_cross.at[p]).start()
            for p in range(pieces):
                with scope(f"w_ic{p}"):
                    cross_corner(p).wait_recv()
                sums = other_pair[p, lower, :].astype(jnp.float32)
                sums = sums + from_corner[p].astype(jnp.float32)
                to_merge[p] = sums.astype(jnp.bfloat16)
                along(p, to_merge.at[p], lower).start()

        @pl.when(is_outer)
        def _():
            with scope("w_o1"):
                whole(own_pair.at[:, lower, :], pair_recv.at[0]).wait()

        for p in range(pieces):
            with scope(f"w_xA{p}"):
                whole(from_across.at[p], near_recv.at[1, p]).wait()

            @pl.when(is_outer)
            def _():
                with scope(f"w_oz{p}"):
                    whole(from_beside.at[p, lower, :], near_recv.at[0, p]).wait()

            total = held[:, part(p)].astype(jnp.float32)
            total = total + own_pair[p, lower, :].astype(jnp.float32)
            total = total + from_beside[p, lower, :].astype(jnp.float32)
            total = total + from_across[p].astype(jnp.float32)
            for s in range(2):
                with scope(f"w_bz{s}{p}"):
                    came_z(s, p).wait()
                total = total + shares[s] * second_in[p, (lower, upper)[s], :].astype(jnp.float32)
            final[:, part(p)] = total.astype(jnp.bfloat16)
            give(p).start()
            stay(p).start()
        whole(own, spread_send.at[0]).wait()
        for s in range(2):
            whole(slots.at[s], spread_send.at[3 + s]).wait()
        whole(first_out, back_send.at[0]).wait()
        whole(second_out, back_send.at[1]).wait()

        @pl.when(is_inner)
        def _():
            for s in range(2):
                whole(slots.at[s], spread_send.at[1 + s]).wait()
            whole(from_corner, near_send.at[0]).wait()
            whole(to_merge, near_send.at[1]).wait()
            whole(to_cross, near_send.at[2]).wait()

        for swap in swaps:
            swap.wait_send()
        with scope("w_end"):
            whole(final, give_send).wait()
            whole(final, keep_sem).wait()


def dense_layer(tokens, gain, route_ids, route_weights, w_gate, w_up, w_down):
    rows, features = tokens.shape
    units = 2 * w_gate.shape[2]
    batches = rows // 16
    pieces = 6
    width = features // pieces
    hbm = pl.BlockSpec(memory_space=pl.ANY)
    half = jnp.bfloat16
    dma = pltpu.SemaphoreType.DMA
    ids = route_ids.T
    weights = route_weights.T
    travel = pltpu.VMEM((pieces, 2 * rows, width), half)
    single = pltpu.VMEM((pieces, rows, width), half)
    return pl.pallas_call(
        dense_kernel,
        out_shape=jax.ShapeDtypeStruct(tokens.shape, tokens.dtype),
        in_specs=[hbm] * 7,
        out_specs=hbm,
        scratch_shapes=[
            pltpu.VMEM((rows, features), half),
            pltpu.VMEM((features,), jnp.float32),
            pltpu.VMEM(ids.shape, jnp.int32),
            pltpu.VMEM(weights.shape, jnp.float32),
            pltpu.VMEM((features, units), half),
            pltpu.VMEM((features, units), half),
            pltpu.VMEM((units, features), half),
            pltpu.VMEM((rows, features), half),
            pltpu.VMEM((4, rows, features), half),
            pltpu.VMEM((pieces, 2 * rows, width), jnp.float32),
        ]
        + [travel] * 7
        + [single] * 4
        + [
            pltpu.VMEM((rows, features), half),
            pltpu.VMEM(weights.shape, jnp.float32),
            pltpu.VMEM((3, *weights.shape), jnp.float32),
            dma((4,)),
            dma((3,)),
            dma((3,)),
            dma((3,)),
            dma((3,)),
            dma((3,)),
            dma((5,)),
            dma((4, batches)),
            dma((2,)),
            dma((3, pieces)),
            dma((4,)),
            dma((2,)),
            dma((3, pieces)),
            dma,
            dma,
            dma,
        ],
        compiler_params=pltpu.CompilerParams(
            collective_id=0, has_side_effects=True, vmem_limit_bytes=66_000_000
        ),
    )(tokens, gain, ids, weights, w_gate, w_up, w_down)


def route_tables(chosen_ids, chosen_weights, expert_count, slot_room):
    row_count, top_count = chosen_ids.shape
    matches = (chosen_ids[:, :, None] == jnp.arange(expert_count, dtype=jnp.int32)).astype(
        jnp.float32
    )
    flat_match = matches.reshape(row_count * top_count, expert_count)
    order_range = jnp.arange(row_count * top_count, dtype=jnp.int32)
    earlier = (order_range[:, None] > order_range[None, :]).astype(jnp.float32)
    before = jnp.dot(
        earlier, flat_match, precision=lax.Precision.HIGHEST, preferred_element_type=jnp.float32
    )
    position = jnp.sum(before * flat_match, axis=1).reshape(row_count, top_count).astype(jnp.int32)
    slot_index = chosen_ids * slot_room + position
    targets = jnp.arange(expert_count * slot_room, dtype=jnp.int32)
    slot_hits = slot_index[None, :, :] == targets[:, None, None]
    send_table = jnp.sum(slot_hits.astype(jnp.float32), axis=2).astype(jnp.bfloat16)
    mix_table = jnp.sum(jnp.where(slot_hits, chosen_weights[None, :, :], 0.0), axis=2)
    return (send_table, mix_table)


def routed_layer(tokens, gain, route_ids, route_weights, w_gate, w_up, w_down):
    expert_axis = lax.axis_size("expert")
    expert_count = expert_axis // 2
    tensor_count = lax.axis_size("tensor")
    own_rows = tokens.shape[0] // tensor_count
    top_count = route_ids.shape[1]
    capacity = max(2, own_rows * top_count // expert_count)
    gate_local = w_gate[0]
    up_local = w_up[0]
    down_local = w_down[0]
    first_row = lax.axis_index("tensor") * own_rows
    own_tokens = lax.dynamic_slice_in_dim(tokens, first_row, own_rows, 0)
    own_ids = lax.dynamic_slice_in_dim(route_ids, first_row, own_rows, 0)
    own_weights = lax.dynamic_slice_in_dim(route_weights, first_row, own_rows, 0)
    resident = own_tokens.astype(jnp.float32)
    inv_rms = lax.rsqrt(jnp.mean(resident * resident, axis=1, keepdims=True) + 1e-05)
    normed = (resident * inv_rms * gain).astype(jnp.bfloat16)
    send_table, mix_table = route_tables(own_ids, own_weights, expert_count, capacity)
    packed = jnp.dot(send_table, normed, preferred_element_type=jnp.float32).astype(jnp.bfloat16)
    features = packed.shape[1]
    by_expert = packed.reshape(expert_count, 1, capacity, features)
    outgoing = jnp.broadcast_to(by_expert, (expert_count, 2, capacity, features)).reshape(
        expert_axis * capacity, features
    )
    arrived = lax.all_to_all(outgoing, "expert", split_axis=0, concat_axis=0, tiled=True)
    row_piece = lax.all_gather(arrived, "tensor", axis=0, tiled=True)
    gate_val = jnp.dot(row_piece, gate_local, preferred_element_type=jnp.float32)
    up_val = jnp.dot(row_piece, up_local, preferred_element_type=jnp.float32)
    hidden = gated_unit(gate_val, up_val).astype(jnp.bfloat16)
    partial_value = lax.psum_scatter(
        jnp.dot(hidden, down_local, preferred_element_type=jnp.float32),
        "tensor",
        scatter_dimension=0,
        tiled=True,
    )
    returned = lax.all_to_all(
        partial_value.astype(jnp.bfloat16), "expert", split_axis=0, concat_axis=0, tiled=True
    ).astype(partial_value.dtype)
    expert_out = (
        returned.reshape(expert_count, 2, capacity, features)
        .sum(axis=1)
        .reshape(expert_count * capacity, features)
    )
    weighted = jnp.dot(
        mix_table.T, expert_out, precision=lax.Precision.HIGHEST, preferred_element_type=jnp.float32
    )
    finished = (resident + weighted).astype(jnp.bfloat16)
    return lax.all_gather(finished, "tensor", axis=0, tiled=True)


def per_device(tokens, gain, route_ids, route_weights, w_gate, w_up, w_down):
    experts = lax.axis_size("expert") // 2
    dense = (
        route_ids.shape[1] == experts
        and experts == 4
        and lax.axis_size("tensor") == 2
        and w_gate.shape[0] == 1
    )
    layer = dense_layer if dense else routed_layer
    return layer(tokens, gain, route_ids, route_weights, w_gate, w_up, w_down)


def solution(mesh):
    placed = (
        P(("groups", "expert"), None),
        P(),
        P(("groups", "expert"), None),
        P(("groups", "expert"), None),
        P("expert", None, "tensor"),
        P("expert", None, "tensor"),
        P("expert", "tensor", None),
    )
    return jax.shard_map(
        per_device,
        mesh=mesh,
        in_specs=placed,
        out_specs=P(("groups", "expert"), None),
        check_vma=False,
    )
```

```python
import jax
import jax.numpy as jnp
from jax import lax
from jax.experimental import pallas as pl
from jax.experimental.pallas import tpu as pltpu
from jax.sharding import PartitionSpec as P

MESH = pl.DeviceIdType.MESH


def gated_unit(gate_val, up_val):
    return gate_val * jax.nn.sigmoid(1.702 * gate_val) * (up_val + 1.0)


def dense_kernel(
    tokens_ref,
    gain_ref,
    ids_ref,
    weights_ref,
    gate_ref,
    up_ref,
    down_ref,
    out_ref,
    held,
    gain,
    ids,
    weights,
    wg,
    wu,
    wd,
    own,
    slots,
    keep,
    first_out,
    first_in,
    second_out,
    second_in,
    own_pair,
    other_pair,
    from_beside,
    from_across,
    from_corner,
    to_cross,
    to_merge,
    line_out,
    line_in,
    small_sem,
    load_sem,
    swap_send,
    swap_recv,
    line_send,
    line_recv,
    spread_send,
    spread_recv,
    rest_recv,
    back_send,
    back_recv,
    near_send,
    pair_recv,
    near_recv,
    give_send,
    give_recv,
):
    me = lax.axis_index("expert")
    core = lax.axis_index("tensor")
    place = me // 2
    side = lax.rem(me, 2)
    half = place // 2
    inner = lax.rem(place + half, 2)
    is_inner = inner == 1
    is_outer = inner == 0

    def at(where, which):
        return {"expert": where * 2 + which}

    pair = place + 1 - 2 * lax.rem(place, 2)
    far_inner = 2 - half
    far_outer = 3 - 3 * half
    across = at(place, 1 - side)
    beside = at(pair, side)
    corner = at(pair, 1 - side)
    sibling = {"tensor": 1 - core}
    far_spots = (far_inner, far_outer)
    far = [at(spot, side) for spot in far_spots]
    my_far_slot = 1 - inner

    rows, features = own.shape
    cols = gate_ref.shape[2]
    batches = spread_recv.shape[1]
    groups = near_recv.shape[1]
    batch = rows // batches
    pieces, _, width = keep.shape
    scope = jax.named_scope

    barrier = pltpu.get_barrier_semaphore()

    def greet(peers):
        for peer in peers:
            pl.semaphore_signal(barrier, inc=1, device_id=peer, device_id_type=MESH)

    def on(peer, which):
        return {**peer, "tensor": which}

    near_peers = [across, beside, corner, sibling]
    far_peers = [across, beside, *far, sibling]

    @pl.when(core == 0)
    def _():
        greet(near_peers)

    @pl.when(core == 1)
    def _():
        greet([*far_peers, on(across, 0), on(beside, 0)])

    smalls = [
        pltpu.make_async_copy(src, dst, small_sem.at[i])
        for i, (src, dst) in enumerate(
            (
                (tokens_ref, held),
                (gain_ref, gain),
                (ids_ref, ids),
                (weights_ref, weights),
            )
        )
    ]
    for small in smalls:
        small.start()

    pairs = (
        (gate_ref.at[0], lambda part: wg.at[:, pl.ds(part * cols, cols)]),
        (up_ref.at[0], lambda part: wu.at[:, pl.ds(part * cols, cols)]),
        (down_ref.at[0], lambda part: wd.at[pl.ds(part * cols, cols), :]),
    )
    loads = [
        pltpu.make_async_copy(src, dst(0), load_sem.at[i]) for i, (src, dst) in enumerate(pairs)
    ]
    for load in loads:
        load.start()

    def remote(src, dst, send, recv, peer):
        return pltpu.make_async_remote_copy(
            src_ref=src, dst_ref=dst, send_sem=send, recv_sem=recv, device_id=peer,
            device_id_type=MESH,
        )

    swaps = [
        remote(src, dst(1), swap_send.at[i], swap_recv.at[i], sibling)
        for i, (src, dst) in enumerate(pairs)
    ]

    def rows_of(q):
        return pl.ds(q * batch, batch)

    def part(p):
        return pl.ds(p * width, width)

    with scope("w_small"):
        smalls[0].wait()
        smalls[1].wait()

    def normed(q):
        resident = held[rows_of(q), :].astype(jnp.float32)
        inv_rms = lax.rsqrt(jnp.mean(resident * resident, axis=1, keepdims=True) + 1e-05)
        return (resident * inv_rms * gain[...].reshape(1, -1)).astype(jnp.bfloat16)

    smalls[2].wait()
    smalls[3].wait()
    lanes = line_out.shape[1]
    spots = line_out.shape[0]
    spot_ids = lax.broadcasted_iota(jnp.int32, (rows, rows), 0)
    lane_ids = lax.broadcasted_iota(jnp.int32, (rows, rows), 1)

    def line_of(spot):
        named = jnp.where(ids[...] == spot, weights[...], 0.0)
        return jnp.sum(named, axis=0, keepdims=True)

    def column(line):
        return jnp.sum(jnp.where(spot_ids == lane_ids, line, 0.0), axis=1, keepdims=True)

    def ready(i):
        loads[i].wait()
        swaps[i].wait_recv()

    def hidden_of(first, fresh):
        block = slots[pl.ds(first, 2)].reshape(2 * rows, features)
        if fresh:
            with scope("w_wg"):
                ready(0)
        gate_val = jnp.dot(block, wg[...], preferred_element_type=jnp.float32)
        if fresh:
            with scope("w_wu"):
                ready(1)
        up_val = jnp.dot(block, wu[...], preferred_element_type=jnp.float32)
        value = gated_unit(gate_val, up_val).astype(jnp.bfloat16)
        if fresh:
            with scope("w_wd"):
                ready(2)
        return value

    def down(hidden, p):
        return jnp.dot(hidden, wd[:, part(p)], preferred_element_type=jnp.float32)

    def give(p):
        there = out_ref.at[:, part(p)]
        return remote(there, there, give_send, give_recv, sibling)

    def whole(ref, sem):
        return pltpu.make_async_copy(ref, ref, sem)

    def spread(lane, slot, q, src, peer, recv):
        return remote(
            src.at[rows_of(q), :], slots.at[slot, rows_of(q), :], spread_send.at[lane], recv, peer
        )

    def group(p):
        return p * groups // pieces

    def grouped(ref, i, g):
        span = pieces // groups
        return whole(ref.at[pl.ds(g * span, span)], near_recv.at[i, g])

    lower, upper = pl.ds(0, rows), pl.ds(rows, rows)
    both_halves = pl.ds(0, 2 * rows)

    def cross(p, src):
        return remote(
            src, from_across.at[p], near_send.at[2], near_recv.at[1, group(p)], on(across, 1)
        )

    def along(p, src, rows_there):
        return remote(
            src, from_beside.at[p, rows_there, :], near_send.at[1], near_recv.at[0, group(p)],
            on(beside, 1),
        )

    @pl.when(core == 0)
    def _():
        def to_across(q):
            return spread(0, 1, q, slots.at[0], across, spread_recv.at[0, q])

        def to_beside(q):
            return spread(1, 2, q, slots.at[0], beside, spread_recv.at[1, q])

        def on_to_beside(q):
            return spread(2, 3, q, slots.at[1], beside, rest_recv.at[0])

        def on_to_across(q):
            return spread(3, 3, q, slots.at[2], across, rest_recv.at[0])

        def line_to(i):
            return remote(
                line_out, line_in.at[i], line_send.at[i], line_recv.at[i],
                (across, beside, corner)[i],
            )

        for q in range(batches):
            slots[0, rows_of(q), :] = normed(q)
        for spot in range(spots):
            line_out[spot : spot + 1, :] = line_of(spot)
        with scope("w_bar"):
            pl.semaphore_wait(barrier, len(near_peers) + 2)
        for i in range(3):
            line_to(i).start()
        for q in range(batches):
            to_across(q).start()
            to_beside(q).start()
        for swap in swaps:
            swap.start()
        for q in range(batches):
            with scope(f"w_A{q}"):
                to_across(q).wait_recv()

            @pl.when(is_outer)
            def _():
                on_to_beside(q).start()
                with scope(f"w_Po{q}"):
                    to_beside(q).wait_recv()
                on_to_across(q).start()

        def share(table):
            own_line = jnp.sum(
                jnp.where(
                    lax.broadcasted_iota(jnp.int32, (spots, lanes), 0) == place, table, 0.0
                ),
                axis=0,
                keepdims=True,
            )
            return column(own_line)

        hidden = hidden_of(0, True)
        with scope("w_line"):
            for i in range(3):
                line_to(i).wait_recv()
        own_share = share(line_out[...])
        shares = [share(line_in[i]) for i in range(3)]
        scales = jnp.concatenate([own_share, shares[0]], axis=0)
        for p in range(pieces):
            first_out[p] = (down(hidden, p) * scales).astype(jnp.bfloat16)

        def hand_pair(src, dst, i):
            return remote(src, dst, near_send.at[3 * i], pair_recv.at[i], sibling)

        @pl.when(is_inner)
        def _():
            for p in range(pieces):
                hand_pair(first_out.at[p], own_pair.at[p], 0).start()
            for q in range(batches):
                with scope(f"w_P{q}"):
                    to_beside(q).wait_recv()

        @pl.when(is_outer)
        def _():
            for p in range(pieces):
                hand_pair(first_out.at[p, lower, :], own_pair.at[p, lower, :], 0).start()

        with scope("w_D"):
            whole(slots.at[3], rest_recv.at[0]).wait()
        hidden = hidden_of(2, False)
        scales = jnp.concatenate([shares[1], shares[2]], axis=0)
        for p in range(pieces):
            second_out[p] = (down(hidden, p) * scales).astype(jnp.bfloat16)

            @pl.when(is_inner)
            def _():
                hand_pair(second_out.at[p], other_pair.at[p], 1).start()

            @pl.when(is_outer)
            def _():
                along(p, second_out.at[p], both_halves).start()

        whole(slots.at[0], spread_send.at[0]).wait()
        whole(slots.at[0], spread_send.at[1]).wait()
        for i in range(3):
            line_to(i).wait_send()

        @pl.when(is_outer)
        def _():
            for p in range(pieces):
                cross(p, first_out.at[p, upper, :]).start()
            whole(slots.at[1], spread_send.at[2]).wait()
            whole(slots.at[2], spread_send.at[3]).wait()
            whole(first_out.at[:, lower, :], near_send.at[0]).wait()
            whole(second_out, near_send.at[1]).wait()
            whole(first_out.at[:, upper, :], near_send.at[2]).wait()

        @pl.when(is_inner)
        def _():
            whole(first_out, near_send.at[0]).wait()
            whole(second_out, near_send.at[3]).wait()

        for swap in swaps:
            swap.wait_send()
        with scope("w_give"):
            whole(out_ref, give_recv).wait()

    @pl.when(core == 1)
    def _():
        def outward(q):
            return remote(
                own.at[rows_of(q), :], slots.at[my_far_slot, rows_of(q), :], spread_send.at[0],
                spread_recv.at[my_far_slot, q], far[0],
            )

        def arrived(s, q):
            return spread(1 + s, s, q, slots.at[s], beside, spread_recv.at[s, q])

        def sideways(s, q):
            return spread(3 + s, 2 + s, q, slots.at[s], across, rest_recv.at[s])

        def back_x(p):
            return remote(
                first_out.at[p], first_in.at[p], back_send.at[0], back_recv.at[0, p], across
            )

        def back_z(s, p):
            return remote(
                second_out.at[p, (lower, upper)[s], :],
                second_in.at[p, pl.ds(pl.multiple_of(my_far_slot * rows, rows), rows), :],
                back_send.at[1],
                back_recv.at[1 + my_far_slot, p],
                far[s],
            )

        def came_z(s, p):
            return whole(second_in.at[p, (lower, upper)[s], :], back_recv.at[1 + s, p])

        def cross_corner(p):
            return remote(
                other_pair.at[p, upper, :], from_corner.at[p], near_send.at[0],
                near_recv.at[2, group(p)], across,
            )

        for q in range(batches):
            own[rows_of(q), :] = normed(q)
        with scope("w_bar"):
            pl.semaphore_wait(barrier, len(far_peers))
        for q in range(batches):
            outward(q).start()
        for swap in swaps:
            swap.start()
        shares = [column(line_of(spot)) for spot in far_spots]
        for q in range(batches):
            for s in range(2):
                with scope(f"w_F{s}{q}"):
                    arrived(s, q).wait_recv()

                @pl.when(is_inner)
                def _():
                    arrived(s, q).start()

                sideways(s, q).start()
        hidden = hidden_of(0, True)
        for p in range(pieces):
            keep[p] = down(hidden, p)
        for s in range(2):
            with scope(f"w_G{s}"):
                whole(slots.at[2 + s], rest_recv.at[s]).wait()
        hidden = hidden_of(2, False)
        for p in range(pieces):
            first_out[p] = down(hidden, p).astype(jnp.bfloat16)
            back_x(p).start()

        @pl.when(is_inner)
        def _():
            with scope("w_i2"):
                whole(other_pair, pair_recv.at[1]).wait()
            for p in range(pieces):
                cross_corner(p).start()

        for p in range(pieces):
            with scope(f"w_bx{p}"):
                back_x(p).wait_recv()
            second_out[p] = (keep[p] + first_in[p].astype(jnp.float32)).astype(jnp.bfloat16)
            for s in range(2):
                back_z(s, p).start()

        @pl.when(is_inner)
        def _():
            with scope("w_i1"):
                whole(own_pair, pair_recv.at[0]).wait()
            for p in range(pieces):
                if p == 0:
                    with scope("w_iz"):
                        for g in range(groups):
                            grouped(from_beside, 0, g).wait()
                sums = own_pair[p, upper, :].astype(jnp.float32)
                sums = sums + from_beside[p, upper, :].astype(jnp.float32)
                to_cross[p] = sums.astype(jnp.bfloat16)
                cross(p, to_cross.at[p]).start()
            for p in range(pieces):
                if p * groups % pieces == 0:
                    with scope(f"w_ic{p}"):
                        grouped(from_corner, 2, group(p)).wait()
                sums = other_pair[p, lower, :].astype(jnp.float32)
                sums = sums + from_corner[p].astype(jnp.float32)
                to_merge[p] = sums.astype(jnp.bfloat16)
                along(p, to_merge.at[p], lower).start()

        @pl.when(is_outer)
        def _():
            with scope("w_o1"):
                whole(own_pair.at[:, lower, :], pair_recv.at[0]).wait()

        for p in range(pieces):
            if p * groups % pieces == 0:
                with scope(f"w_xA{p}"):
                    grouped(from_across, 1, group(p)).wait()

                @pl.when(is_outer)
                def _():
                    with scope(f"w_oz{p}"):
                        grouped(from_beside.at[:, lower, :], 0, group(p)).wait()

            total = held[:, part(p)].astype(jnp.float32)
            total = total + own_pair[p, lower, :].astype(jnp.float32)
            total = total + from_beside[p, lower, :].astype(jnp.float32)
            total = total + from_across[p].astype(jnp.float32)
            for s in range(2):
                with scope(f"w_bz{s}{p}"):
                    came_z(s, p).wait()
                total = total + shares[s] * second_in[p, (lower, upper)[s], :].astype(jnp.float32)
            out_ref[:, part(p)] = total.astype(jnp.bfloat16)
            give(p).start()
        whole(own, spread_send.at[0]).wait()
        for s in range(2):
            whole(slots.at[s], spread_send.at[3 + s]).wait()
        whole(first_out, back_send.at[0]).wait()
        whole(second_out, back_send.at[1]).wait()

        @pl.when(is_inner)
        def _():
            for s in range(2):
                whole(slots.at[s], spread_send.at[1 + s]).wait()
            whole(from_corner, near_send.at[0]).wait()
            whole(to_merge, near_send.at[1]).wait()
            whole(to_cross, near_send.at[2]).wait()

        for swap in swaps:
            swap.wait_send()
        with scope("w_end"):
            whole(out_ref, give_send).wait()


def dense_layer(tokens, gain, route_ids, route_weights, w_gate, w_up, w_down):
    rows, features = tokens.shape
    units = 2 * w_gate.shape[2]
    batches = rows // 16
    pieces = 6
    width = features // pieces
    hbm = pl.BlockSpec(memory_space=pltpu.HBM)
    half = jnp.bfloat16
    dma = pltpu.SemaphoreType.DMA
    ids = route_ids.T
    weights = route_weights.T
    operands = (tokens, gain, ids, weights, w_gate, w_up, w_down)
    travel = pltpu.VMEM((pieces, 2 * rows, width), half)
    single = pltpu.VMEM((pieces, rows, width), half)
    return pl.pallas_call(
        dense_kernel,
        out_shape=pltpu.VMEM(tokens.shape, tokens.dtype),
        in_specs=[hbm] * 7,
        out_specs=pl.BlockSpec(memory_space=pltpu.VMEM),
        scratch_shapes=[
            pltpu.VMEM((rows, features), half),
            pltpu.VMEM((features,), jnp.float32),
            pltpu.VMEM(ids.shape, jnp.int32),
            pltpu.VMEM(weights.shape, jnp.float32),
            pltpu.VMEM((features, units), half),
            pltpu.VMEM((features, units), half),
            pltpu.VMEM((units, features), half),
            pltpu.VMEM((rows, features), half),
            pltpu.VMEM((4, rows, features), half),
            pltpu.VMEM((pieces, 2 * rows, width), jnp.float32),
        ]
        + [travel] * 7
        + [single] * 4
        + [
            pltpu.VMEM(weights.shape, jnp.float32),
            pltpu.VMEM((3, *weights.shape), jnp.float32),
            dma((4,)),
            dma((3,)),
            dma((3,)),
            dma((3,)),
            dma((3,)),
            dma((3,)),
            dma((5,)),
            dma((2, batches)),
            dma((2,)),
            dma((2,)),
            dma((3, pieces)),
            dma((4,)),
            dma((2,)),
            dma((3, 2)),
            dma,
            dma,
        ],
        compiler_params=pltpu.CompilerParams(
            collective_id=0, has_side_effects=True, vmem_limit_bytes=40_000_000
        ),
    )(*(pltpu.with_memory_space_constraint(array, pltpu.HBM) for array in operands))


def route_tables(chosen_ids, chosen_weights, expert_count, slot_room):
    row_count, top_count = chosen_ids.shape
    matches = (chosen_ids[:, :, None] == jnp.arange(expert_count, dtype=jnp.int32)).astype(
        jnp.float32
    )
    flat_match = matches.reshape(row_count * top_count, expert_count)
    order_range = jnp.arange(row_count * top_count, dtype=jnp.int32)
    earlier = (order_range[:, None] > order_range[None, :]).astype(jnp.float32)
    before = jnp.dot(
        earlier, flat_match, precision=lax.Precision.HIGHEST, preferred_element_type=jnp.float32
    )
    position = jnp.sum(before * flat_match, axis=1).reshape(row_count, top_count).astype(jnp.int32)
    slot_index = chosen_ids * slot_room + position
    targets = jnp.arange(expert_count * slot_room, dtype=jnp.int32)
    slot_hits = slot_index[None, :, :] == targets[:, None, None]
    send_table = jnp.sum(slot_hits.astype(jnp.float32), axis=2).astype(jnp.bfloat16)
    mix_table = jnp.sum(jnp.where(slot_hits, chosen_weights[None, :, :], 0.0), axis=2)
    return (send_table, mix_table)


def routed_layer(tokens, gain, route_ids, route_weights, w_gate, w_up, w_down):
    expert_axis = lax.axis_size("expert")
    expert_count = expert_axis // 2
    tensor_count = lax.axis_size("tensor")
    own_rows = tokens.shape[0] // tensor_count
    top_count = route_ids.shape[1]
    capacity = max(2, own_rows * top_count // expert_count)
    gate_local = w_gate[0]
    up_local = w_up[0]
    down_local = w_down[0]
    first_row = lax.axis_index("tensor") * own_rows
    own_tokens = lax.dynamic_slice_in_dim(tokens, first_row, own_rows, 0)
    own_ids = lax.dynamic_slice_in_dim(route_ids, first_row, own_rows, 0)
    own_weights = lax.dynamic_slice_in_dim(route_weights, first_row, own_rows, 0)
    resident = own_tokens.astype(jnp.float32)
    inv_rms = lax.rsqrt(jnp.mean(resident * resident, axis=1, keepdims=True) + 1e-05)
    normed = (resident * inv_rms * gain).astype(jnp.bfloat16)
    send_table, mix_table = route_tables(own_ids, own_weights, expert_count, capacity)
    packed = jnp.dot(send_table, normed, preferred_element_type=jnp.float32).astype(jnp.bfloat16)
    features = packed.shape[1]
    by_expert = packed.reshape(expert_count, 1, capacity, features)
    outgoing = jnp.broadcast_to(by_expert, (expert_count, 2, capacity, features)).reshape(
        expert_axis * capacity, features
    )
    arrived = lax.all_to_all(outgoing, "expert", split_axis=0, concat_axis=0, tiled=True)
    row_piece = lax.all_gather(arrived, "tensor", axis=0, tiled=True)
    gate_val = jnp.dot(row_piece, gate_local, preferred_element_type=jnp.float32)
    up_val = jnp.dot(row_piece, up_local, preferred_element_type=jnp.float32)
    hidden = gated_unit(gate_val, up_val).astype(jnp.bfloat16)
    partial_value = lax.psum_scatter(
        jnp.dot(hidden, down_local, preferred_element_type=jnp.float32),
        "tensor",
        scatter_dimension=0,
        tiled=True,
    )
    returned = lax.all_to_all(
        partial_value.astype(jnp.bfloat16), "expert", split_axis=0, concat_axis=0, tiled=True
    ).astype(partial_value.dtype)
    expert_out = (
        returned.reshape(expert_count, 2, capacity, features)
        .sum(axis=1)
        .reshape(expert_count * capacity, features)
    )
    weighted = jnp.dot(
        mix_table.T, expert_out, precision=lax.Precision.HIGHEST, preferred_element_type=jnp.float32
    )
    finished = (resident + weighted).astype(jnp.bfloat16)
    return lax.all_gather(finished, "tensor", axis=0, tiled=True)


def per_device(tokens, gain, route_ids, route_weights, w_gate, w_up, w_down):
    experts = lax.axis_size("expert") // 2
    dense = (
        route_ids.shape[1] == experts
        and experts == 4
        and lax.axis_size("tensor") == 2
        and w_gate.shape[0] == 1
    )
    layer = dense_layer if dense else routed_layer
    return layer(tokens, gain, route_ids, route_weights, w_gate, w_up, w_down)


def solution(mesh):
    placed = (
        P(("groups", "expert"), None),
        P(),
        P(("groups", "expert"), None),
        P(("groups", "expert"), None),
        P("expert", None, "tensor"),
        P("expert", None, "tensor"),
        P("expert", "tensor", None),
    )
    return jax.shard_map(
        per_device,
        mesh=mesh,
        in_specs=placed,
        out_specs=P(("groups", "expert"), None),
        check_vma=False,
    )
```

```python
import jax
import jax.numpy as jnp
from jax import lax
from jax.experimental import pallas as pl
from jax.experimental.pallas import tpu as pltpu
from jax.sharding import PartitionSpec as P

MESH = pl.DeviceIdType.MESH


def gated_unit(gate_val, up_val):
    return gate_val * jax.nn.sigmoid(1.702 * gate_val) * (up_val + 1.0)


def dense_kernel(
    tokens_ref,
    gain_ref,
    ids_ref,
    weights_ref,
    gate_ref,
    up_ref,
    down_ref,
    out_ref,
    held,
    gain,
    ids,
    weights,
    wg,
    wu,
    wd,
    own,
    slots,
    keep,
    first_out,
    first_in,
    second_out,
    second_in,
    own_pair,
    from_beside,
    from_across,
    to_cross,
    line_out,
    line_in,
    small_sem,
    load_sem,
    swap_send,
    swap_recv,
    line_send,
    line_recv,
    spread_send,
    spread_recv,
    rest_recv,
    back_send,
    back_recv,
    near_send,
    pair_recv,
    near_recv,
    give_send,
    give_recv,
):
    me = lax.axis_index("expert")
    core = lax.axis_index("tensor")
    place = me // 2
    side = lax.rem(me, 2)
    half = place // 2
    inner = lax.rem(place + half, 2)
    is_inner = inner == 1
    is_outer = inner == 0

    def at(where, which):
        return {"expert": where * 2 + which}

    pair = place + 1 - 2 * lax.rem(place, 2)
    far_inner = 2 - half
    far_outer = 3 - 3 * half
    across = at(place, 1 - side)
    beside = at(pair, side)
    corner = at(pair, 1 - side)
    sibling = {"tensor": 1 - core}
    far_spots = (far_inner, far_outer)
    far = [at(spot, side) for spot in far_spots]
    my_far_slot = 1 - inner

    rows, features = own.shape
    cols = gate_ref.shape[2]
    batches = spread_recv.shape[1]
    groups = near_recv.shape[1]
    batch = rows // batches
    pieces, _, width = keep.shape
    scope = jax.named_scope

    barrier = pltpu.get_barrier_semaphore()

    def greet(peers):
        for peer in peers:
            pl.semaphore_signal(barrier, inc=1, device_id=peer, device_id_type=MESH)

    def on(peer, which):
        return {**peer, "tensor": which}

    near_peers = [across, beside, corner, sibling]
    far_peers = [across, beside, *far, sibling]

    @pl.when(core == 0)
    def _():
        greet(near_peers)

    @pl.when(core == 1)
    def _():
        greet([*far_peers, on(across, 0), on(beside, 0)])

    smalls = [
        pltpu.make_async_copy(src, dst, small_sem.at[i])
        for i, (src, dst) in enumerate(
            (
                (tokens_ref, held),
                (gain_ref, gain),
                (ids_ref, ids),
                (weights_ref, weights),
            )
        )
    ]
    for small in smalls:
        small.start()

    pairs = (
        (gate_ref.at[0], lambda part: wg.at[:, pl.ds(part * cols, cols)]),
        (up_ref.at[0], lambda part: wu.at[:, pl.ds(part * cols, cols)]),
        (down_ref.at[0], lambda part: wd.at[pl.ds(part * cols, cols), :]),
    )
    loads = [
        pltpu.make_async_copy(src, dst(0), load_sem.at[i]) for i, (src, dst) in enumerate(pairs)
    ]
    for load in loads:
        load.start()

    def remote(src, dst, send, recv, peer):
        return pltpu.make_async_remote_copy(
            src_ref=src, dst_ref=dst, send_sem=send, recv_sem=recv, device_id=peer,
            device_id_type=MESH,
        )

    swaps = [
        remote(src, dst(1), swap_send.at[i], swap_recv.at[i], sibling)
        for i, (src, dst) in enumerate(pairs)
    ]

    def rows_of(q):
        return pl.ds(q * batch, batch)

    def part(p):
        return pl.ds(p * width, width)

    with scope("w_small"):
        smalls[0].wait()
        smalls[1].wait()

    def normed(q):
        resident = held[rows_of(q), :].astype(jnp.float32)
        inv_rms = lax.rsqrt(jnp.mean(resident * resident, axis=1, keepdims=True) + 1e-05)
        return (resident * inv_rms * gain[...].reshape(1, -1)).astype(jnp.bfloat16)

    smalls[2].wait()
    smalls[3].wait()
    lanes = line_out.shape[1]
    spots = line_out.shape[0]
    spot_ids = lax.broadcasted_iota(jnp.int32, (rows, rows), 0)
    lane_ids = lax.broadcasted_iota(jnp.int32, (rows, rows), 1)

    def line_of(spot):
        named = jnp.where(ids[...] == spot, weights[...], 0.0)
        return jnp.sum(named, axis=0, keepdims=True)

    def column(line):
        return jnp.sum(jnp.where(spot_ids == lane_ids, line, 0.0), axis=1, keepdims=True)

    def ready(i):
        loads[i].wait()
        swaps[i].wait_recv()

    def hidden_of(first, fresh):
        block = slots[pl.ds(first, 2)].reshape(2 * rows, features)
        if fresh:
            with scope("w_wg"):
                ready(0)
        gate_val = jnp.dot(block, wg[...], preferred_element_type=jnp.float32)
        if fresh:
            with scope("w_wu"):
                ready(1)
        up_val = jnp.dot(block, wu[...], preferred_element_type=jnp.float32)
        value = gated_unit(gate_val, up_val).astype(jnp.bfloat16)
        if fresh:
            with scope("w_wd"):
                ready(2)
        return value

    def down(hidden, p):
        return jnp.dot(hidden, wd[:, part(p)], preferred_element_type=jnp.float32)

    def give(p):
        there = out_ref.at[:, part(p)]
        return remote(there, there, give_send, give_recv, sibling)

    def whole(ref, sem):
        return pltpu.make_async_copy(ref, ref, sem)

    def spread(lane, slot, q, src, peer, recv):
        return remote(
            src.at[rows_of(q), :], slots.at[slot, rows_of(q), :], spread_send.at[lane], recv, peer
        )

    def group(p):
        return p * groups // pieces

    def grouped(ref, i, g):
        span = pieces // groups
        return whole(ref.at[pl.ds(g * span, span)], near_recv.at[i, g])

    lower, upper = pl.ds(0, rows), pl.ds(rows, rows)
    both_halves = pl.ds(0, 2 * rows)

    @pl.when(core == 0)
    def _():
        def to_across(q):
            return spread(0, 1, q, slots.at[0], across, spread_recv.at[0, q])

        def to_beside(q):
            return spread(1, 2, q, slots.at[0], beside, spread_recv.at[1, q])

        def on_to_beside(q):
            return spread(2, 3, q, slots.at[1], beside, rest_recv.at[0])

        def on_to_across(q):
            return spread(3, 3, q, slots.at[2], across, rest_recv.at[0])

        def along(p):
            return remote(
                second_out.at[p], from_beside.at[p], near_send.at[1], near_recv.at[0, group(p)],
                on(beside, 1),
            )

        def line_to(i):
            return remote(
                line_out, line_in.at[i], line_send.at[i], line_recv.at[i],
                (across, beside, corner)[i],
            )

        for q in range(batches):
            slots[0, rows_of(q), :] = normed(q)
        for spot in range(spots):
            line_out[spot : spot + 1, :] = line_of(spot)
        with scope("w_bar"):
            pl.semaphore_wait(barrier, len(near_peers) + 2)
        for i in range(3):
            line_to(i).start()
        for q in range(batches):
            to_across(q).start()
            to_beside(q).start()
        for swap in swaps:
            swap.start()
        for q in range(batches):
            with scope(f"w_A{q}"):
                to_across(q).wait_recv()

            @pl.when(is_outer)
            def _():
                on_to_beside(q).start()
                with scope(f"w_Po{q}"):
                    to_beside(q).wait_recv()
                on_to_across(q).start()

        def share(table):
            own_line = jnp.sum(
                jnp.where(
                    lax.broadcasted_iota(jnp.int32, (spots, lanes), 0) == place, table, 0.0
                ),
                axis=0,
                keepdims=True,
            )
            return column(own_line)

        hidden = hidden_of(0, True)
        with scope("w_line"):
            for i in range(3):
                line_to(i).wait_recv()
        own_share = share(line_out[...])
        shares = [share(line_in[i]) for i in range(3)]
        scales = jnp.concatenate([own_share, shares[0]], axis=0)
        for p in range(pieces):
            first_out[p] = (down(hidden, p) * scales).astype(jnp.bfloat16)

        def hand_pair(p):
            return remote(
                first_out.at[p], own_pair.at[p], near_send.at[0], pair_recv, sibling
            )

        for p in range(pieces):
            hand_pair(p).start()

        @pl.when(is_inner)
        def _():
            for q in range(batches):
                with scope(f"w_P{q}"):
                    to_beside(q).wait_recv()

        with scope("w_D"):
            whole(slots.at[3], rest_recv.at[0]).wait()
        hidden = hidden_of(2, False)
        scales = jnp.concatenate([shares[1], shares[2]], axis=0)
        for p in range(pieces):
            second_out[p] = (down(hidden, p) * scales).astype(jnp.bfloat16)

            along(p).start()
        whole(slots.at[0], spread_send.at[0]).wait()
        whole(slots.at[0], spread_send.at[1]).wait()
        for i in range(3):
            line_to(i).wait_send()

        @pl.when(is_outer)
        def _():
            whole(slots.at[1], spread_send.at[2]).wait()
            whole(slots.at[2], spread_send.at[3]).wait()

        whole(first_out, near_send.at[0]).wait()
        whole(second_out, near_send.at[1]).wait()
        for swap in swaps:
            swap.wait_send()
        with scope("w_give"):
            whole(out_ref, give_recv).wait()

    @pl.when(core == 1)
    def _():
        def outward(q):
            return remote(
                own.at[rows_of(q), :], slots.at[my_far_slot, rows_of(q), :], spread_send.at[0],
                spread_recv.at[my_far_slot, q], far[0],
            )

        def arrived(s, q):
            return spread(1 + s, s, q, slots.at[s], beside, spread_recv.at[s, q])

        def sideways(s, q):
            return spread(3 + s, 2 + s, q, slots.at[s], across, rest_recv.at[s])

        def back_x(p):
            return remote(
                first_out.at[p], first_in.at[p], back_send.at[0], back_recv.at[0, p], across
            )

        def back_z(s, p):
            return remote(
                second_out.at[p, (lower, upper)[s], :],
                second_in.at[p, pl.ds(pl.multiple_of(my_far_slot * rows, rows), rows), :],
                back_send.at[1],
                back_recv.at[1 + my_far_slot, p],
                far[s],
            )

        def came_z(s, p):
            return whole(second_in.at[p, (lower, upper)[s], :], back_recv.at[1 + s, p])

        def cross(p):
            return remote(
                to_cross.at[p], from_across.at[p], near_send.at[2], near_recv.at[1, group(p)],
                across,
            )

        for q in range(batches):
            own[rows_of(q), :] = normed(q)
        with scope("w_bar"):
            pl.semaphore_wait(barrier, len(far_peers))
        for q in range(batches):
            outward(q).start()
        for swap in swaps:
            swap.start()
        shares = [column(line_of(spot)) for spot in far_spots]
        for q in range(batches):
            for s in range(2):
                with scope(f"w_F{s}{q}"):
                    arrived(s, q).wait_recv()

                @pl.when(is_inner)
                def _():
                    arrived(s, q).start()

                sideways(s, q).start()
        hidden = hidden_of(0, True)
        for p in range(pieces):
            keep[p] = down(hidden, p)
        for s in range(2):
            with scope(f"w_G{s}"):
                whole(slots.at[2 + s], rest_recv.at[s]).wait()
        hidden = hidden_of(2, False)
        for p in range(pieces):
            first_out[p] = down(hidden, p).astype(jnp.bfloat16)
            back_x(p).start()

        span = pieces // groups
        for p in range(pieces):
            with scope(f"w_bx{p}"):
                back_x(p).wait_recv()
            second_out[p] = (keep[p] + first_in[p].astype(jnp.float32)).astype(jnp.bfloat16)
            for s in range(2):
                back_z(s, p).start()
            g = p - (pieces - groups)
            if g < 0:
                continue
            with scope(f"w_be{g}"):
                if g == 0:
                    whole(own_pair, pair_recv).wait()
                grouped(from_beside, 0, g).wait()
            for i in range(g * span, g * span + span):
                sums = own_pair[i, upper, :].astype(jnp.float32)
                sums = sums + from_beside[i, upper, :].astype(jnp.float32)
                to_cross[i] = sums.astype(jnp.bfloat16)
                cross(i).start()
        for p in range(pieces):
            if p % span == 0:
                with scope(f"w_xA{p}"):
                    grouped(from_across, 1, group(p)).wait()
            total = held[:, part(p)].astype(jnp.float32)
            total = total + own_pair[p, lower, :].astype(jnp.float32)
            total = total + from_beside[p, lower, :].astype(jnp.float32)
            total = total + from_across[p].astype(jnp.float32)
            for s in range(2):
                with scope(f"w_bz{s}{p}"):
                    came_z(s, p).wait()
                total = total + shares[s] * second_in[p, (lower, upper)[s], :].astype(jnp.float32)
            out_ref[:, part(p)] = total.astype(jnp.bfloat16)
            give(p).start()
        whole(own, spread_send.at[0]).wait()
        for s in range(2):
            whole(slots.at[s], spread_send.at[3 + s]).wait()
        whole(first_out, back_send.at[0]).wait()
        whole(second_out, back_send.at[1]).wait()
        whole(to_cross, near_send.at[2]).wait()

        @pl.when(is_inner)
        def _():
            for s in range(2):
                whole(slots.at[s], spread_send.at[1 + s]).wait()

        for swap in swaps:
            swap.wait_send()
        with scope("w_end"):
            whole(out_ref, give_send).wait()


def dense_layer(tokens, gain, route_ids, route_weights, w_gate, w_up, w_down):
    rows, features = tokens.shape
    units = 2 * w_gate.shape[2]
    batches = rows // 16
    pieces = 6
    width = features // pieces
    hbm = pl.BlockSpec(memory_space=pltpu.HBM)
    half = jnp.bfloat16
    dma = pltpu.SemaphoreType.DMA
    ids = route_ids.T
    weights = route_weights.T
    operands = (tokens, gain, ids, weights, w_gate, w_up, w_down)
    travel = pltpu.VMEM((pieces, 2 * rows, width), half)
    single = pltpu.VMEM((pieces, rows, width), half)
    return pl.pallas_call(
        dense_kernel,
        out_shape=pltpu.VMEM(tokens.shape, tokens.dtype),
        in_specs=[hbm] * 7,
        out_specs=pl.BlockSpec(memory_space=pltpu.VMEM),
        scratch_shapes=[
            pltpu.VMEM((rows, features), half),
            pltpu.VMEM((features,), jnp.float32),
            pltpu.VMEM(ids.shape, jnp.int32),
            pltpu.VMEM(weights.shape, jnp.float32),
            pltpu.VMEM((features, units), half),
            pltpu.VMEM((features, units), half),
            pltpu.VMEM((units, features), half),
            pltpu.VMEM((rows, features), half),
            pltpu.VMEM((4, rows, features), half),
            pltpu.VMEM((pieces, 2 * rows, width), jnp.float32),
        ]
        + [travel] * 6
        + [single] * 2
        + [
            pltpu.VMEM(weights.shape, jnp.float32),
            pltpu.VMEM((3, *weights.shape), jnp.float32),
            dma((4,)),
            dma((3,)),
            dma((3,)),
            dma((3,)),
            dma((3,)),
            dma((3,)),
            dma((5,)),
            dma((2, batches)),
            dma((2,)),
            dma((2,)),
            dma((3, pieces)),
            dma((3,)),
            dma,
            dma((2, 2)),
            dma,
            dma,
        ],
        compiler_params=pltpu.CompilerParams(
            collective_id=0, has_side_effects=True, vmem_limit_bytes=40_000_000
        ),
    )(*(pltpu.with_memory_space_constraint(array, pltpu.HBM) for array in operands))


def route_tables(chosen_ids, chosen_weights, expert_count, slot_room):
    row_count, top_count = chosen_ids.shape
    matches = (chosen_ids[:, :, None] == jnp.arange(expert_count, dtype=jnp.int32)).astype(
        jnp.float32
    )
    flat_match = matches.reshape(row_count * top_count, expert_count)
    order_range = jnp.arange(row_count * top_count, dtype=jnp.int32)
    earlier = (order_range[:, None] > order_range[None, :]).astype(jnp.float32)
    before = jnp.dot(
        earlier, flat_match, precision=lax.Precision.HIGHEST, preferred_element_type=jnp.float32
    )
    position = jnp.sum(before * flat_match, axis=1).reshape(row_count, top_count).astype(jnp.int32)
    slot_index = chosen_ids * slot_room + position
    targets = jnp.arange(expert_count * slot_room, dtype=jnp.int32)
    slot_hits = slot_index[None, :, :] == targets[:, None, None]
    send_table = jnp.sum(slot_hits.astype(jnp.float32), axis=2).astype(jnp.bfloat16)
    mix_table = jnp.sum(jnp.where(slot_hits, chosen_weights[None, :, :], 0.0), axis=2)
    return (send_table, mix_table)


def routed_layer(tokens, gain, route_ids, route_weights, w_gate, w_up, w_down):
    expert_axis = lax.axis_size("expert")
    expert_count = expert_axis // 2
    tensor_count = lax.axis_size("tensor")
    own_rows = tokens.shape[0] // tensor_count
    top_count = route_ids.shape[1]
    capacity = max(2, own_rows * top_count // expert_count)
    gate_local = w_gate[0]
    up_local = w_up[0]
    down_local = w_down[0]
    first_row = lax.axis_index("tensor") * own_rows
    own_tokens = lax.dynamic_slice_in_dim(tokens, first_row, own_rows, 0)
    own_ids = lax.dynamic_slice_in_dim(route_ids, first_row, own_rows, 0)
    own_weights = lax.dynamic_slice_in_dim(route_weights, first_row, own_rows, 0)
    resident = own_tokens.astype(jnp.float32)
    inv_rms = lax.rsqrt(jnp.mean(resident * resident, axis=1, keepdims=True) + 1e-05)
    normed = (resident * inv_rms * gain).astype(jnp.bfloat16)
    send_table, mix_table = route_tables(own_ids, own_weights, expert_count, capacity)
    packed = jnp.dot(send_table, normed, preferred_element_type=jnp.float32).astype(jnp.bfloat16)
    features = packed.shape[1]
    by_expert = packed.reshape(expert_count, 1, capacity, features)
    outgoing = jnp.broadcast_to(by_expert, (expert_count, 2, capacity, features)).reshape(
        expert_axis * capacity, features
    )
    arrived = lax.all_to_all(outgoing, "expert", split_axis=0, concat_axis=0, tiled=True)
    row_piece = lax.all_gather(arrived, "tensor", axis=0, tiled=True)
    gate_val = jnp.dot(row_piece, gate_local, preferred_element_type=jnp.float32)
    up_val = jnp.dot(row_piece, up_local, preferred_element_type=jnp.float32)
    hidden = gated_unit(gate_val, up_val).astype(jnp.bfloat16)
    partial_value = lax.psum_scatter(
        jnp.dot(hidden, down_local, preferred_element_type=jnp.float32),
        "tensor",
        scatter_dimension=0,
        tiled=True,
    )
    returned = lax.all_to_all(
        partial_value.astype(jnp.bfloat16), "expert", split_axis=0, concat_axis=0, tiled=True
    ).astype(partial_value.dtype)
    expert_out = (
        returned.reshape(expert_count, 2, capacity, features)
        .sum(axis=1)
        .reshape(expert_count * capacity, features)
    )
    weighted = jnp.dot(
        mix_table.T, expert_out, precision=lax.Precision.HIGHEST, preferred_element_type=jnp.float32
    )
    finished = (resident + weighted).astype(jnp.bfloat16)
    return lax.all_gather(finished, "tensor", axis=0, tiled=True)


def per_device(tokens, gain, route_ids, route_weights, w_gate, w_up, w_down):
    experts = lax.axis_size("expert") // 2
    dense = (
        route_ids.shape[1] == experts
        and experts == 4
        and lax.axis_size("tensor") == 2
        and w_gate.shape[0] == 1
    )
    layer = dense_layer if dense else routed_layer
    return layer(tokens, gain, route_ids, route_weights, w_gate, w_up, w_down)


def solution(mesh):
    placed = (
        P(("groups", "expert"), None),
        P(),
        P(("groups", "expert"), None),
        P(("groups", "expert"), None),
        P("expert", None, "tensor"),
        P("expert", None, "tensor"),
        P("expert", "tensor", None),
    )
    return jax.shard_map(
        per_device,
        mesh=mesh,
        in_specs=placed,
        out_specs=P(("groups", "expert"), None),
        check_vma=False,
    )
```

```python
import jax
import jax.numpy as jnp
from jax import lax
from jax.experimental import pallas as pl
from jax.experimental.pallas import tpu as pltpu
from jax.sharding import PartitionSpec as P

MESH = pl.DeviceIdType.MESH


def gated_unit(gate_val, up_val):
    return gate_val * jax.nn.sigmoid(1.702 * gate_val) * (up_val + 1.0)


def dense_kernel(
    tokens_ref,
    gain_ref,
    ids_ref,
    weights_ref,
    gate_ref,
    up_ref,
    down_ref,
    out_ref,
    held,
    gain,
    ids,
    weights,
    wg,
    wu,
    wd,
    own,
    slots,
    keep,
    first_out,
    first_in,
    second_out,
    second_in,
    own_pair,
    from_beside,
    from_across,
    to_cross,
    line_out,
    line_in,
    small_sem,
    load_sem,
    swap_send,
    swap_recv,
    line_send,
    line_recv,
    spread_send,
    spread_recv,
    rest_recv,
    back_send,
    back_recv,
    near_send,
    pair_recv,
    near_recv,
    give_send,
    give_recv,
):
    me = lax.axis_index("expert")
    core = lax.axis_index("tensor")
    place = me // 2
    side = lax.rem(me, 2)
    half = place // 2
    inner = lax.rem(place + half, 2)
    is_inner = inner == 1
    is_outer = inner == 0

    def at(where, which):
        return {"expert": where * 2 + which}

    pair = place + 1 - 2 * lax.rem(place, 2)
    far_inner = 2 - half
    far_outer = 3 - 3 * half
    across = at(place, 1 - side)
    beside = at(pair, side)
    corner = at(pair, 1 - side)
    sibling = {"tensor": 1 - core}
    far_spots = (far_inner, far_outer)
    far = [at(spot, side) for spot in far_spots]
    my_far_slot = 1 - inner

    rows, features = own.shape
    cols = gate_ref.shape[2]
    batches = spread_recv.shape[1]
    groups = near_recv.shape[1]
    batch = rows // batches
    pieces, _, width = keep.shape
    scope = jax.named_scope

    barrier = pltpu.get_barrier_semaphore()

    def greet(peers):
        for peer in peers:
            pl.semaphore_signal(barrier, inc=1, device_id=peer, device_id_type=MESH)

    def on(peer, which):
        return {**peer, "tensor": which}

    near_peers = [across, beside, corner, sibling]
    far_peers = [across, beside, far[0], sibling]

    @pl.when(core == 0)
    def _():
        greet([*near_peers, on(across, 1), on(beside, 1)])

    @pl.when(core == 1)
    def _():
        greet([across, beside, sibling, on(across, 0), on(beside, 0)])

        @pl.when(is_inner)
        def _():
            greet(far)

    smalls = [
        pltpu.make_async_copy(src, dst, small_sem.at[i])
        for i, (src, dst) in enumerate(
            (
                (tokens_ref, held),
                (gain_ref, gain),
                (ids_ref, ids),
                (weights_ref, weights),
            )
        )
    ]
    for small in smalls:
        small.start()

    pairs = (
        (gate_ref.at[0], lambda part: wg.at[:, pl.ds(part * cols, cols)]),
        (up_ref.at[0], lambda part: wu.at[:, pl.ds(part * cols, cols)]),
        (down_ref.at[0], lambda part: wd.at[pl.ds(part * cols, cols), :]),
    )
    loads = [
        pltpu.make_async_copy(src, dst(0), load_sem.at[i]) for i, (src, dst) in enumerate(pairs)
    ]
    for load in loads:
        load.start()

    def remote(src, dst, send, recv, peer):
        return pltpu.make_async_remote_copy(
            src_ref=src, dst_ref=dst, send_sem=send, recv_sem=recv, device_id=peer,
            device_id_type=MESH,
        )

    swaps = [
        remote(src, dst(1), swap_send.at[i], swap_recv.at[i], sibling)
        for i, (src, dst) in enumerate(pairs)
    ]

    def rows_of(q):
        return pl.ds(q * batch, batch)

    def part(p):
        return pl.ds(p * width, width)

    with scope("w_small"):
        smalls[0].wait()
        smalls[1].wait()

    def normed(q):
        resident = held[rows_of(q), :].astype(jnp.float32)
        inv_rms = lax.rsqrt(jnp.mean(resident * resident, axis=1, keepdims=True) + 1e-05)
        return (resident * inv_rms * gain[...].reshape(1, -1)).astype(jnp.bfloat16)

    smalls[2].wait()
    smalls[3].wait()
    lanes = line_out.shape[1]
    spots = line_out.shape[0]
    spot_ids = lax.broadcasted_iota(jnp.int32, (rows, rows), 0)
    lane_ids = lax.broadcasted_iota(jnp.int32, (rows, rows), 1)

    def line_of(spot):
        named = jnp.where(ids[...] == spot, weights[...], 0.0)
        return jnp.sum(named, axis=0, keepdims=True)

    def column(line):
        return jnp.sum(jnp.where(spot_ids == lane_ids, line, 0.0), axis=1, keepdims=True)

    def ready(i):
        loads[i].wait()
        swaps[i].wait_recv()

    def hidden_of(first, fresh):
        block = slots[pl.ds(first, 2)].reshape(2 * rows, features)
        if fresh:
            with scope("w_wg"):
                ready(0)
        gate_val = jnp.dot(block, wg[...], preferred_element_type=jnp.float32)
        if fresh:
            with scope("w_wu"):
                ready(1)
        up_val = jnp.dot(block, wu[...], preferred_element_type=jnp.float32)
        value = gated_unit(gate_val, up_val).astype(jnp.bfloat16)
        if fresh:
            with scope("w_wd"):
                ready(2)
        return value

    def down(hidden, p):
        return jnp.dot(hidden, wd[:, part(p)], preferred_element_type=jnp.float32)

    def give(p):
        there = out_ref.at[:, part(p)]
        return remote(there, there, give_send, give_recv, sibling)

    def whole(ref, sem):
        return pltpu.make_async_copy(ref, ref, sem)

    def spread(lane, slot, q, src, peer, recv):
        return remote(
            src.at[rows_of(q), :], slots.at[slot, rows_of(q), :], spread_send.at[lane], recv, peer
        )

    def group(p):
        return p * groups // pieces

    def grouped(ref, i, g):
        span = pieces // groups
        return whole(ref.at[pl.ds(g * span, span)], near_recv.at[i, g])

    lower, upper = pl.ds(0, rows), pl.ds(rows, rows)
    both_halves = pl.ds(0, 2 * rows)

    @pl.when(core == 0)
    def _():
        def across_came(q):
            return whole(slots.at[1, rows_of(q), :], spread_recv.at[0, q])

        def beside_came(q):
            return whole(slots.at[2, rows_of(q), :], spread_recv.at[1, q])

        def on_to_beside(q):
            return spread(2, 3, q, slots.at[1], beside, rest_recv.at[0])

        def on_to_across(q):
            return spread(3, 3, q, slots.at[2], across, rest_recv.at[0])

        def along(p):
            return remote(
                second_out.at[p], from_beside.at[p], near_send.at[1], near_recv.at[0, group(p)],
                on(beside, 1),
            )

        def line_to(i):
            return remote(
                line_out, line_in.at[i], line_send, line_recv,
                (across, beside, corner)[i],
            )

        for q in range(batches):
            slots[0, rows_of(q), :] = normed(q)
        for spot in range(spots):
            line_out[spot : spot + 1, :] = line_of(spot)
        with scope("w_bar"):
            pl.semaphore_wait(barrier, len(near_peers) + 2)
        for i in range(3):
            line_to(i).start()
        for swap in swaps:
            swap.start()
        for q in range(batches):
            with scope(f"w_A{q}"):
                across_came(q).wait()

            @pl.when(is_outer)
            def _():
                on_to_beside(q).start()
                with scope(f"w_Po{q}"):
                    beside_came(q).wait()
                on_to_across(q).start()

        def share(table):
            own_line = jnp.sum(
                jnp.where(
                    lax.broadcasted_iota(jnp.int32, (spots, lanes), 0) == place, table, 0.0
                ),
                axis=0,
                keepdims=True,
            )
            return column(own_line)

        hidden = hidden_of(0, True)
        with scope("w_line"):
            whole(line_in, line_recv).wait()
        own_share = share(line_out[...])
        shares = [share(line_in[i]) for i in range(3)]
        scales = jnp.concatenate([own_share, shares[0]], axis=0)
        for p in range(pieces):
            first_out[p] = (down(hidden, p) * scales).astype(jnp.bfloat16)

        def hand_pair(p):
            return remote(
                first_out.at[p], own_pair.at[p], near_send.at[0], pair_recv, sibling
            )

        for p in range(pieces):
            hand_pair(p).start()

        @pl.when(is_inner)
        def _():
            for q in range(batches):
                with scope(f"w_P{q}"):
                    beside_came(q).wait()

        with scope("w_D"):
            whole(slots.at[3], rest_recv.at[0]).wait()
        hidden = hidden_of(2, False)
        scales = jnp.concatenate([shares[1], shares[2]], axis=0)
        for p in range(pieces):
            second_out[p] = (down(hidden, p) * scales).astype(jnp.bfloat16)

            along(p).start()
        whole(line_in, line_send).wait()

        @pl.when(is_outer)
        def _():
            whole(slots.at[1], spread_send.at[2]).wait()
            whole(slots.at[2], spread_send.at[3]).wait()

        whole(first_out, near_send.at[0]).wait()
        whole(second_out, near_send.at[1]).wait()
        for swap in swaps:
            swap.wait_send()
        with scope("w_give"):
            whole(out_ref, give_recv).wait()

    @pl.when(core == 1)
    def _():
        def near_x(q):
            return remote(
                own.at[rows_of(q), :], slots.at[1, rows_of(q), :], spread_send.at[5],
                spread_recv.at[0, q], on(across, 0),
            )

        def near_z(q):
            return remote(
                own.at[rows_of(q), :], slots.at[2, rows_of(q), :], spread_send.at[6],
                spread_recv.at[1, q], on(beside, 0),
            )

        def outward(q):
            return remote(
                own.at[rows_of(q), :], slots.at[my_far_slot, rows_of(q), :], spread_send.at[0],
                spread_recv.at[my_far_slot, q], far[0],
            )

        def arrived(s, q):
            return spread(1 + s, s, q, slots.at[s], beside, spread_recv.at[s, q])

        def sideways(s, q):
            return spread(3 + s, 2 + s, q, slots.at[s], across, rest_recv.at[s])

        def back_x(p):
            return remote(
                first_out.at[p], first_in.at[p], back_send.at[0], back_recv.at[0, p], across
            )

        def back_z(s, p):
            return remote(
                second_out.at[p, (lower, upper)[s], :],
                second_in.at[p, pl.ds(pl.multiple_of(my_far_slot * rows, rows), rows), :],
                back_send.at[1],
                back_recv.at[1 + my_far_slot, p],
                far[s],
            )

        def came_z(s, p):
            return whole(second_in.at[p, (lower, upper)[s], :], back_recv.at[1 + s, p])

        def cross(p):
            return remote(
                to_cross.at[p], from_across.at[p], near_send.at[2], near_recv.at[1, group(p)],
                across,
            )

        for q in range(batches):
            own[rows_of(q), :] = normed(q)
            if q == 0:
                with scope("w_bar"):
                    pl.semaphore_wait(barrier, len(far_peers) + 2)
            outward(q).start()
            near_x(q).start()
        for q in range(batches):
            near_z(q).start()
        for swap in swaps:
            swap.start()
        shares = [column(line_of(spot)) for spot in far_spots]
        for q in range(batches):
            for s in range(2):
                with scope(f"w_F{s}{q}"):
                    arrived(s, q).wait_recv()

                @pl.when(is_inner)
                def _():
                    arrived(s, q).start()

                sideways(s, q).start()
        hidden = hidden_of(0, True)
        for p in range(pieces):
            keep[p] = down(hidden, p)
        for s in range(2):
            with scope(f"w_G{s}"):
                whole(slots.at[2 + s], rest_recv.at[s]).wait()
        hidden = hidden_of(2, False)
        for p in range(pieces):
            first_out[p] = down(hidden, p).astype(jnp.bfloat16)
            back_x(p).start()

        span = pieces // groups
        for p in range(pieces):
            with scope(f"w_bx{p}"):
                back_x(p).wait_recv()
            second_out[p] = (keep[p] + first_in[p].astype(jnp.float32)).astype(jnp.bfloat16)
            for s in (1, 0):
                back_z(s, p).start()
            g = p - (pieces - groups)
            if g < 0:
                continue
            with scope(f"w_be{g}"):
                if g == 0:
                    whole(own_pair, pair_recv).wait()
                grouped(from_beside, 0, g).wait()
            for i in range(g * span, g * span + span):
                sums = own_pair[i, upper, :].astype(jnp.float32)
                sums = sums + from_beside[i, upper, :].astype(jnp.float32)
                to_cross[i] = sums.astype(jnp.bfloat16)
                cross(i).start()
        for p in range(pieces):
            if p % span == 0:
                with scope(f"w_xA{p}"):
                    grouped(from_across, 1, group(p)).wait()
            total = held[:, part(p)].astype(jnp.float32)
            total = total + own_pair[p, lower, :].astype(jnp.float32)
            total = total + from_beside[p, lower, :].astype(jnp.float32)
            total = total + from_across[p].astype(jnp.float32)
            for s in range(2):
                with scope(f"w_bz{s}{p}"):
                    came_z(s, p).wait()
                total = total + shares[s] * second_in[p, (lower, upper)[s], :].astype(jnp.float32)
            out_ref[:, part(p)] = total.astype(jnp.bfloat16)
            give(p).start()
        for lane in (0, 5, 6):
            whole(own, spread_send.at[lane]).wait()
        for s in range(2):
            whole(slots.at[s], spread_send.at[3 + s]).wait()
        whole(first_out, back_send.at[0]).wait()
        whole(second_out, back_send.at[1]).wait()
        whole(to_cross, near_send.at[2]).wait()

        @pl.when(is_inner)
        def _():
            for s in range(2):
                whole(slots.at[s], spread_send.at[1 + s]).wait()

        for swap in swaps:
            swap.wait_send()
        with scope("w_end"):
            whole(out_ref, give_send).wait()


def dense_layer(tokens, gain, route_ids, route_weights, w_gate, w_up, w_down):
    rows, features = tokens.shape
    units = 2 * w_gate.shape[2]
    batches = rows // 16
    pieces = 6
    width = features // pieces
    hbm = pl.BlockSpec(memory_space=pltpu.HBM)
    half = jnp.bfloat16
    dma = pltpu.SemaphoreType.DMA
    ids = route_ids.T
    weights = route_weights.T
    operands = (tokens, gain, ids, weights, w_gate, w_up, w_down)
    travel = pltpu.VMEM((pieces, 2 * rows, width), half)
    single = pltpu.VMEM((pieces, rows, width), half)
    return pl.pallas_call(
        dense_kernel,
        out_shape=pltpu.VMEM(tokens.shape, tokens.dtype),
        in_specs=[hbm] * 7,
        out_specs=pl.BlockSpec(memory_space=pltpu.VMEM),
        scratch_shapes=[
            pltpu.VMEM((rows, features), half),
            pltpu.VMEM((features,), jnp.float32),
            pltpu.VMEM(ids.shape, jnp.int32),
            pltpu.VMEM(weights.shape, jnp.float32),
            pltpu.VMEM((features, units), half),
            pltpu.VMEM((features, units), half),
            pltpu.VMEM((units, features), half),
            pltpu.VMEM((rows, features), half),
            pltpu.VMEM((4, rows, features), half),
            pltpu.VMEM((pieces, 2 * rows, width), jnp.float32),
        ]
        + [travel] * 6
        + [single] * 2
        + [
            pltpu.VMEM(weights.shape, jnp.float32),
            pltpu.VMEM((3, *weights.shape), jnp.float32),
            dma((4,)),
            dma((3,)),
            dma((3,)),
            dma((3,)),
            dma,
            dma,
            dma((7,)),
            dma((2, batches)),
            dma((2,)),
            dma((2,)),
            dma((3, pieces)),
            dma((3,)),
            dma,
            dma((2, 2)),
            dma,
            dma,
        ],
        compiler_params=pltpu.CompilerParams(
            collective_id=0, has_side_effects=True, vmem_limit_bytes=40_000_000
        ),
    )(*(pltpu.with_memory_space_constraint(array, pltpu.HBM) for array in operands))


def route_tables(chosen_ids, chosen_weights, expert_count, slot_room):
    row_count, top_count = chosen_ids.shape
    matches = (chosen_ids[:, :, None] == jnp.arange(expert_count, dtype=jnp.int32)).astype(
        jnp.float32
    )
    flat_match = matches.reshape(row_count * top_count, expert_count)
    order_range = jnp.arange(row_count * top_count, dtype=jnp.int32)
    earlier = (order_range[:, None] > order_range[None, :]).astype(jnp.float32)
    before = jnp.dot(
        earlier, flat_match, precision=lax.Precision.HIGHEST, preferred_element_type=jnp.float32
    )
    position = jnp.sum(before * flat_match, axis=1).reshape(row_count, top_count).astype(jnp.int32)
    slot_index = chosen_ids * slot_room + position
    targets = jnp.arange(expert_count * slot_room, dtype=jnp.int32)
    slot_hits = slot_index[None, :, :] == targets[:, None, None]
    send_table = jnp.sum(slot_hits.astype(jnp.float32), axis=2).astype(jnp.bfloat16)
    mix_table = jnp.sum(jnp.where(slot_hits, chosen_weights[None, :, :], 0.0), axis=2)
    return (send_table, mix_table)


def routed_layer(tokens, gain, route_ids, route_weights, w_gate, w_up, w_down):
    expert_axis = lax.axis_size("expert")
    expert_count = expert_axis // 2
    tensor_count = lax.axis_size("tensor")
    own_rows = tokens.shape[0] // tensor_count
    top_count = route_ids.shape[1]
    capacity = max(2, own_rows * top_count // expert_count)
    gate_local = w_gate[0]
    up_local = w_up[0]
    down_local = w_down[0]
    first_row = lax.axis_index("tensor") * own_rows
    own_tokens = lax.dynamic_slice_in_dim(tokens, first_row, own_rows, 0)
    own_ids = lax.dynamic_slice_in_dim(route_ids, first_row, own_rows, 0)
    own_weights = lax.dynamic_slice_in_dim(route_weights, first_row, own_rows, 0)
    resident = own_tokens.astype(jnp.float32)
    inv_rms = lax.rsqrt(jnp.mean(resident * resident, axis=1, keepdims=True) + 1e-05)
    normed = (resident * inv_rms * gain).astype(jnp.bfloat16)
    send_table, mix_table = route_tables(own_ids, own_weights, expert_count, capacity)
    packed = jnp.dot(send_table, normed, preferred_element_type=jnp.float32).astype(jnp.bfloat16)
    features = packed.shape[1]
    by_expert = packed.reshape(expert_count, 1, capacity, features)
    outgoing = jnp.broadcast_to(by_expert, (expert_count, 2, capacity, features)).reshape(
        expert_axis * capacity, features
    )
    arrived = lax.all_to_all(outgoing, "expert", split_axis=0, concat_axis=0, tiled=True)
    row_piece = lax.all_gather(arrived, "tensor", axis=0, tiled=True)
    gate_val = jnp.dot(row_piece, gate_local, preferred_element_type=jnp.float32)
    up_val = jnp.dot(row_piece, up_local, preferred_element_type=jnp.float32)
    hidden = gated_unit(gate_val, up_val).astype(jnp.bfloat16)
    partial_value = lax.psum_scatter(
        jnp.dot(hidden, down_local, preferred_element_type=jnp.float32),
        "tensor",
        scatter_dimension=0,
        tiled=True,
    )
    returned = lax.all_to_all(
        partial_value.astype(jnp.bfloat16), "expert", split_axis=0, concat_axis=0, tiled=True
    ).astype(partial_value.dtype)
    expert_out = (
        returned.reshape(expert_count, 2, capacity, features)
        .sum(axis=1)
        .reshape(expert_count * capacity, features)
    )
    weighted = jnp.dot(
        mix_table.T, expert_out, precision=lax.Precision.HIGHEST, preferred_element_type=jnp.float32
    )
    finished = (resident + weighted).astype(jnp.bfloat16)
    return lax.all_gather(finished, "tensor", axis=0, tiled=True)


def per_device(tokens, gain, route_ids, route_weights, w_gate, w_up, w_down):
    experts = lax.axis_size("expert") // 2
    dense = (
        route_ids.shape[1] == experts
        and experts == 4
        and lax.axis_size("tensor") == 2
        and w_gate.shape[0] == 1
    )
    layer = dense_layer if dense else routed_layer
    return layer(tokens, gain, route_ids, route_weights, w_gate, w_up, w_down)


def solution(mesh):
    placed = (
        P(("groups", "expert"), None),
        P(),
        P(("groups", "expert"), None),
        P(("groups", "expert"), None),
        P("expert", None, "tensor"),
        P("expert", None, "tensor"),
        P("expert", "tensor", None),
    )
    return jax.shard_map(
        per_device,
        mesh=mesh,
        in_specs=placed,
        out_specs=P(("groups", "expert"), None),
        check_vma=False,
    )
```

```python
import functools

import jax
import jax.numpy as jnp
from jax import lax
from jax.experimental import pallas as pl
from jax.experimental.pallas import tpu as pltpu
from jax.sharding import PartitionSpec as P

MESH = pl.DeviceIdType.MESH


def gated_unit(gate_val, up_val):
    return gate_val * jax.nn.sigmoid(1.702 * gate_val) * (up_val + 1.0)


def dense_kernel(
    tokens_ref,
    gain_ref,
    ids_ref,
    weights_ref,
    gate_ref,
    up_ref,
    down_ref,
    out_ref,
    held,
    gain,
    ids,
    weights,
    wg,
    wu,
    wd,
    own,
    slots,
    keep,
    first_out,
    first_in,
    second_out,
    second_in,
    own_pair,
    from_beside,
    from_across,
    to_cross,
    line_out,
    line_in,
    small_sem,
    load_sem,
    swap_recv,
    sent,
    spread_recv,
    rest_recv,
    done_recv,
    near_recv,
    pair_recv,
):
    me = lax.axis_index("expert")
    core = lax.axis_index("tensor")
    place = me // 2
    side = lax.rem(me, 2)
    half = place // 2
    inner = lax.rem(place + half, 2)
    is_inner = inner == 1
    is_outer = inner == 0

    def at(where, which):
        return {"expert": where * 2 + which}

    pair = place + 1 - 2 * lax.rem(place, 2)
    far_inner = 2 - half
    far_outer = 3 - 3 * half
    across = at(place, 1 - side)
    beside = at(pair, side)
    corner = at(pair, 1 - side)
    sibling = {"tensor": 1 - core}
    far_spots = (far_inner, far_outer)
    far = [at(spot, side) for spot in far_spots]
    my_far_slot = 1 - inner

    rows, features = own.shape
    cols = gate_ref.shape[2]
    batches = rows // 16
    groups = near_recv.shape[1]
    batch = rows // batches
    pieces, _, width = keep.shape
    scope = jax.named_scope

    barrier = pltpu.get_barrier_semaphore()

    def greet(peers):
        for peer in peers:
            pl.semaphore_signal(barrier, inc=1, device_id=peer, device_id_type=MESH)

    def on(peer, which):
        return {**peer, "tensor": which}

    near_peers = [across, beside, corner, sibling]
    far_peers = [across, beside, far[0], sibling]

    @pl.when(core == 0)
    def _():
        greet([*near_peers, on(across, 1), on(beside, 1)])

    @pl.when(core == 1)
    def _():
        greet([across, beside, sibling, on(across, 0), on(beside, 0)])

        @pl.when(is_inner)
        def _():
            greet(far)

    smalls = [
        pltpu.make_async_copy(src, dst, small_sem.at[i])
        for i, (src, dst) in enumerate(
            (
                (tokens_ref, held),
                (gain_ref, gain),
                (ids_ref, ids),
                (weights_ref, weights),
            )
        )
    ]
    for small in smalls:
        small.start()

    pairs = (
        (gate_ref.at[0], lambda part: wg.at[:, pl.ds(part * cols, cols)]),
        (up_ref.at[0], lambda part: wu.at[:, pl.ds(part * cols, cols)]),
        (down_ref.at[0], lambda part: wd.at[pl.ds(part * cols, cols), :]),
    )
    loads = [
        pltpu.make_async_copy(src, dst(0), load_sem.at[i]) for i, (src, dst) in enumerate(pairs)
    ]
    for load in loads:
        load.start()

    def remote(src, dst, send, recv, peer):
        return pltpu.make_async_remote_copy(
            src_ref=src, dst_ref=dst, send_sem=send, recv_sem=recv, device_id=peer,
            device_id_type=MESH,
        )

    swaps = [
        remote(src, dst(1), sent.at[3 + i // 2], swap_recv.at[i], sibling)
        for i, (src, dst) in enumerate(pairs)
    ]

    def rows_of(q):
        return pl.ds(q * batch, batch)

    def part(p):
        return pl.ds(p * width, width)

    with scope("w_small"):
        smalls[0].wait()
        smalls[1].wait()

    def normed():
        resident = held[...].astype(jnp.float32)
        inv_rms = lax.rsqrt(jnp.mean(resident * resident, axis=1, keepdims=True) + 1e-05)
        return (resident * inv_rms * gain[...].reshape(1, -1)).astype(jnp.bfloat16)

    lanes = line_out.shape[1]
    spots = line_out.shape[0]
    spot_ids = lax.broadcasted_iota(jnp.int32, (rows, rows), 0)
    lane_ids = lax.broadcasted_iota(jnp.int32, (rows, rows), 1)

    def line_of(spot):
        named = jnp.where(ids[...] == spot, weights[...], 0.0)
        return jnp.sum(named, axis=0, keepdims=True)

    def column(line):
        return jnp.sum(jnp.where(spot_ids == lane_ids, line, 0.0), axis=1, keepdims=True)

    def ready(i):
        loads[i].wait()
        swaps[i].wait_recv()

    def hidden_of(first, fresh):
        block = slots[pl.ds(first, 2)].reshape(2 * rows, features)
        if fresh:
            with scope("w_wg"):
                ready(0)
        gate_val = jnp.dot(block, wg[...], preferred_element_type=jnp.float32)
        if fresh:
            with scope("w_wu"):
                ready(1)
        up_val = jnp.dot(block, wu[...], preferred_element_type=jnp.float32)
        value = gated_unit(gate_val, up_val).astype(jnp.bfloat16)
        if fresh:
            with scope("w_wd"):
                ready(2)
        return value

    def down(hidden, p):
        return jnp.dot(hidden, wd[:, part(p)], preferred_element_type=jnp.float32)

    def give(p):
        there = out_ref.at[:, part(p)]
        return remote(there, there, sent.at[5], done_recv.at[1], sibling)

    def whole(ref, sem):
        return pltpu.make_async_copy(ref, ref, sem)

    def spread(slot, q, src, peer, recv):
        return remote(
            src.at[rows_of(q), :], slots.at[slot, rows_of(q), :], sent.at[0], recv, peer
        )

    def blocks_sent(count):
        whole(wd.at[pl.ds(0, count * rows), :], sent.at[0]).wait()

    def swaps_sent():
        whole(wg, sent.at[3]).wait()
        swaps[2].wait_send()

    def group(p):
        return p * groups // pieces

    def grouped(ref, i, g):
        span = pieces // groups
        return whole(ref.at[pl.ds(g * span, span)], near_recv.at[i, g])

    lower, upper = pl.ds(0, rows), pl.ds(rows, rows)
    both_halves = pl.ds(0, 2 * rows)

    @pl.when(core == 0)
    def _():
        def across_came(q):
            return whole(slots.at[1, rows_of(q), :], spread_recv.at[0, q])

        def beside_came(q):
            return whole(slots.at[2, rows_of(q), :], spread_recv.at[1, q])

        def on_to_beside(q):
            return spread(3, q, slots.at[1], beside, rest_recv)

        def on_to_across(q):
            return spread(3, q, slots.at[2], across, rest_recv)

        def along(p):
            return remote(
                second_out.at[p], from_beside.at[p], sent.at[2], near_recv.at[0, group(p)],
                on(beside, 1),
            )

        def line_to(i):
            return remote(
                line_out, line_in.at[i], sent.at[5], done_recv.at[0],
                (across, beside, corner)[i],
            )

        slots[0] = normed()
        smalls[2].wait()
        smalls[3].wait()
        for spot in range(spots):
            line_out[spot : spot + 1, :] = line_of(spot)
        with scope("w_bar"):
            pl.semaphore_wait(barrier, len(near_peers) + 2)
        for i in range(3):
            line_to(i).start()
        for swap in swaps:
            swap.start()
        for q in range(batches):
            with scope(f"w_A{q}"):
                across_came(q).wait()

            @pl.when(is_outer)
            def _():
                on_to_beside(q).start()
                with scope(f"w_Po{q}"):
                    beside_came(q).wait()
                on_to_across(q).start()

        def share(table):
            own_line = jnp.sum(
                jnp.where(
                    lax.broadcasted_iota(jnp.int32, (spots, lanes), 0) == place, table, 0.0
                ),
                axis=0,
                keepdims=True,
            )
            return column(own_line)

        hidden = hidden_of(0, True)
        with scope("w_line"):
            whole(line_in, done_recv.at[0]).wait()
        own_share = share(line_out[...])
        shares = [share(line_in[i]) for i in range(3)]
        scales = jnp.concatenate([own_share, shares[0]], axis=0)
        for p in range(pieces):
            first_out[p] = (down(hidden, p) * scales).astype(jnp.bfloat16)

        def hand_pair(p):
            return remote(
                first_out.at[p], own_pair.at[p], sent.at[1], pair_recv, sibling
            )

        for p in range(pieces):
            hand_pair(p).start()

        @pl.when(is_inner)
        def _():
            for q in range(batches):
                with scope(f"w_P{q}"):
                    beside_came(q).wait()

        with scope("w_D"):
            whole(slots.at[3], rest_recv).wait()
        hidden = hidden_of(2, False)
        scales = jnp.concatenate([shares[1], shares[2]], axis=0)
        for p in range(pieces):
            second_out[p] = (down(hidden, p) * scales).astype(jnp.bfloat16)

            along(p).start()
        whole(line_in, sent.at[5]).wait()

        @pl.when(is_outer)
        def _():
            blocks_sent(2)

        whole(first_out, sent.at[1]).wait()
        whole(second_out, sent.at[2]).wait()
        swaps_sent()
        with scope("w_give"):
            whole(out_ref, done_recv.at[1]).wait()

    @pl.when(core == 1)
    def _():
        def near_x(q):
            return remote(
                own.at[rows_of(q), :], slots.at[1, rows_of(q), :], sent.at[0],
                spread_recv.at[0, q], on(across, 0),
            )

        def near_z(q):
            return remote(
                own.at[rows_of(q), :], slots.at[2, rows_of(q), :], sent.at[0],
                spread_recv.at[1, q], on(beside, 0),
            )

        def outward(q):
            return remote(
                own.at[rows_of(q), :], slots.at[my_far_slot, rows_of(q), :], sent.at[0],
                spread_recv.at[my_far_slot, q], far[0],
            )

        def arrived(s, q):
            return spread(s, q, slots.at[s], beside, spread_recv.at[s, q])

        def sideways(s, q):
            return spread(2 + s, q, slots.at[s], across, rest_recv)

        def back_x(s, p):
            rows_there = (lower, upper)[s]
            return remote(
                first_out.at[p, rows_there, :], first_in.at[p, rows_there, :], sent.at[1],
                spread_recv.at[s, p], across,
            )

        def back_z(s, p):
            return remote(
                second_out.at[p, (lower, upper)[s], :],
                second_in.at[p, pl.ds(pl.multiple_of(my_far_slot * rows, rows), rows), :],
                sent.at[1],
                done_recv.at[p],
                far[s],
            )

        def came_z(p):
            return whole(second_in.at[p], done_recv.at[p])

        def cross(p):
            return remote(
                to_cross.at[p], from_across.at[p], sent.at[2], near_recv.at[1, group(p)],
                across,
            )

        own[...] = normed()
        with scope("w_bar"):
            pl.semaphore_wait(barrier, len(far_peers) + 2)
        for q in range(batches):
            outward(q).start()
        for q in range(batches):
            near_x(q).start()
        for q in range(batches):
            near_z(q).start()
        for swap in swaps:
            swap.start()
        smalls[2].wait()
        smalls[3].wait()
        shares = [column(line_of(spot)) for spot in far_spots]
        order = [(0, 0)] + [(1, q) for q in range(batches)] + [(0, q) for q in range(1, batches)]
        for s, q in order:
            with scope(f"w_F{s}{q}"):
                arrived(s, q).wait_recv()

            @pl.when(is_inner)
            def _():
                arrived(s, q).start()

            sideways(s, q).start()
        hidden = hidden_of(0, True)
        for p in range(pieces):
            keep[p] = down(hidden, p)
        with scope("w_G"):
            whole(slots.at[pl.ds(2, 2)], rest_recv).wait()
        hidden = hidden_of(2, False)
        for p in range(pieces):
            first_out[p] = down(hidden, p).astype(jnp.bfloat16)
            for s in (1, 0):
                back_x(s, p).start()

        span = pieces // groups

        def merge(g):
            with scope(f"w_be{g}"):
                if g == 0:
                    whole(own_pair, pair_recv).wait()
                grouped(from_beside, 0, g).wait()
            for i in range(g * span, g * span + span):
                sums = own_pair[i, upper, :].astype(jnp.float32)
                sums = sums + from_beside[i, upper, :].astype(jnp.float32)
                to_cross[i] = sums.astype(jnp.bfloat16)
                cross(i).start()

        for p in range(pieces):
            for s in (1, 0):
                there = (lower, upper)[s]
                with scope(f"w_bx{s}{p}"):
                    back_x(s, p).wait_recv()
                both = keep[p, there, :] + first_in[p, there, :].astype(jnp.float32)
                second_out[p, there, :] = both.astype(jnp.bfloat16)
                back_z(s, p).start()
            for g in range(groups):
                if p == pieces - groups + g:
                    pl.when(is_inner)(functools.partial(merge, g))
                if p == 1 + 2 * g:
                    pl.when(is_outer)(functools.partial(merge, g))
        for p in range(pieces):
            if p % span == 0:
                with scope(f"w_xA{p}"):
                    grouped(from_across, 1, group(p)).wait()
            total = held[:, part(p)].astype(jnp.float32)
            total = total + own_pair[p, lower, :].astype(jnp.float32)
            total = total + from_beside[p, lower, :].astype(jnp.float32)
            total = total + from_across[p].astype(jnp.float32)
            with scope(f"w_bz{p}"):
                came_z(p).wait()
            for s in range(2):
                total = total + shares[s] * second_in[p, (lower, upper)[s], :].astype(jnp.float32)
            out_ref[:, part(p)] = total.astype(jnp.bfloat16)
            give(p).start()
        whole(keep, sent.at[1]).wait()
        whole(to_cross, sent.at[2]).wait()

        @pl.when(is_inner)
        def _():
            blocks_sent(7)

        @pl.when(is_outer)
        def _():
            blocks_sent(5)

        swaps_sent()
        with scope("w_end"):
            whole(out_ref, sent.at[5]).wait()


def dense_layer(tokens, gain, route_ids, route_weights, w_gate, w_up, w_down):
    rows, features = tokens.shape
    units = 2 * w_gate.shape[2]
    batches = rows // 16
    pieces = 6
    width = features // pieces
    hbm = pl.BlockSpec(memory_space=pltpu.HBM)
    half = jnp.bfloat16
    dma = pltpu.SemaphoreType.DMA
    ids = route_ids.T
    weights = route_weights.T
    operands = (tokens, gain, ids, weights, w_gate, w_up, w_down)
    travel = pltpu.VMEM((pieces, 2 * rows, width), half)
    single = pltpu.VMEM((pieces, rows, width), half)
    return pl.pallas_call(
        dense_kernel,
        out_shape=pltpu.VMEM(tokens.shape, tokens.dtype),
        in_specs=[hbm] * 7,
        out_specs=pl.BlockSpec(memory_space=pltpu.VMEM),
        scratch_shapes=[
            pltpu.VMEM((rows, features), half),
            pltpu.VMEM((features,), jnp.float32),
            pltpu.VMEM(ids.shape, jnp.int32),
            pltpu.VMEM(weights.shape, jnp.float32),
            pltpu.VMEM((features, units), half),
            pltpu.VMEM((features, units), half),
            pltpu.VMEM((units, features), half),
            pltpu.VMEM((rows, features), half),
            pltpu.VMEM((4, rows, features), half),
            pltpu.VMEM((pieces, 2 * rows, width), jnp.float32),
        ]
        + [travel] * 6
        + [single] * 2
        + [
            pltpu.VMEM(weights.shape, jnp.float32),
            pltpu.VMEM((3, *weights.shape), jnp.float32),
            dma((4,)),
            dma((3,)),
            dma((3,)),
            dma((6,)),
            dma((2, max(batches, pieces))),
            dma,
            dma((pieces,)),
            dma((2, 2)),
            dma,
        ],
        compiler_params=pltpu.CompilerParams(
            collective_id=0, has_side_effects=True, vmem_limit_bytes=40_000_000
        ),
    )(*(pltpu.with_memory_space_constraint(array, pltpu.HBM) for array in operands))


def route_tables(chosen_ids, chosen_weights, expert_count, slot_room):
    row_count, top_count = chosen_ids.shape
    matches = (chosen_ids[:, :, None] == jnp.arange(expert_count, dtype=jnp.int32)).astype(
        jnp.float32
    )
    flat_match = matches.reshape(row_count * top_count, expert_count)
    order_range = jnp.arange(row_count * top_count, dtype=jnp.int32)
    earlier = (order_range[:, None] > order_range[None, :]).astype(jnp.float32)
    before = jnp.dot(
        earlier, flat_match, precision=lax.Precision.HIGHEST, preferred_element_type=jnp.float32
    )
    position = jnp.sum(before * flat_match, axis=1).reshape(row_count, top_count).astype(jnp.int32)
    slot_index = chosen_ids * slot_room + position
    targets = jnp.arange(expert_count * slot_room, dtype=jnp.int32)
    slot_hits = slot_index[None, :, :] == targets[:, None, None]
    send_table = jnp.sum(slot_hits.astype(jnp.float32), axis=2).astype(jnp.bfloat16)
    mix_table = jnp.sum(jnp.where(slot_hits, chosen_weights[None, :, :], 0.0), axis=2)
    return (send_table, mix_table)


def routed_layer(tokens, gain, route_ids, route_weights, w_gate, w_up, w_down):
    expert_axis = lax.axis_size("expert")
    expert_count = expert_axis // 2
    tensor_count = lax.axis_size("tensor")
    own_rows = tokens.shape[0] // tensor_count
    top_count = route_ids.shape[1]
    capacity = max(2, own_rows * top_count // expert_count)
    gate_local = w_gate[0]
    up_local = w_up[0]
    down_local = w_down[0]
    first_row = lax.axis_index("tensor") * own_rows
    own_tokens = lax.dynamic_slice_in_dim(tokens, first_row, own_rows, 0)
    own_ids = lax.dynamic_slice_in_dim(route_ids, first_row, own_rows, 0)
    own_weights = lax.dynamic_slice_in_dim(route_weights, first_row, own_rows, 0)
    resident = own_tokens.astype(jnp.float32)
    inv_rms = lax.rsqrt(jnp.mean(resident * resident, axis=1, keepdims=True) + 1e-05)
    normed = (resident * inv_rms * gain).astype(jnp.bfloat16)
    send_table, mix_table = route_tables(own_ids, own_weights, expert_count, capacity)
    packed = jnp.dot(send_table, normed, preferred_element_type=jnp.float32).astype(jnp.bfloat16)
    features = packed.shape[1]
    by_expert = packed.reshape(expert_count, 1, capacity, features)
    outgoing = jnp.broadcast_to(by_expert, (expert_count, 2, capacity, features)).reshape(
        expert_axis * capacity, features
    )
    arrived = lax.all_to_all(outgoing, "expert", split_axis=0, concat_axis=0, tiled=True)
    row_piece = lax.all_gather(arrived, "tensor", axis=0, tiled=True)
    gate_val = jnp.dot(row_piece, gate_local, preferred_element_type=jnp.float32)
    up_val = jnp.dot(row_piece, up_local, preferred_element_type=jnp.float32)
    hidden = gated_unit(gate_val, up_val).astype(jnp.bfloat16)
    partial_value = lax.psum_scatter(
        jnp.dot(hidden, down_local, preferred_element_type=jnp.float32),
        "tensor",
        scatter_dimension=0,
        tiled=True,
    )
    returned = lax.all_to_all(
        partial_value.astype(jnp.bfloat16), "expert", split_axis=0, concat_axis=0, tiled=True
    ).astype(partial_value.dtype)
    expert_out = (
        returned.reshape(expert_count, 2, capacity, features)
        .sum(axis=1)
        .reshape(expert_count * capacity, features)
    )
    weighted = jnp.dot(
        mix_table.T, expert_out, precision=lax.Precision.HIGHEST, preferred_element_type=jnp.float32
    )
    finished = (resident + weighted).astype(jnp.bfloat16)
    return lax.all_gather(finished, "tensor", axis=0, tiled=True)


def per_device(tokens, gain, route_ids, route_weights, w_gate, w_up, w_down):
    experts = lax.axis_size("expert") // 2
    dense = (
        route_ids.shape[1] == experts
        and experts == 4
        and lax.axis_size("tensor") == 2
        and w_gate.shape[0] == 1
    )
    layer = dense_layer if dense else routed_layer
    return layer(tokens, gain, route_ids, route_weights, w_gate, w_up, w_down)


def solution(mesh):
    placed = (
        P(("groups", "expert"), None),
        P(),
        P(("groups", "expert"), None),
        P(("groups", "expert"), None),
        P("expert", None, "tensor"),
        P("expert", None, "tensor"),
        P("expert", "tensor", None),
    )
    return jax.shard_map(
        per_device,
        mesh=mesh,
        in_specs=placed,
        out_specs=P(("groups", "expert"), None),
        check_vma=False,
    )
```

```python
import functools

import jax
import jax.numpy as jnp
from jax import lax
from jax.experimental import pallas as pl
from jax.experimental.pallas import tpu as pltpu
from jax.sharding import PartitionSpec as P

MESH = pl.DeviceIdType.MESH


def gated_unit(gate_val, up_val):
    return gate_val * jax.nn.sigmoid(1.702 * gate_val) * (up_val + 1.0)


def dense_kernel(
    tokens_ref,
    gain_ref,
    ids_ref,
    weights_ref,
    gate_ref,
    up_ref,
    down_ref,
    out_ref,
    held,
    gain,
    ids,
    weights,
    wg,
    wu,
    wd,
    own,
    slots,
    keep,
    first_out,
    first_in,
    second_out,
    second_in,
    own_pair,
    from_beside,
    from_across,
    to_cross,
    line_out,
    line_in,
    small_sem,
    load_sem,
    swap_recv,
    sent,
    spread_recv,
    rest_recv,
    done_recv,
    near_recv,
    pair_recv,
):
    me = lax.axis_index("expert")
    core = lax.axis_index("tensor")
    place = me // 2
    side = lax.rem(me, 2)
    half = place // 2
    inner = lax.rem(place + half, 2)
    is_inner = inner == 1
    is_outer = inner == 0

    def at(where, which):
        return {"expert": where * 2 + which}

    pair = place + 1 - 2 * lax.rem(place, 2)
    far_inner = 2 - half
    far_outer = 3 - 3 * half
    across = at(place, 1 - side)
    beside = at(pair, side)
    corner = at(pair, 1 - side)
    sibling = {"tensor": 1 - core}
    far_spots = (far_inner, far_outer)
    far = [at(spot, side) for spot in far_spots]
    my_far_slot = 1 - inner

    rows, features = own.shape
    cols = gate_ref.shape[2]
    batches = rows // 16
    groups = near_recv.shape[1]
    batch = rows // batches
    pieces, _, width = keep.shape
    scope = jax.named_scope

    barrier = pltpu.get_barrier_semaphore()

    def greet(peers):
        for peer in peers:
            pl.semaphore_signal(barrier, inc=1, device_id=peer, device_id_type=MESH)

    def on(peer, which):
        return {**peer, "tensor": which}

    near_peers = [across, beside, corner, sibling]
    far_peers = [across, beside, far[0], sibling]

    @pl.when(core == 0)
    def _():
        greet([*near_peers, on(across, 1), on(beside, 1)])

    @pl.when(core == 1)
    def _():
        greet([across, beside, sibling, on(across, 0), on(beside, 0)])

        @pl.when(is_inner)
        def _():
            greet(far)

    smalls = [
        pltpu.make_async_copy(src, dst, small_sem.at[i])
        for i, (src, dst) in enumerate(
            (
                (tokens_ref, held),
                (gain_ref, gain),
                (ids_ref, ids),
                (weights_ref, weights),
            )
        )
    ]
    for small in smalls:
        small.start()

    pairs = (
        (gate_ref.at[0], lambda part: wg.at[:, pl.ds(part * cols, cols)]),
        (up_ref.at[0], lambda part: wu.at[:, pl.ds(part * cols, cols)]),
        (down_ref.at[0], lambda part: wd.at[pl.ds(part * cols, cols), :]),
    )
    loads = [
        pltpu.make_async_copy(src, dst(0), load_sem.at[i]) for i, (src, dst) in enumerate(pairs)
    ]
    for load in loads:
        load.start()

    def remote(src, dst, send, recv, peer):
        return pltpu.make_async_remote_copy(
            src_ref=src, dst_ref=dst, send_sem=send, recv_sem=recv, device_id=peer,
            device_id_type=MESH,
        )

    swaps = [
        remote(src, dst(1), sent.at[3 + i // 2], swap_recv.at[i], sibling)
        for i, (src, dst) in enumerate(pairs)
    ]

    def rows_of(q):
        return pl.ds(q * batch, batch)

    def part(p):
        return pl.ds(p * width, width)

    with scope("w_small"):
        smalls[0].wait()
        smalls[1].wait()

    def normed():
        resident = held[...].astype(jnp.float32)
        inv_rms = lax.rsqrt(jnp.mean(resident * resident, axis=1, keepdims=True) + 1e-05)
        return (resident * inv_rms * gain[...].reshape(1, -1)).astype(jnp.bfloat16)

    lanes = line_out.shape[1]
    spots = line_out.shape[0]
    spot_ids = lax.broadcasted_iota(jnp.int32, (rows, rows), 0)
    lane_ids = lax.broadcasted_iota(jnp.int32, (rows, rows), 1)

    def line_of(spot):
        named = jnp.where(ids[...] == spot, weights[...], 0.0)
        return jnp.sum(named, axis=0, keepdims=True)

    def column(line):
        return jnp.sum(jnp.where(spot_ids == lane_ids, line, 0.0), axis=1, keepdims=True)

    def ready(i):
        loads[i].wait()
        swaps[i].wait_recv()

    def hidden_of(first, count, fresh):
        block = slots[pl.ds(first, count)].reshape(count * rows, features)
        if fresh:
            with scope("w_wg"):
                ready(0)
        gate_val = jnp.dot(block, wg[...], preferred_element_type=jnp.float32)
        if fresh:
            with scope("w_wu"):
                ready(1)
        up_val = jnp.dot(block, wu[...], preferred_element_type=jnp.float32)
        value = gated_unit(gate_val, up_val).astype(jnp.bfloat16)
        if fresh:
            with scope("w_wd"):
                ready(2)
        return value

    def down(hidden, p):
        return jnp.dot(hidden, wd[:, part(p)], preferred_element_type=jnp.float32)

    def give(p):
        there = out_ref.at[:, part(p)]
        return remote(there, there, sent.at[5], done_recv.at[1], sibling)

    def whole(ref, sem):
        return pltpu.make_async_copy(ref, ref, sem)

    def spread(slot, q, src, peer, recv):
        return remote(
            src.at[rows_of(q), :], slots.at[slot, rows_of(q), :], sent.at[0], recv, peer
        )

    def blocks_sent(count):
        whole(wd.at[pl.ds(0, count * rows), :], sent.at[0]).wait()

    def swaps_sent():
        whole(wg, sent.at[3]).wait()
        swaps[2].wait_send()

    def group(p):
        return p * groups // pieces

    def grouped(ref, i, g):
        span = pieces // groups
        return whole(ref.at[pl.ds(g * span, span)], near_recv.at[i, g])

    batched = (range(1), range(1, pieces // 2), range(pieces // 2, pieces))
    lower, upper = pl.ds(0, rows), pl.ds(rows, rows)

    @pl.when(core == 0)
    def _():
        def across_came(q):
            return whole(slots.at[1, rows_of(q), :], spread_recv.at[0, q])

        def beside_came(q):
            return whole(slots.at[2, rows_of(q), :], spread_recv.at[1, q])

        def on_to_beside(q):
            return spread(3, q, slots.at[1], beside, rest_recv.at[0])

        def on_to_across(q):
            return spread(3, q, slots.at[2], across, rest_recv.at[0])

        def along(p, half, recv):
            return remote(
                second_out.at[p, half, :], from_beside.at[p, half, :], sent.at[2], recv,
                on(beside, 1),
            )

        def line_to(i):
            return remote(
                line_out, line_in.at[i], sent.at[5], done_recv.at[0],
                (across, beside, corner)[i],
            )

        slots[0] = normed()
        smalls[2].wait()
        smalls[3].wait()
        for spot in range(spots):
            line_out[spot : spot + 1, :] = line_of(spot)
        with scope("w_bar"):
            pl.semaphore_wait(barrier, len(near_peers) + 2)
        for i in range(3):
            line_to(i).start()
        for swap in swaps:
            swap.start()
        for q in range(batches):
            with scope(f"w_A{q}"):
                across_came(q).wait()

            @pl.when(is_outer)
            def _():
                on_to_beside(q).start()
                with scope(f"w_Po{q}"):
                    beside_came(q).wait()
                on_to_across(q).start()

        def share(table):
            own_line = jnp.sum(
                jnp.where(
                    lax.broadcasted_iota(jnp.int32, (spots, lanes), 0) == place, table, 0.0
                ),
                axis=0,
                keepdims=True,
            )
            return column(own_line)

        hidden = hidden_of(0, 2, True)
        with scope("w_line"):
            whole(line_in, done_recv.at[0]).wait()
        own_share = share(line_out[...])
        shares = [share(line_in[i]) for i in range(3)]
        scales = jnp.concatenate([own_share, shares[0]], axis=0)
        for p in range(pieces):
            first_out[p] = (down(hidden, p) * scales).astype(jnp.bfloat16)

        def hand_pair(p):
            return remote(
                first_out.at[p], own_pair.at[p], sent.at[1], pair_recv, sibling
            )

        for p in range(pieces):
            hand_pair(p).start()

        @pl.when(is_inner)
        def _():
            for q in range(batches):
                with scope(f"w_P{q}"):
                    beside_came(q).wait()

        with scope("w_D"):
            whole(slots.at[3], rest_recv.at[0]).wait()
        hidden = hidden_of(2, 2, False)
        scales = jnp.concatenate([shares[1], shares[2]], axis=0)
        for batch_of in batched:
            for p in batch_of:
                second_out[p] = (down(hidden, p) * scales).astype(jnp.bfloat16)
            for p in batch_of:
                along(p, upper, near_recv.at[0, group(p)]).start()
        for p in range(pieces):
            along(p, lower, near_recv.at[2, 0]).start()
        whole(line_in, sent.at[5]).wait()

        @pl.when(is_outer)
        def _():
            blocks_sent(2)

        whole(first_out, sent.at[1]).wait()
        whole(second_out, sent.at[2]).wait()
        swaps_sent()
        with scope("w_give"):
            whole(out_ref, done_recv.at[1]).wait()

    @pl.when(core == 1)
    def _():
        def near_x(q):
            return remote(
                own.at[rows_of(q), :], slots.at[1, rows_of(q), :], sent.at[0],
                spread_recv.at[0, q], on(across, 0),
            )

        def near_z(q):
            return remote(
                own.at[rows_of(q), :], slots.at[2, rows_of(q), :], sent.at[0],
                spread_recv.at[1, q], on(beside, 0),
            )

        def outward(q):
            return remote(
                own.at[rows_of(q), :], slots.at[my_far_slot, rows_of(q), :], sent.at[0],
                spread_recv.at[my_far_slot, q], far[0],
            )

        def arrived(s, q):
            return spread(s, q, slots.at[s], beside, spread_recv.at[s, q])

        def sideways(s, q):
            return spread(3 - s, q, slots.at[s], across, rest_recv.at[s])

        def back_x(s, p):
            rows_there = (lower, upper)[s]
            return remote(
                first_out.at[p, rows_there, :], first_in.at[p, rows_there, :], sent.at[1],
                spread_recv.at[s, p], across,
            )

        def back_z(s, p):
            return remote(
                second_out.at[p, (lower, upper)[s], :],
                second_in.at[p, pl.ds(pl.multiple_of(my_far_slot * rows, rows), rows), :],
                sent.at[1],
                done_recv.at[p],
                far[s],
            )

        def came_z(p):
            return whole(second_in.at[p], done_recv.at[p])

        def cross(p):
            return remote(
                to_cross.at[p], from_across.at[p], sent.at[2], near_recv.at[1, group(p)],
                across,
            )

        own[...] = normed()
        with scope("w_bar"):
            pl.semaphore_wait(barrier, len(far_peers) + 2)
        for q in range(batches):
            outward(q).start()
        for q in range(batches):
            near_x(q).start()
        for q in range(batches):
            near_z(q).start()
        for swap in swaps:
            swap.start()
        smalls[2].wait()
        smalls[3].wait()
        shares = [column(line_of(spot)) for spot in far_spots]
        for s, q in [(1, q) for q in range(batches)] + [(0, q) for q in range(batches)]:
            with scope(f"w_F{s}{q}"):
                arrived(s, q).wait_recv()

            @pl.when(is_inner)
            def _():
                arrived(s, q).start()

            sideways(s, q).start()
        with scope("w_G1"):
            whole(slots.at[2], rest_recv.at[1]).wait()
        hidden = hidden_of(0, 3, True)
        for batch_of in batched:
            for p in batch_of:
                first_out[p, upper, :] = down(hidden[2 * rows :], p).astype(jnp.bfloat16)
            for p in batch_of:
                back_x(1, p).start()
        with scope("w_G0"):
            whole(slots.at[3], rest_recv.at[0]).wait()
        late_hidden = hidden_of(3, 1, False)
        for batch_of in batched:
            for p in batch_of:
                first_out[p, lower, :] = down(late_hidden, p).astype(jnp.bfloat16)
            for p in batch_of:
                back_x(0, p).start()
        for p in range(pieces):
            keep[p] = down(hidden[: 2 * rows], p)
        span = pieces // groups

        def merge(g):
            with scope(f"w_be{g}"):
                if g == 0:
                    whole(own_pair, pair_recv).wait()
                grouped(from_beside.at[:, upper, :], 0, g).wait()
            for i in range(g * span, g * span + span):
                sums = own_pair[i, upper, :].astype(jnp.float32)
                sums = sums + from_beside[i, upper, :].astype(jnp.float32)
                to_cross[i] = sums.astype(jnp.bfloat16)
                cross(i).start()

        for s in (1, 0):
            there = (lower, upper)[s]
            for p in range(pieces):
                with scope(f"w_bx{s}{p}"):
                    back_x(s, p).wait_recv()
                both = keep[p, there, :] + first_in[p, there, :].astype(jnp.float32)
                second_out[p, there, :] = both.astype(jnp.bfloat16)
                back_z(s, p).start()
            if s == 1:
                for g in range(groups):
                    merge(g)
        with scope("w_low"):
            whole(from_beside.at[:, lower, :], near_recv.at[2, 0]).wait()
        for p in range(pieces):
            if p % span == 0:
                with scope(f"w_xA{p}"):
                    grouped(from_across, 1, group(p)).wait()
            total = held[:, part(p)].astype(jnp.float32)
            total = total + own_pair[p, lower, :].astype(jnp.float32)
            total = total + from_beside[p, lower, :].astype(jnp.float32)
            total = total + from_across[p].astype(jnp.float32)
            with scope(f"w_bz{p}"):
                came_z(p).wait()
            for s in range(2):
                total = total + shares[s] * second_in[p, (lower, upper)[s], :].astype(jnp.float32)
            out_ref[:, part(p)] = total.astype(jnp.bfloat16)
            give(p).start()
        whole(keep, sent.at[1]).wait()
        whole(to_cross, sent.at[2]).wait()

        @pl.when(is_inner)
        def _():
            blocks_sent(7)

        @pl.when(is_outer)
        def _():
            blocks_sent(5)

        swaps_sent()
        with scope("w_end"):
            whole(out_ref, sent.at[5]).wait()


def dense_layer(tokens, gain, route_ids, route_weights, w_gate, w_up, w_down):
    rows, features = tokens.shape
    units = 2 * w_gate.shape[2]
    batches = rows // 16
    pieces = 6
    width = features // pieces
    hbm = pl.BlockSpec(memory_space=pltpu.HBM)
    half = jnp.bfloat16
    dma = pltpu.SemaphoreType.DMA
    ids = route_ids.T
    weights = route_weights.T
    operands = (tokens, gain, ids, weights, w_gate, w_up, w_down)
    travel = pltpu.VMEM((pieces, 2 * rows, width), half)
    single = pltpu.VMEM((pieces, rows, width), half)
    return pl.pallas_call(
        dense_kernel,
        out_shape=pltpu.VMEM(tokens.shape, tokens.dtype),
        in_specs=[hbm] * 7,
        out_specs=pl.BlockSpec(memory_space=pltpu.VMEM),
        scratch_shapes=[
            pltpu.VMEM((rows, features), half),
            pltpu.VMEM((features,), jnp.float32),
            pltpu.VMEM(ids.shape, jnp.int32),
            pltpu.VMEM(weights.shape, jnp.float32),
            pltpu.VMEM((features, units), half),
            pltpu.VMEM((features, units), half),
            pltpu.VMEM((units, features), half),
            pltpu.VMEM((rows, features), half),
            pltpu.VMEM((4, rows, features), half),
            pltpu.VMEM((pieces, 2 * rows, width), jnp.float32),
        ]
        + [travel] * 6
        + [single] * 2
        + [
            pltpu.VMEM(weights.shape, jnp.float32),
            pltpu.VMEM((3, *weights.shape), jnp.float32),
            dma((4,)),
            dma((3,)),
            dma((3,)),
            dma((6,)),
            dma((2, max(batches, pieces))),
            dma((2,)),
            dma((pieces,)),
            dma((3, 2)),
            dma,
        ],
        compiler_params=pltpu.CompilerParams(
            collective_id=0, has_side_effects=True, vmem_limit_bytes=40_000_000
        ),
    )(*(pltpu.with_memory_space_constraint(array, pltpu.HBM) for array in operands))


def route_tables(chosen_ids, chosen_weights, expert_count, slot_room):
    row_count, top_count = chosen_ids.shape
    matches = (chosen_ids[:, :, None] == jnp.arange(expert_count, dtype=jnp.int32)).astype(
        jnp.float32
    )
    flat_match = matches.reshape(row_count * top_count, expert_count)
    order_range = jnp.arange(row_count * top_count, dtype=jnp.int32)
    earlier = (order_range[:, None] > order_range[None, :]).astype(jnp.float32)
    before = jnp.dot(
        earlier, flat_match, precision=lax.Precision.HIGHEST, preferred_element_type=jnp.float32
    )
    position = jnp.sum(before * flat_match, axis=1).reshape(row_count, top_count).astype(jnp.int32)
    slot_index = chosen_ids * slot_room + position
    targets = jnp.arange(expert_count * slot_room, dtype=jnp.int32)
    slot_hits = slot_index[None, :, :] == targets[:, None, None]
    send_table = jnp.sum(slot_hits.astype(jnp.float32), axis=2).astype(jnp.bfloat16)
    mix_table = jnp.sum(jnp.where(slot_hits, chosen_weights[None, :, :], 0.0), axis=2)
    return (send_table, mix_table)


def routed_layer(tokens, gain, route_ids, route_weights, w_gate, w_up, w_down):
    expert_axis = lax.axis_size("expert")
    expert_count = expert_axis // 2
    tensor_count = lax.axis_size("tensor")
    own_rows = tokens.shape[0] // tensor_count
    top_count = route_ids.shape[1]
    capacity = max(2, own_rows * top_count // expert_count)
    gate_local = w_gate[0]
    up_local = w_up[0]
    down_local = w_down[0]
    first_row = lax.axis_index("tensor") * own_rows
    own_tokens = lax.dynamic_slice_in_dim(tokens, first_row, own_rows, 0)
    own_ids = lax.dynamic_slice_in_dim(route_ids, first_row, own_rows, 0)
    own_weights = lax.dynamic_slice_in_dim(route_weights, first_row, own_rows, 0)
    resident = own_tokens.astype(jnp.float32)
    inv_rms = lax.rsqrt(jnp.mean(resident * resident, axis=1, keepdims=True) + 1e-05)
    normed = (resident * inv_rms * gain).astype(jnp.bfloat16)
    send_table, mix_table = route_tables(own_ids, own_weights, expert_count, capacity)
    packed = jnp.dot(send_table, normed, preferred_element_type=jnp.float32).astype(jnp.bfloat16)
    features = packed.shape[1]
    by_expert = packed.reshape(expert_count, 1, capacity, features)
    outgoing = jnp.broadcast_to(by_expert, (expert_count, 2, capacity, features)).reshape(
        expert_axis * capacity, features
    )
    arrived = lax.all_to_all(outgoing, "expert", split_axis=0, concat_axis=0, tiled=True)
    row_piece = lax.all_gather(arrived, "tensor", axis=0, tiled=True)
    gate_val = jnp.dot(row_piece, gate_local, preferred_element_type=jnp.float32)
    up_val = jnp.dot(row_piece, up_local, preferred_element_type=jnp.float32)
    hidden = gated_unit(gate_val, up_val).astype(jnp.bfloat16)
    partial_value = lax.psum_scatter(
        jnp.dot(hidden, down_local, preferred_element_type=jnp.float32),
        "tensor",
        scatter_dimension=0,
        tiled=True,
    )
    returned = lax.all_to_all(
        partial_value.astype(jnp.bfloat16), "expert", split_axis=0, concat_axis=0, tiled=True
    ).astype(partial_value.dtype)
    expert_out = (
        returned.reshape(expert_count, 2, capacity, features)
        .sum(axis=1)
        .reshape(expert_count * capacity, features)
    )
    weighted = jnp.dot(
        mix_table.T, expert_out, precision=lax.Precision.HIGHEST, preferred_element_type=jnp.float32
    )
    finished = (resident + weighted).astype(jnp.bfloat16)
    return lax.all_gather(finished, "tensor", axis=0, tiled=True)


def per_device(tokens, gain, route_ids, route_weights, w_gate, w_up, w_down):
    experts = lax.axis_size("expert") // 2
    dense = (
        route_ids.shape[1] == experts
        and experts == 4
        and lax.axis_size("tensor") == 2
        and w_gate.shape[0] == 1
    )
    layer = dense_layer if dense else routed_layer
    return layer(tokens, gain, route_ids, route_weights, w_gate, w_up, w_down)


def solution(mesh):
    placed = (
        P(("groups", "expert"), None),
        P(),
        P(("groups", "expert"), None),
        P(("groups", "expert"), None),
        P("expert", None, "tensor"),
        P("expert", None, "tensor"),
        P("expert", "tensor", None),
    )
    return jax.shard_map(
        per_device,
        mesh=mesh,
        in_specs=placed,
        out_specs=P(("groups", "expert"), None),
        check_vma=False,
    )
```

```python
import functools

import jax
import jax.numpy as jnp
from jax import lax
from jax.experimental import pallas as pl
from jax.experimental.pallas import tpu as pltpu
from jax.sharding import PartitionSpec as P

MESH = pl.DeviceIdType.MESH


def gated_unit(gate_val, up_val):
    return gate_val * jax.nn.sigmoid(1.702 * gate_val) * (up_val + 1.0)


def dense_kernel(
    tokens_ref,
    gain_ref,
    ids_ref,
    weights_ref,
    gate_ref,
    up_ref,
    down_ref,
    out_ref,
    held,
    gain,
    ids,
    weights,
    wg,
    wu,
    wd,
    own,
    slots,
    far_rows,
    far_out,
    far_in,
    first_out,
    first_in,
    second_out,
    second_in,
    own_pair,
    from_beside,
    from_across,
    to_cross,
    line_out,
    line_in,
    small_sem,
    load_sem,
    swap_recv,
    sent,
    spread_recv,
    rest_recv,
    done_recv,
    near_recv,
    pair_recv,
):
    me = lax.axis_index("expert")
    core = lax.axis_index("tensor")
    place = me // 2
    side = lax.rem(me, 2)
    half = place // 2
    inner = lax.rem(place + half, 2)
    is_inner = inner == 1
    is_outer = inner == 0

    def at(where, which):
        return {"expert": where * 2 + which}

    pair = place + 1 - 2 * lax.rem(place, 2)
    far_inner = 2 - half
    far_outer = 3 - 3 * half
    across = at(place, 1 - side)
    beside = at(pair, side)
    corner = at(pair, 1 - side)
    sibling = {"tensor": 1 - core}
    far_spots = (far_inner, far_outer)
    far = [at(spot, side) for spot in far_spots]
    my_far_slot = 1 - inner

    rows, features = own.shape
    cols = gate_ref.shape[2]
    batches = rows // 16
    groups = near_recv.shape[1]
    batch = rows // batches
    pieces, _, width = far_out.shape
    scope = jax.named_scope

    barrier = pltpu.get_barrier_semaphore()

    def greet(peers):
        for peer in peers:
            pl.semaphore_signal(barrier, inc=1, device_id=peer, device_id_type=MESH)

    def on(peer, which):
        return {**peer, "tensor": which}

    near_peers = [across, beside, corner, sibling]
    far_peers = [across, beside, far[0], sibling]

    @pl.when(core == 0)
    def _():
        greet([*near_peers, on(across, 1), on(beside, 1)])

    @pl.when(core == 1)
    def _():
        greet([across, beside, sibling, on(across, 0), on(beside, 0)])

        @pl.when(is_inner)
        def _():
            greet(far)

    smalls = [
        pltpu.make_async_copy(src, dst, small_sem.at[i])
        for i, (src, dst) in enumerate(
            (
                (tokens_ref, held),
                (gain_ref, gain),
                (ids_ref, ids),
                (weights_ref, weights),
            )
        )
    ]
    for small in smalls:
        small.start()

    pairs = (
        (gate_ref.at[0], lambda part: wg.at[:, pl.ds(part * cols, cols)]),
        (up_ref.at[0], lambda part: wu.at[:, pl.ds(part * cols, cols)]),
        (down_ref.at[0], lambda part: wd.at[pl.ds(part * cols, cols), :]),
    )
    loads = [
        pltpu.make_async_copy(src, dst(0), load_sem.at[i]) for i, (src, dst) in enumerate(pairs)
    ]
    for load in loads:
        load.start()

    def remote(src, dst, send, recv, peer):
        return pltpu.make_async_remote_copy(
            src_ref=src, dst_ref=dst, send_sem=send, recv_sem=recv, device_id=peer,
            device_id_type=MESH,
        )

    swaps = [
        remote(src, dst(1), sent.at[3 + i // 2], swap_recv.at[i], sibling)
        for i, (src, dst) in enumerate(pairs)
    ]

    def rows_of(q):
        return pl.ds(q * batch, batch)

    def part(p):
        return pl.ds(p * width, width)

    with scope("w_small"):
        smalls[0].wait()
        smalls[1].wait()

    def normed():
        resident = held[...].astype(jnp.float32)
        inv_rms = lax.rsqrt(jnp.mean(resident * resident, axis=1, keepdims=True) + 1e-05)
        return (resident * inv_rms * gain[...].reshape(1, -1)).astype(jnp.bfloat16)

    lanes = line_out.shape[1]
    spots = line_out.shape[0]
    spot_ids = lax.broadcasted_iota(jnp.int32, (rows, rows), 0)
    lane_ids = lax.broadcasted_iota(jnp.int32, (rows, rows), 1)

    def line_of(spot):
        named = jnp.where(ids[...] == spot, weights[...], 0.0)
        return jnp.sum(named, axis=0, keepdims=True)

    def column(line):
        return jnp.sum(jnp.where(spot_ids == lane_ids, line, 0.0), axis=1, keepdims=True)

    def ready(i):
        loads[i].wait()
        swaps[i].wait_recv()

    def hidden_of(block, fresh):
        if fresh:
            with scope("w_wg"):
                ready(0)
        gate_val = jnp.dot(block, wg[...], preferred_element_type=jnp.float32)
        if fresh:
            with scope("w_wu"):
                ready(1)
        up_val = jnp.dot(block, wu[...], preferred_element_type=jnp.float32)
        value = gated_unit(gate_val, up_val).astype(jnp.bfloat16)
        if fresh:
            with scope("w_wd"):
                ready(2)
        return value

    def stacked(ref, first):
        return ref[pl.ds(first, 2)].reshape(2 * rows, features)

    def down(hidden, p):
        return jnp.dot(hidden, wd[:, part(p)], preferred_element_type=jnp.float32)

    def give(p):
        there = out_ref.at[:, part(p)]
        return remote(there, there, sent.at[5], done_recv.at[1], sibling)

    def whole(ref, sem):
        return pltpu.make_async_copy(ref, ref, sem)

    def spread(slot, q, src, peer, recv):
        return remote(
            src.at[rows_of(q), :], slots.at[slot, rows_of(q), :], sent.at[0], recv, peer
        )

    def blocks_sent(count):
        whole(wd.at[pl.ds(0, count * rows), :], sent.at[0]).wait()

    def swaps_sent():
        whole(wg, sent.at[3]).wait()
        swaps[2].wait_send()

    def group(p):
        return p * groups // pieces

    def grouped(ref, i, g):
        span = pieces // groups
        return whole(ref.at[pl.ds(g * span, span)], near_recv.at[i, g])

    batched = (range(1), range(1, pieces // 2), range(pieces // 2, pieces))
    lower, upper = pl.ds(0, rows), pl.ds(rows, rows)

    @pl.when(core == 0)
    def _():
        def across_came(q):
            return whole(slots.at[1, rows_of(q), :], spread_recv.at[0, q])

        def beside_came(q):
            return whole(slots.at[2, rows_of(q), :], spread_recv.at[1, q])

        def on_to_beside(q):
            return spread(3, q, slots.at[1], beside, rest_recv.at[0])

        def on_to_across(q):
            return spread(3, q, slots.at[2], across, rest_recv.at[0])

        def along(p, half, recv):
            return remote(
                second_out.at[p, half, :], from_beside.at[p, half, :], sent.at[2], recv,
                on(beside, 1),
            )

        def line_to(i):
            return remote(
                line_out, line_in.at[i], sent.at[5], done_recv.at[0],
                (across, beside, corner)[i],
            )

        slots[0] = normed()
        smalls[2].wait()
        smalls[3].wait()
        for spot in range(spots):
            line_out[spot : spot + 1, :] = line_of(spot)
        with scope("w_bar"):
            pl.semaphore_wait(barrier, len(near_peers) + 2)
        for i in range(3):
            line_to(i).start()
        for swap in swaps:
            swap.start()
        for q in range(batches):
            with scope(f"w_A{q}"):
                across_came(q).wait()

            @pl.when(is_outer)
            def _():
                on_to_beside(q).start()
                with scope(f"w_Po{q}"):
                    beside_came(q).wait()
                on_to_across(q).start()

        def share(table):
            own_line = jnp.sum(
                jnp.where(
                    lax.broadcasted_iota(jnp.int32, (spots, lanes), 0) == place, table, 0.0
                ),
                axis=0,
                keepdims=True,
            )
            return column(own_line)

        hidden = hidden_of(stacked(slots, 0), True)
        with scope("w_line"):
            whole(line_in, done_recv.at[0]).wait()
        own_share = share(line_out[...])
        shares = [share(line_in[i]) for i in range(3)]
        scales = jnp.concatenate([own_share, shares[0]], axis=0)
        for p in range(pieces):
            first_out[p] = (down(hidden, p) * scales).astype(jnp.bfloat16)

        def hand_pair(p):
            return remote(
                first_out.at[p], own_pair.at[p], sent.at[1], pair_recv, sibling
            )

        for p in range(pieces):
            hand_pair(p).start()

        def far_products():
            with scope("w_far"):
                whole(far_rows, rest_recv.at[1]).wait()
            value = hidden_of(stacked(far_rows, 0), False)
            for p in range(pieces):
                far_out[p] = down(value, p).astype(jnp.bfloat16)
            for p in range(pieces):
                remote(
                    far_out.at[p], far_in.at[p], sent.at[6], near_recv.at[3, 0], sibling
                ).start()

        pl.when(is_inner)(far_products)

        @pl.when(is_inner)
        def _():
            for q in range(batches):
                with scope(f"w_P{q}"):
                    beside_came(q).wait()

        with scope("w_D"):
            whole(slots.at[3], rest_recv.at[0]).wait()
        hidden = hidden_of(stacked(slots, 2), False)
        scales = jnp.concatenate([shares[1], shares[2]], axis=0)
        for batch_of in batched:
            for p in batch_of:
                second_out[p] = (down(hidden, p) * scales).astype(jnp.bfloat16)
            for p in batch_of:
                along(p, upper, near_recv.at[0, group(p)]).start()
        for p in range(pieces):
            along(p, lower, near_recv.at[2, group(p)]).start()
        pl.when(is_outer)(far_products)
        whole(far_out, sent.at[6]).wait()
        whole(line_in, sent.at[5]).wait()

        @pl.when(is_outer)
        def _():
            blocks_sent(2)

        whole(first_out, sent.at[1]).wait()
        whole(second_out, sent.at[2]).wait()
        swaps_sent()
        with scope("w_give"):
            whole(out_ref, done_recv.at[1]).wait()

    @pl.when(core == 1)
    def _():
        def near_x(q):
            return remote(
                own.at[rows_of(q), :], slots.at[1, rows_of(q), :], sent.at[0],
                spread_recv.at[0, q], on(across, 0),
            )

        def near_z(q):
            return remote(
                own.at[rows_of(q), :], slots.at[2, rows_of(q), :], sent.at[0],
                spread_recv.at[1, q], on(beside, 0),
            )

        def outward(q):
            return remote(
                own.at[rows_of(q), :], slots.at[my_far_slot, rows_of(q), :], sent.at[0],
                spread_recv.at[my_far_slot, q], far[0],
            )

        def arrived(s, q):
            return spread(s, q, slots.at[s], beside, spread_recv.at[s, q])

        def pass_on(s, q):
            return remote(
                slots.at[s, rows_of(q), :], far_rows.at[s, rows_of(q), :], sent.at[0],
                rest_recv.at[1], sibling,
            )

        def sideways(s, q):
            return spread(3 - s, q, slots.at[s], across, rest_recv.at[s])

        def back_x(s, p):
            rows_there = (lower, upper)[s]
            return remote(
                first_out.at[p, rows_there, :], first_in.at[p, rows_there, :], sent.at[1],
                spread_recv.at[s, p], across,
            )

        def back_z(s, p):
            return remote(
                second_out.at[p, (lower, upper)[s], :],
                second_in.at[p, pl.ds(pl.multiple_of(my_far_slot * rows, rows), rows), :],
                sent.at[1],
                done_recv.at[p],
                far[s],
            )

        def came_z(p):
            return whole(second_in.at[p], done_recv.at[p])

        def cross(p):
            return remote(
                to_cross.at[p], from_across.at[p], sent.at[2], near_recv.at[1, group(p)],
                across,
            )

        own[...] = normed()
        with scope("w_bar"):
            pl.semaphore_wait(barrier, len(far_peers) + 2)
        for q in range(batches):
            outward(q).start()
        for q in range(batches):
            near_x(q).start()
        for q in range(batches):
            near_z(q).start()
        for swap in swaps:
            swap.start()
        smalls[2].wait()
        smalls[3].wait()
        shares = [column(line_of(spot)) for spot in far_spots]
        for s, q in [(1, q) for q in range(batches)] + [(0, q) for q in range(batches)]:
            with scope(f"w_F{s}{q}"):
                arrived(s, q).wait_recv()

            @pl.when(is_inner)
            def _():
                arrived(s, q).start()

            sideways(s, q).start()
            pass_on(s, q).start()
        with scope("w_G1"):
            whole(slots.at[2], rest_recv.at[1]).wait()
        hidden = hidden_of(slots[2], True)
        for batch_of in batched:
            for p in batch_of:
                first_out[p, upper, :] = down(hidden, p).astype(jnp.bfloat16)
            for p in batch_of:
                back_x(1, p).start()
        with scope("w_G0"):
            whole(slots.at[3], rest_recv.at[0]).wait()
        late_hidden = hidden_of(slots[3], False)
        for batch_of in batched:
            for p in batch_of:
                first_out[p, lower, :] = down(late_hidden, p).astype(jnp.bfloat16)
            for p in batch_of:
                back_x(0, p).start()
        with scope("w_far"):
            whole(far_in, near_recv.at[3, 0]).wait()
        span = pieces // groups

        def merge(g):
            with scope(f"w_be{g}"):
                if g == 0:
                    whole(own_pair, pair_recv).wait()
                grouped(from_beside.at[:, upper, :], 0, g).wait()
            for i in range(g * span, g * span + span):
                sums = own_pair[i, upper, :].astype(jnp.float32)
                sums = sums + from_beside[i, upper, :].astype(jnp.float32)
                to_cross[i] = sums.astype(jnp.bfloat16)
                cross(i).start()

        for s in (1, 0):
            there = (lower, upper)[s]
            for p in range(pieces):
                with scope(f"w_bx{s}{p}"):
                    back_x(s, p).wait_recv()
                both = far_in[p, there, :].astype(jnp.float32)
                both = both + first_in[p, there, :].astype(jnp.float32)
                second_out[p, there, :] = both.astype(jnp.bfloat16)
                back_z(s, p).start()

            @pl.when((place == 0) == (s == 1))
            def _():
                for g in range(groups):
                    merge(g)

        for p in range(pieces):
            if p % span == 0:
                with scope(f"w_xA{p}"):
                    grouped(from_across, 1, group(p)).wait()
                with scope(f"w_low{p}"):
                    grouped(from_beside.at[:, lower, :], 2, group(p)).wait()
            total = held[:, part(p)].astype(jnp.float32)
            total = total + own_pair[p, lower, :].astype(jnp.float32)
            total = total + from_beside[p, lower, :].astype(jnp.float32)
            total = total + from_across[p].astype(jnp.float32)
            with scope(f"w_bz{p}"):
                came_z(p).wait()
            for s in range(2):
                total = total + shares[s] * second_in[p, (lower, upper)[s], :].astype(jnp.float32)
            out_ref[:, part(p)] = total.astype(jnp.bfloat16)
            give(p).start()
        whole(slots, sent.at[1]).wait()
        whole(to_cross, sent.at[2]).wait()

        @pl.when(is_inner)
        def _():
            blocks_sent(9)

        @pl.when(is_outer)
        def _():
            blocks_sent(7)

        swaps_sent()
        with scope("w_end"):
            whole(out_ref, sent.at[5]).wait()


def dense_layer(tokens, gain, route_ids, route_weights, w_gate, w_up, w_down):
    rows, features = tokens.shape
    units = 2 * w_gate.shape[2]
    batches = rows // 16
    pieces = 6
    width = features // pieces
    hbm = pl.BlockSpec(memory_space=pltpu.HBM)
    half = jnp.bfloat16
    dma = pltpu.SemaphoreType.DMA
    ids = route_ids.T
    weights = route_weights.T
    operands = (tokens, gain, ids, weights, w_gate, w_up, w_down)
    travel = pltpu.VMEM((pieces, 2 * rows, width), half)
    single = pltpu.VMEM((pieces, rows, width), half)
    return pl.pallas_call(
        dense_kernel,
        out_shape=pltpu.VMEM(tokens.shape, tokens.dtype),
        in_specs=[hbm] * 7,
        out_specs=pl.BlockSpec(memory_space=pltpu.VMEM),
        scratch_shapes=[
            pltpu.VMEM((rows, features), half),
            pltpu.VMEM((features,), jnp.float32),
            pltpu.VMEM(ids.shape, jnp.int32),
            pltpu.VMEM(weights.shape, jnp.float32),
            pltpu.VMEM((features, units), half),
            pltpu.VMEM((features, units), half),
            pltpu.VMEM((units, features), half),
            pltpu.VMEM((rows, features), half),
            pltpu.VMEM((4, rows, features), half),
            pltpu.VMEM((2, rows, features), half),
        ]
        + [travel] * 8
        + [single] * 2
        + [
            pltpu.VMEM(weights.shape, jnp.float32),
            pltpu.VMEM((3, *weights.shape), jnp.float32),
            dma((4,)),
            dma((3,)),
            dma((3,)),
            dma((7,)),
            dma((2, max(batches, pieces))),
            dma((2,)),
            dma((pieces,)),
            dma((4, 2)),
            dma,
        ],
        compiler_params=pltpu.CompilerParams(
            collective_id=0, has_side_effects=True, vmem_limit_bytes=40_000_000
        ),
    )(*(pltpu.with_memory_space_constraint(array, pltpu.HBM) for array in operands))


def route_tables(chosen_ids, chosen_weights, expert_count, slot_room):
    row_count, top_count = chosen_ids.shape
    matches = (chosen_ids[:, :, None] == jnp.arange(expert_count, dtype=jnp.int32)).astype(
        jnp.float32
    )
    flat_match = matches.reshape(row_count * top_count, expert_count)
    order_range = jnp.arange(row_count * top_count, dtype=jnp.int32)
    earlier = (order_range[:, None] > order_range[None, :]).astype(jnp.float32)
    before = jnp.dot(
        earlier, flat_match, precision=lax.Precision.HIGHEST, preferred_element_type=jnp.float32
    )
    position = jnp.sum(before * flat_match, axis=1).reshape(row_count, top_count).astype(jnp.int32)
    slot_index = chosen_ids * slot_room + position
    targets = jnp.arange(expert_count * slot_room, dtype=jnp.int32)
    slot_hits = slot_index[None, :, :] == targets[:, None, None]
    send_table = jnp.sum(slot_hits.astype(jnp.float32), axis=2).astype(jnp.bfloat16)
    mix_table = jnp.sum(jnp.where(slot_hits, chosen_weights[None, :, :], 0.0), axis=2)
    return (send_table, mix_table)


def routed_layer(tokens, gain, route_ids, route_weights, w_gate, w_up, w_down):
    expert_axis = lax.axis_size("expert")
    expert_count = expert_axis // 2
    tensor_count = lax.axis_size("tensor")
    own_rows = tokens.shape[0] // tensor_count
    top_count = route_ids.shape[1]
    capacity = max(2, own_rows * top_count // expert_count)
    gate_local = w_gate[0]
    up_local = w_up[0]
    down_local = w_down[0]
    first_row = lax.axis_index("tensor") * own_rows
    own_tokens = lax.dynamic_slice_in_dim(tokens, first_row, own_rows, 0)
    own_ids = lax.dynamic_slice_in_dim(route_ids, first_row, own_rows, 0)
    own_weights = lax.dynamic_slice_in_dim(route_weights, first_row, own_rows, 0)
    resident = own_tokens.astype(jnp.float32)
    inv_rms = lax.rsqrt(jnp.mean(resident * resident, axis=1, keepdims=True) + 1e-05)
    normed = (resident * inv_rms * gain).astype(jnp.bfloat16)
    send_table, mix_table = route_tables(own_ids, own_weights, expert_count, capacity)
    packed = jnp.dot(send_table, normed, preferred_element_type=jnp.float32).astype(jnp.bfloat16)
    features = packed.shape[1]
    by_expert = packed.reshape(expert_count, 1, capacity, features)
    outgoing = jnp.broadcast_to(by_expert, (expert_count, 2, capacity, features)).reshape(
        expert_axis * capacity, features
    )
    arrived = lax.all_to_all(outgoing, "expert", split_axis=0, concat_axis=0, tiled=True)
    row_piece = lax.all_gather(arrived, "tensor", axis=0, tiled=True)
    gate_val = jnp.dot(row_piece, gate_local, preferred_element_type=jnp.float32)
    up_val = jnp.dot(row_piece, up_local, preferred_element_type=jnp.float32)
    hidden = gated_unit(gate_val, up_val).astype(jnp.bfloat16)
    partial_value = lax.psum_scatter(
        jnp.dot(hidden, down_local, preferred_element_type=jnp.float32),
        "tensor",
        scatter_dimension=0,
        tiled=True,
    )
    returned = lax.all_to_all(
        partial_value.astype(jnp.bfloat16), "expert", split_axis=0, concat_axis=0, tiled=True
    ).astype(partial_value.dtype)
    expert_out = (
        returned.reshape(expert_count, 2, capacity, features)
        .sum(axis=1)
        .reshape(expert_count * capacity, features)
    )
    weighted = jnp.dot(
        mix_table.T, expert_out, precision=lax.Precision.HIGHEST, preferred_element_type=jnp.float32
    )
    finished = (resident + weighted).astype(jnp.bfloat16)
    return lax.all_gather(finished, "tensor", axis=0, tiled=True)


def per_device(tokens, gain, route_ids, route_weights, w_gate, w_up, w_down):
    experts = lax.axis_size("expert") // 2
    dense = (
        route_ids.shape[1] == experts
        and experts == 4
        and lax.axis_size("tensor") == 2
        and w_gate.shape[0] == 1
    )
    layer = dense_layer if dense else routed_layer
    return layer(tokens, gain, route_ids, route_weights, w_gate, w_up, w_down)


def solution(mesh):
    placed = (
        P(("groups", "expert"), None),
        P(),
        P(("groups", "expert"), None),
        P(("groups", "expert"), None),
        P("expert", None, "tensor"),
        P("expert", None, "tensor"),
        P("expert", "tensor", None),
    )
    return jax.shard_map(
        per_device,
        mesh=mesh,
        in_specs=placed,
        out_specs=P(("groups", "expert"), None),
        check_vma=False,
    )
```

```python
import functools

import jax
import jax.numpy as jnp
from jax import lax
from jax.experimental import pallas as pl
from jax.experimental.pallas import tpu as pltpu
from jax.sharding import PartitionSpec as P

MESH = pl.DeviceIdType.MESH


def gated_unit(gate_val, up_val):
    return gate_val * jax.nn.sigmoid(1.702 * gate_val) * (up_val + 1.0)


def dense_kernel(
    tokens_ref,
    gain_ref,
    ids_ref,
    weights_ref,
    gate_ref,
    up_ref,
    down_ref,
    out_ref,
    held,
    gain,
    ids,
    weights,
    wg,
    wu,
    wd,
    own,
    slots,
    far_rows,
    far_out,
    far_in,
    first_out,
    first_in,
    second_out,
    second_in,
    own_pair,
    from_beside,
    from_across,
    to_cross,
    line_out,
    line_in,
    small_sem,
    load_sem,
    sent,
    spread_recv,
    rest_recv,
    done_recv,
    near_recv,
    pair_recv,
):
    me = lax.axis_index("expert")
    core = lax.axis_index("tensor")
    place = me // 2
    side = lax.rem(me, 2)
    half = place // 2
    inner = lax.rem(place + half, 2)
    is_inner = inner == 1
    is_outer = inner == 0

    def at(where, which):
        return {"expert": where * 2 + which}

    pair = place + 1 - 2 * lax.rem(place, 2)
    far_inner = 2 - half
    far_outer = 3 - 3 * half
    across = at(place, 1 - side)
    beside = at(pair, side)
    corner = at(pair, 1 - side)
    sibling = {"tensor": 1 - core}
    far_spots = (far_inner, far_outer)
    far = [at(spot, side) for spot in far_spots]
    my_far_slot = 1 - inner

    rows, features = own.shape
    cols = gate_ref.shape[2]
    batches = rows // 16
    groups = near_recv.shape[1]
    batch = rows // batches
    pieces, _, width = far_out.shape
    scope = jax.named_scope

    barrier = pltpu.get_barrier_semaphore()

    def greet(peers):
        for peer in peers:
            pl.semaphore_signal(barrier, inc=1, device_id=peer, device_id_type=MESH)

    def on(peer, which):
        return {**peer, "tensor": which}

    near_peers = [across, beside, corner, sibling]
    far_peers = [across, beside, far[0], sibling]

    @pl.when(core == 0)
    def _():
        greet([*near_peers, on(across, 1), on(beside, 1)])

    @pl.when(core == 1)
    def _():
        greet([across, beside, sibling, on(across, 0), on(beside, 0)])

        @pl.when(is_inner)
        def _():
            greet(far)

    smalls = [
        pltpu.make_async_copy(src, dst, small_sem.at[i])
        for i, (src, dst) in enumerate(
            (
                (tokens_ref, held),
                (gain_ref, gain),
                (ids_ref, ids),
                (weights_ref, weights),
            )
        )
    ]
    for small in smalls:
        small.start()

    pairs = (
        (gate_ref.at[0], lambda part: wg.at[:, pl.ds(part * cols, cols)]),
        (up_ref.at[0], lambda part: wu.at[:, pl.ds(part * cols, cols)]),
        (down_ref.at[0], lambda part: wd.at[pl.ds(part * cols, cols), :]),
    )
    loads = [
        pltpu.make_async_copy(src, dst(0), load_sem.at[i]) for i, (src, dst) in enumerate(pairs)
    ]
    for load in loads:
        load.start()

    def remote(src, dst, send, recv, peer):
        return pltpu.make_async_remote_copy(
            src_ref=src, dst_ref=dst, send_sem=send, recv_sem=recv, device_id=peer,
            device_id_type=MESH,
        )

    swaps = [
        remote(src, dst(1), sent.at[3 + i // 2], load_sem.at[i], sibling)
        for i, (src, dst) in enumerate(pairs)
    ]

    def rows_of(q):
        return pl.ds(q * batch, batch)

    def part(p):
        return pl.ds(p * width, width)

    with scope("w_small"):
        smalls[0].wait()
        smalls[1].wait()

    def normed():
        resident = held[...].astype(jnp.float32)
        inv_rms = lax.rsqrt(jnp.mean(resident * resident, axis=1, keepdims=True) + 1e-05)
        return (resident * inv_rms * gain[...].reshape(1, -1)).astype(jnp.bfloat16)

    lanes = line_out.shape[1]
    spots = line_out.shape[0]
    spot_ids = lax.broadcasted_iota(jnp.int32, (rows, rows), 0)
    lane_ids = lax.broadcasted_iota(jnp.int32, (rows, rows), 1)

    def line_of(spot):
        named = jnp.where(ids[...] == spot, weights[...], 0.0)
        return jnp.sum(named, axis=0, keepdims=True)

    def column(line):
        return jnp.sum(jnp.where(spot_ids == lane_ids, line, 0.0), axis=1, keepdims=True)

    def ready(i):
        whole((wg, wu, wd)[i], load_sem.at[i]).wait()

    def hidden_of(block, fresh):
        if fresh:
            with scope("w_wg"):
                ready(0)
        gate_val = jnp.dot(block, wg[...], preferred_element_type=jnp.float32)
        if fresh:
            with scope("w_wu"):
                ready(1)
        up_val = jnp.dot(block, wu[...], preferred_element_type=jnp.float32)
        value = gated_unit(gate_val, up_val).astype(jnp.bfloat16)
        if fresh:
            with scope("w_wd"):
                ready(2)
        return value

    def stacked(ref, first):
        return ref[pl.ds(first, 2)].reshape(2 * rows, features)

    def down(hidden, p):
        return jnp.dot(hidden, wd[:, part(p)], preferred_element_type=jnp.float32)

    def give(g):
        span = features // groups
        there = out_ref.at[:, pl.ds(g * span, span)]
        return remote(there, there, sent.at[5], done_recv.at[1], sibling)

    def whole(ref, sem):
        return pltpu.make_async_copy(ref, ref, sem)

    def spread(slot, q, src, peer, recv):
        return remote(
            src.at[rows_of(q), :], slots.at[slot, rows_of(q), :], sent.at[0], recv, peer
        )

    def blocks_sent(count):
        whole(wd.at[pl.ds(0, count * rows), :], sent.at[0]).wait()

    def swaps_sent():
        whole(wg, sent.at[3]).wait()
        swaps[2].wait_send()

    def group(p):
        return p * groups // pieces

    def grouped(ref, i, g):
        span = pieces // groups
        return whole(ref.at[pl.ds(g * span, span)], near_recv.at[i, g])

    batched = (range(1), range(1, pieces // 2), range(pieces // 2, pieces))
    lower, upper = pl.ds(0, rows), pl.ds(rows, rows)

    @pl.when(core == 0)
    def _():
        def across_came(q):
            return whole(slots.at[1, rows_of(q), :], spread_recv.at[0, q])

        def beside_came(q):
            return whole(slots.at[2, rows_of(q), :], spread_recv.at[1, q])

        def on_to_beside(q):
            return spread(3, q, slots.at[1], beside, rest_recv.at[0])

        def on_to_across(q):
            return spread(3, q, slots.at[2], across, rest_recv.at[0])

        def along(p, half, recv):
            return remote(
                second_out.at[p, half, :], from_beside.at[p, half, :], sent.at[2], recv,
                on(beside, 1),
            )

        def line_to(i):
            return remote(
                line_out, line_in.at[i], sent.at[5], done_recv.at[0],
                (across, beside, corner)[i],
            )

        slots[0] = normed()
        smalls[2].wait()
        smalls[3].wait()
        for spot in range(spots):
            line_out[spot : spot + 1, :] = line_of(spot)
        with scope("w_bar"):
            pl.semaphore_wait(barrier, len(near_peers) + 2)
        for i in range(3):
            line_to(i).start()
        for swap in swaps:
            swap.start()
        for q in range(batches):
            with scope(f"w_A{q}"):
                across_came(q).wait()

            @pl.when(is_outer)
            def _():
                on_to_beside(q).start()
                with scope(f"w_Po{q}"):
                    beside_came(q).wait()
                on_to_across(q).start()

        def share(table):
            own_line = jnp.sum(
                jnp.where(
                    lax.broadcasted_iota(jnp.int32, (spots, lanes), 0) == place, table, 0.0
                ),
                axis=0,
                keepdims=True,
            )
            return column(own_line)

        hidden = hidden_of(stacked(slots, 0), True)
        with scope("w_line"):
            whole(line_in, done_recv.at[0]).wait()
        own_share = share(line_out[...])
        shares = [share(line_in[i]) for i in range(3)]
        scales = jnp.concatenate([own_share, shares[0]], axis=0)
        for p in range(pieces):
            first_out[p] = (down(hidden, p) * scales).astype(jnp.bfloat16)

        def hand_pair(p):
            return remote(
                first_out.at[p], own_pair.at[p], sent.at[1], pair_recv, sibling
            )

        for p in range(pieces):
            hand_pair(p).start()

        def far_products():
            with scope("w_far"):
                whole(far_rows, rest_recv.at[1]).wait()
            value = hidden_of(stacked(far_rows, 0), False)
            for p in range(pieces):
                far_out[p] = down(value, p).astype(jnp.bfloat16)
            for p in range(pieces):
                remote(
                    far_out.at[p], far_in.at[p], sent.at[6], near_recv.at[3, 0], sibling
                ).start()

        pl.when(is_inner)(far_products)

        @pl.when(is_inner)
        def _():
            for q in range(batches):
                with scope(f"w_P{q}"):
                    beside_came(q).wait()

        with scope("w_D"):
            whole(slots.at[3], rest_recv.at[0]).wait()
        hidden = hidden_of(stacked(slots, 2), False)
        scales = jnp.concatenate([shares[1], shares[2]], axis=0)
        for batch_of in batched:
            for p in batch_of:
                second_out[p] = (down(hidden, p) * scales).astype(jnp.bfloat16)
            for p in batch_of:
                along(p, upper, near_recv.at[0, group(p)]).start()
        for p in range(pieces):
            along(p, lower, near_recv.at[2, group(p)]).start()
        pl.when(is_outer)(far_products)
        whole(far_out, sent.at[6]).wait()
        whole(line_in, sent.at[5]).wait()

        @pl.when(is_outer)
        def _():
            blocks_sent(2)

        whole(first_out, sent.at[1]).wait()
        whole(second_out, sent.at[2]).wait()
        swaps_sent()
        with scope("w_give"):
            whole(out_ref, done_recv.at[1]).wait()

    @pl.when(core == 1)
    def _():
        def near_x(q):
            return remote(
                own.at[rows_of(q), :], slots.at[1, rows_of(q), :], sent.at[0],
                spread_recv.at[0, q], on(across, 0),
            )

        def near_z(q):
            return remote(
                own.at[rows_of(q), :], slots.at[2, rows_of(q), :], sent.at[0],
                spread_recv.at[1, q], on(beside, 0),
            )

        def outward(q):
            return remote(
                own.at[rows_of(q), :], slots.at[my_far_slot, rows_of(q), :], sent.at[0],
                spread_recv.at[my_far_slot, q], far[0],
            )

        def arrived(s, q):
            return spread(s, q, slots.at[s], beside, spread_recv.at[s, q])

        def pass_on(s, q):
            return remote(
                slots.at[s, rows_of(q), :], far_rows.at[s, rows_of(q), :], sent.at[0],
                rest_recv.at[1], sibling,
            )

        def sideways(s, q):
            return spread(3 - s, q, slots.at[s], across, rest_recv.at[s])

        def back_x(s, p):
            rows_there = (lower, upper)[s]
            return remote(
                first_out.at[p, rows_there, :], first_in.at[p, rows_there, :], sent.at[1],
                spread_recv.at[s, p], across,
            )

        def back_z(s, p):
            return remote(
                second_out.at[p, (lower, upper)[s], :],
                second_in.at[p, pl.ds(pl.multiple_of(my_far_slot * rows, rows), rows), :],
                sent.at[1],
                done_recv.at[p],
                far[s],
            )

        def came_z(p):
            return whole(second_in.at[p], done_recv.at[p])

        def cross(p):
            return remote(
                to_cross.at[p], from_across.at[p], sent.at[2], near_recv.at[1, group(p)],
                across,
            )

        own[...] = normed()
        with scope("w_bar"):
            pl.semaphore_wait(barrier, len(far_peers) + 2)
        for q in range(batches):
            outward(q).start()
        for q in range(batches):
            near_x(q).start()
        for q in range(batches):
            near_z(q).start()
        for swap in swaps:
            swap.start()
        smalls[2].wait()
        smalls[3].wait()
        shares = [column(line_of(spot)) for spot in far_spots]
        for s, q in [(1, q) for q in range(batches)] + [(0, q) for q in range(batches)]:
            with scope(f"w_F{s}{q}"):
                arrived(s, q).wait_recv()

            @pl.when(is_inner)
            def _():
                arrived(s, q).start()

            sideways(s, q).start()
            pass_on(s, q).start()
        with scope("w_G1"):
            whole(slots.at[2], rest_recv.at[1]).wait()
        hidden = hidden_of(slots[2], True)
        for batch_of in batched:
            for p in batch_of:
                first_out[p, upper, :] = down(hidden, p).astype(jnp.bfloat16)
            for p in batch_of:
                back_x(1, p).start()
        with scope("w_G0"):
            whole(slots.at[3], rest_recv.at[0]).wait()
        late_hidden = hidden_of(slots[3], False)
        for batch_of in batched:
            for p in batch_of:
                first_out[p, lower, :] = down(late_hidden, p).astype(jnp.bfloat16)
            for p in batch_of:
                back_x(0, p).start()
        with scope("w_far"):
            whole(far_in, near_recv.at[3, 0]).wait()
        span = pieces // groups

        def merge(g):
            with scope(f"w_be{g}"):
                if g == 0:
                    whole(own_pair, pair_recv).wait()
                grouped(from_beside.at[:, upper, :], 0, g).wait()
            for i in range(g * span, g * span + span):
                sums = own_pair[i, upper, :].astype(jnp.float32)
                sums = sums + from_beside[i, upper, :].astype(jnp.float32)
                to_cross[i] = sums.astype(jnp.bfloat16)
                cross(i).start()

        for s in (1, 0):
            there = (lower, upper)[s]
            for p in range(pieces):
                with scope(f"w_bx{s}{p}"):
                    back_x(s, p).wait_recv()
                both = far_in[p, there, :].astype(jnp.float32)
                both = both + first_in[p, there, :].astype(jnp.float32)
                second_out[p, there, :] = both.astype(jnp.bfloat16)
                back_z(s, p).start()

            @pl.when((place == 0) == (s == 1))
            def _():
                for g in range(groups):
                    merge(g)

        for p in range(pieces):
            if p % span == 0:
                with scope(f"w_xA{p}"):
                    grouped(from_across, 1, group(p)).wait()
                with scope(f"w_low{p}"):
                    grouped(from_beside.at[:, lower, :], 2, group(p)).wait()
            total = held[:, part(p)].astype(jnp.float32)
            total = total + own_pair[p, lower, :].astype(jnp.float32)
            total = total + from_beside[p, lower, :].astype(jnp.float32)
            total = total + from_across[p].astype(jnp.float32)
            with scope(f"w_bz{p}"):
                came_z(p).wait()
            for s in range(2):
                total = total + shares[s] * second_in[p, (lower, upper)[s], :].astype(jnp.float32)
            out_ref[:, part(p)] = total.astype(jnp.bfloat16)
            if (p + 1) % span == 0:
                give(group(p)).start()
        whole(slots, sent.at[1]).wait()
        whole(to_cross, sent.at[2]).wait()

        @pl.when(is_inner)
        def _():
            blocks_sent(9)

        @pl.when(is_outer)
        def _():
            blocks_sent(7)

        swaps_sent()
        with scope("w_end"):
            whole(out_ref, sent.at[5]).wait()


def dense_layer(tokens, gain, route_ids, route_weights, w_gate, w_up, w_down):
    rows, features = tokens.shape
    units = 2 * w_gate.shape[2]
    batches = rows // 16
    pieces = 6
    width = features // pieces
    hbm = pl.BlockSpec(memory_space=pltpu.HBM)
    half = jnp.bfloat16
    dma = pltpu.SemaphoreType.DMA
    ids = route_ids.T
    weights = route_weights.T
    operands = (tokens, gain, ids, weights, w_gate, w_up, w_down)
    travel = pltpu.VMEM((pieces, 2 * rows, width), half)
    single = pltpu.VMEM((pieces, rows, width), half)
    return pl.pallas_call(
        dense_kernel,
        out_shape=pltpu.VMEM(tokens.shape, tokens.dtype),
        in_specs=[hbm] * 7,
        out_specs=pl.BlockSpec(memory_space=pltpu.VMEM),
        scratch_shapes=[
            pltpu.VMEM((rows, features), half),
            pltpu.VMEM((features,), jnp.float32),
            pltpu.VMEM(ids.shape, jnp.int32),
            pltpu.VMEM(weights.shape, jnp.float32),
            pltpu.VMEM((features, units), half),
            pltpu.VMEM((features, units), half),
            pltpu.VMEM((units, features), half),
            pltpu.VMEM((rows, features), half),
            pltpu.VMEM((4, rows, features), half),
            pltpu.VMEM((2, rows, features), half),
        ]
        + [travel] * 8
        + [single] * 2
        + [
            pltpu.VMEM(weights.shape, jnp.float32),
            pltpu.VMEM((3, *weights.shape), jnp.float32),
            dma((4,)),
            dma((3,)),
            dma((7,)),
            dma((2, max(batches, pieces))),
            dma((2,)),
            dma((pieces,)),
            dma((4, 2)),
            dma,
        ],
        compiler_params=pltpu.CompilerParams(
            collective_id=0, has_side_effects=True, vmem_limit_bytes=40_000_000
        ),
    )(*(pltpu.with_memory_space_constraint(array, pltpu.HBM) for array in operands))


def route_tables(chosen_ids, chosen_weights, expert_count, slot_room):
    row_count, top_count = chosen_ids.shape
    matches = (chosen_ids[:, :, None] == jnp.arange(expert_count, dtype=jnp.int32)).astype(
        jnp.float32
    )
    flat_match = matches.reshape(row_count * top_count, expert_count)
    order_range = jnp.arange(row_count * top_count, dtype=jnp.int32)
    earlier = (order_range[:, None] > order_range[None, :]).astype(jnp.float32)
    before = jnp.dot(
        earlier, flat_match, precision=lax.Precision.HIGHEST, preferred_element_type=jnp.float32
    )
    position = jnp.sum(before * flat_match, axis=1).reshape(row_count, top_count).astype(jnp.int32)
    slot_index = chosen_ids * slot_room + position
    targets = jnp.arange(expert_count * slot_room, dtype=jnp.int32)
    slot_hits = slot_index[None, :, :] == targets[:, None, None]
    send_table = jnp.sum(slot_hits.astype(jnp.float32), axis=2).astype(jnp.bfloat16)
    mix_table = jnp.sum(jnp.where(slot_hits, chosen_weights[None, :, :], 0.0), axis=2)
    return (send_table, mix_table)


def routed_layer(tokens, gain, route_ids, route_weights, w_gate, w_up, w_down):
    expert_axis = lax.axis_size("expert")
    expert_count = expert_axis // 2
    tensor_count = lax.axis_size("tensor")
    own_rows = tokens.shape[0] // tensor_count
    top_count = route_ids.shape[1]
    capacity = max(2, own_rows * top_count // expert_count)
    gate_local = w_gate[0]
    up_local = w_up[0]
    down_local = w_down[0]
    first_row = lax.axis_index("tensor") * own_rows
    own_tokens = lax.dynamic_slice_in_dim(tokens, first_row, own_rows, 0)
    own_ids = lax.dynamic_slice_in_dim(route_ids, first_row, own_rows, 0)
    own_weights = lax.dynamic_slice_in_dim(route_weights, first_row, own_rows, 0)
    resident = own_tokens.astype(jnp.float32)
    inv_rms = lax.rsqrt(jnp.mean(resident * resident, axis=1, keepdims=True) + 1e-05)
    normed = (resident * inv_rms * gain).astype(jnp.bfloat16)
    send_table, mix_table = route_tables(own_ids, own_weights, expert_count, capacity)
    packed = jnp.dot(send_table, normed, preferred_element_type=jnp.float32).astype(jnp.bfloat16)
    features = packed.shape[1]
    by_expert = packed.reshape(expert_count, 1, capacity, features)
    outgoing = jnp.broadcast_to(by_expert, (expert_count, 2, capacity, features)).reshape(
        expert_axis * capacity, features
    )
    arrived = lax.all_to_all(outgoing, "expert", split_axis=0, concat_axis=0, tiled=True)
    row_piece = lax.all_gather(arrived, "tensor", axis=0, tiled=True)
    gate_val = jnp.dot(row_piece, gate_local, preferred_element_type=jnp.float32)
    up_val = jnp.dot(row_piece, up_local, preferred_element_type=jnp.float32)
    hidden = gated_unit(gate_val, up_val).astype(jnp.bfloat16)
    partial_value = lax.psum_scatter(
        jnp.dot(hidden, down_local, preferred_element_type=jnp.float32),
        "tensor",
        scatter_dimension=0,
        tiled=True,
    )
    returned = lax.all_to_all(
        partial_value.astype(jnp.bfloat16), "expert", split_axis=0, concat_axis=0, tiled=True
    ).astype(partial_value.dtype)
    expert_out = (
        returned.reshape(expert_count, 2, capacity, features)
        .sum(axis=1)
        .reshape(expert_count * capacity, features)
    )
    weighted = jnp.dot(
        mix_table.T, expert_out, precision=lax.Precision.HIGHEST, preferred_element_type=jnp.float32
    )
    finished = (resident + weighted).astype(jnp.bfloat16)
    return lax.all_gather(finished, "tensor", axis=0, tiled=True)


def per_device(tokens, gain, route_ids, route_weights, w_gate, w_up, w_down):
    experts = lax.axis_size("expert") // 2
    dense = (
        route_ids.shape[1] == experts
        and experts == 4
        and lax.axis_size("tensor") == 2
        and w_gate.shape[0] == 1
    )
    layer = dense_layer if dense else routed_layer
    return layer(tokens, gain, route_ids, route_weights, w_gate, w_up, w_down)


def solution(mesh):
    placed = (
        P(("groups", "expert"), None),
        P(),
        P(("groups", "expert"), None),
        P(("groups", "expert"), None),
        P("expert", None, "tensor"),
        P("expert", None, "tensor"),
        P("expert", "tensor", None),
    )
    return jax.shard_map(
        per_device,
        mesh=mesh,
        in_specs=placed,
        out_specs=P(("groups", "expert"), None),
        check_vma=False,
    )
```

```python
import functools

import jax
import jax.numpy as jnp
from jax import lax
from jax.experimental import pallas as pl
from jax.experimental.pallas import tpu as pltpu
from jax.sharding import PartitionSpec as P

MESH = pl.DeviceIdType.MESH


def gated_unit(gate_val, up_val):
    return gate_val * jax.nn.sigmoid(1.702 * gate_val) * (up_val + 1.0)


def dense_kernel(
    tokens_ref,
    gain_ref,
    ids_ref,
    weights_ref,
    gate_ref,
    up_ref,
    down_ref,
    out_ref,
    held,
    gain,
    ids,
    weights,
    wg,
    wu,
    wd,
    own,
    slots,
    far_rows,
    far_out,
    far_in,
    first_out,
    first_in,
    second_out,
    second_in,
    own_pair,
    from_beside,
    from_across,
    to_cross,
    line_out,
    line_in,
    small_sem,
    load_sem,
    sent,
    spread_recv,
    rest_recv,
    done_recv,
    near_recv,
    pair_recv,
):
    me = lax.axis_index("expert")
    core = lax.axis_index("tensor")
    place = me // 2
    side = lax.rem(me, 2)
    half = place // 2
    inner = lax.rem(place + half, 2)
    is_inner = inner == 1
    is_outer = inner == 0

    def at(where, which):
        return {"expert": where * 2 + which}

    pair = place + 1 - 2 * lax.rem(place, 2)
    far_inner = 2 - half
    far_outer = 3 - 3 * half
    across = at(place, 1 - side)
    beside = at(pair, side)
    corner = at(pair, 1 - side)
    sibling = {"tensor": 1 - core}
    far_spots = (far_inner, far_outer)
    far = [at(spot, side) for spot in far_spots]
    my_far_slot = 1 - inner

    rows, features = own.shape
    cols = gate_ref.shape[2]
    batches = rows // 16
    groups = near_recv.shape[1]
    batch = rows // batches
    pieces, _, width = far_out.shape
    scope = jax.named_scope

    barrier = pltpu.get_barrier_semaphore()

    def greet(peers):
        for peer in peers:
            pl.semaphore_signal(barrier, inc=1, device_id=peer, device_id_type=MESH)

    def on(peer, which):
        return {**peer, "tensor": which}

    near_peers = [across, beside, corner, sibling]
    far_peers = [across, beside, far[0], sibling]

    @pl.when(core == 0)
    def _():
        greet([*near_peers, on(across, 1), on(beside, 1)])

    @pl.when(core == 1)
    def _():
        greet([across, beside, sibling, on(across, 0), on(beside, 0)])

        @pl.when(is_inner)
        def _():
            greet(far)

    smalls = [
        pltpu.make_async_copy(src, dst, small_sem.at[min(i, 2)])
        for i, (src, dst) in enumerate(
            (
                (tokens_ref, held),
                (gain_ref, gain),
                (ids_ref, ids),
                (weights_ref, weights),
            )
        )
    ]
    for small in smalls:
        small.start()

    pairs = (
        (gate_ref.at[0], lambda part: wg.at[:, pl.ds(part * cols, cols)]),
        (up_ref.at[0], lambda part: wu.at[:, pl.ds(part * cols, cols)]),
        (down_ref.at[0], lambda part: wd.at[pl.ds(part * cols, cols), :]),
    )
    loads = [
        pltpu.make_async_copy(src, dst(0), load_sem.at[i]) for i, (src, dst) in enumerate(pairs)
    ]
    for load in loads:
        load.start()

    def remote(src, dst, send, recv, peer):
        return pltpu.make_async_remote_copy(
            src_ref=src, dst_ref=dst, send_sem=send, recv_sem=recv, device_id=peer,
            device_id_type=MESH,
        )

    swaps = [
        remote(src, dst(1), sent.at[3 + i // 2], load_sem.at[i], sibling)
        for i, (src, dst) in enumerate(pairs)
    ]

    def rows_of(q):
        return pl.ds(q * batch, batch)

    def part(p):
        return pl.ds(p * width, width)

    with scope("w_small"):
        smalls[0].wait()
        smalls[1].wait()

    def normed():
        resident = held[...].astype(jnp.float32)
        inv_rms = lax.rsqrt(jnp.mean(resident * resident, axis=1, keepdims=True) + 1e-05)
        return (resident * inv_rms * gain[...].reshape(1, -1)).astype(jnp.bfloat16)

    lanes = line_out.shape[1]
    spots = line_out.shape[0]
    spot_ids = lax.broadcasted_iota(jnp.int32, (rows, rows), 0)
    lane_ids = lax.broadcasted_iota(jnp.int32, (rows, rows), 1)

    def line_of(spot):
        named = jnp.where(ids[...] == spot, weights[...], 0.0)
        return jnp.sum(named, axis=0, keepdims=True)

    def column(line):
        return jnp.sum(jnp.where(spot_ids == lane_ids, line, 0.0), axis=1, keepdims=True)

    def ready(i):
        whole((wg, wu, wd)[i], load_sem.at[i]).wait()

    def hidden_of(block, fresh):
        if fresh:
            with scope("w_wg"):
                ready(0)
        gate_val = jnp.dot(block, wg[...], preferred_element_type=jnp.float32)
        if fresh:
            with scope("w_wu"):
                ready(1)
        up_val = jnp.dot(block, wu[...], preferred_element_type=jnp.float32)
        value = gated_unit(gate_val, up_val).astype(jnp.bfloat16)
        if fresh:
            with scope("w_wd"):
                ready(2)
        return value

    def stacked(ref, first):
        return ref[pl.ds(first, 2)].reshape(2 * rows, features)

    def down(hidden, p):
        return jnp.dot(hidden, wd[:, part(p)], preferred_element_type=jnp.float32)

    def give(g):
        span = features // groups
        there = out_ref.at[:, pl.ds(g * span, span)]
        return remote(there, there, sent.at[5], done_recv.at[1], sibling)

    def whole(ref, sem):
        return pltpu.make_async_copy(ref, ref, sem)

    def spread(slot, q, src, peer, recv):
        return remote(
            src.at[rows_of(q), :], slots.at[slot, rows_of(q), :], sent.at[0], recv, peer
        )

    def blocks_sent(count):
        whole(wd.at[pl.ds(0, count * rows), :], sent.at[0]).wait()

    def swaps_sent():
        whole(wg, sent.at[3]).wait()
        swaps[2].wait_send()

    def group(p):
        return p * groups // pieces

    def grouped(ref, i, g):
        span = pieces // groups
        return whole(ref.at[pl.ds(g * span, span)], near_recv.at[i, g])

    batched = (range(1), range(1, pieces // 2), range(pieces // 2, pieces))
    lower, upper = pl.ds(0, rows), pl.ds(rows, rows)

    @pl.when(core == 0)
    def _():
        def across_came(q):
            return whole(slots.at[1, rows_of(q), :], spread_recv.at[0, q])

        def beside_came(q):
            return whole(slots.at[2, rows_of(q), :], spread_recv.at[1, q])

        def on_to_beside(q):
            return spread(3, q, slots.at[1], beside, rest_recv.at[0])

        def on_to_across(q):
            return spread(3, q, slots.at[2], across, rest_recv.at[0])

        def along(p, half, recv):
            return remote(
                second_out.at[p, half, :], from_beside.at[p, half, :], sent.at[2], recv,
                on(beside, 1),
            )

        def line_to(i):
            return remote(
                line_out, line_in.at[i], sent.at[5], done_recv.at[0],
                (across, beside, corner)[i],
            )

        slots[0] = normed()
        whole(line_in.at[pl.ds(0, 2)], small_sem.at[2]).wait()
        for spot in range(spots):
            line_out[spot : spot + 1, :] = line_of(spot)
        with scope("w_bar"):
            pl.semaphore_wait(barrier, len(near_peers) + 2)
        for i in range(3):
            line_to(i).start()
        for swap in swaps:
            swap.start()
        for q in range(batches):
            with scope(f"w_A{q}"):
                across_came(q).wait()

            @pl.when(is_outer)
            def _():
                on_to_beside(q).start()
                with scope(f"w_Po{q}"):
                    beside_came(q).wait()
                on_to_across(q).start()

        def share(table):
            own_line = jnp.sum(
                jnp.where(
                    lax.broadcasted_iota(jnp.int32, (spots, lanes), 0) == place, table, 0.0
                ),
                axis=0,
                keepdims=True,
            )
            return column(own_line)

        hidden = hidden_of(stacked(slots, 0), True)
        with scope("w_line"):
            whole(line_in, done_recv.at[0]).wait()
        own_share = share(line_out[...])
        shares = [share(line_in[i]) for i in range(3)]
        scales = jnp.concatenate([own_share, shares[0]], axis=0)
        for p in range(pieces):
            first_out[p] = (down(hidden, p) * scales).astype(jnp.bfloat16)

        def hand_pair(p):
            return remote(
                first_out.at[p], own_pair.at[p], sent.at[1], pair_recv, sibling
            )

        for p in range(pieces):
            hand_pair(p).start()

        def far_products():
            with scope("w_far"):
                whole(far_rows, rest_recv.at[1]).wait()
            value = hidden_of(stacked(far_rows, 0), False)
            for p in range(pieces):
                far_out[p] = down(value, p).astype(jnp.bfloat16)
            for p in range(pieces):
                remote(
                    far_out.at[p], far_in.at[p], sent.at[6], sent.at[6], sibling
                ).start()

        pl.when(is_inner)(far_products)

        @pl.when(is_inner)
        def _():
            for q in range(batches):
                with scope(f"w_P{q}"):
                    beside_came(q).wait()

        with scope("w_D"):
            whole(slots.at[3], rest_recv.at[0]).wait()
        hidden = hidden_of(stacked(slots, 2), False)
        scales = jnp.concatenate([shares[1], shares[2]], axis=0)
        for batch_of in batched:
            for p in batch_of:
                second_out[p] = (down(hidden, p) * scales).astype(jnp.bfloat16)
            for p in batch_of:
                along(p, upper, near_recv.at[0, group(p)]).start()
        for p in range(pieces):
            along(p, lower, near_recv.at[2, group(p)]).start()
        pl.when(is_outer)(far_products)
        whole(far_out, sent.at[6]).wait()
        whole(line_in, sent.at[5]).wait()

        @pl.when(is_outer)
        def _():
            blocks_sent(2)

        whole(first_out, sent.at[1]).wait()
        whole(second_out, sent.at[2]).wait()
        swaps_sent()
        with scope("w_give"):
            whole(out_ref, done_recv.at[1]).wait()

    @pl.when(core == 1)
    def _():
        def near_x(q):
            return remote(
                own.at[rows_of(q), :], slots.at[1, rows_of(q), :], sent.at[0],
                spread_recv.at[0, q], on(across, 0),
            )

        def near_z(q):
            return remote(
                own.at[rows_of(q), :], slots.at[2, rows_of(q), :], sent.at[0],
                spread_recv.at[1, q], on(beside, 0),
            )

        def outward(q):
            return remote(
                own.at[rows_of(q), :], slots.at[my_far_slot, rows_of(q), :], sent.at[0],
                spread_recv.at[my_far_slot, q], far[0],
            )

        def arrived(s, q):
            return spread(s, q, slots.at[s], beside, spread_recv.at[s, q])

        def pass_on(s, q):
            return remote(
                slots.at[s, rows_of(q), :], far_rows.at[s, rows_of(q), :], sent.at[0],
                rest_recv.at[1], sibling,
            )

        def sideways(s, q):
            return spread(3 - s, q, slots.at[s], across, rest_recv.at[s])

        def back_x(s, p):
            rows_there = (lower, upper)[s]
            return remote(
                first_out.at[p, rows_there, :], first_in.at[p, rows_there, :], sent.at[1],
                spread_recv.at[s, p], across,
            )

        def back_z(s, p):
            return remote(
                second_out.at[p, (lower, upper)[s], :],
                second_in.at[p, pl.ds(pl.multiple_of(my_far_slot * rows, rows), rows), :],
                sent.at[1],
                done_recv.at[p // 2],
                far[s],
            )

        def came_z(p):
            return whole(second_in.at[pl.ds(p, 2)], done_recv.at[p // 2])

        def cross(p):
            return remote(
                to_cross.at[p], from_across.at[p], sent.at[2], near_recv.at[1, group(p)],
                across,
            )

        own[...] = normed()
        with scope("w_bar"):
            pl.semaphore_wait(barrier, len(far_peers) + 2)
        for q in range(batches):
            outward(q).start()
        for q in range(batches):
            near_x(q).start()
        for q in range(batches):
            near_z(q).start()
        for swap in swaps:
            swap.start()
        whole(line_in.at[pl.ds(0, 2)], small_sem.at[2]).wait()
        shares = [column(line_of(spot)) for spot in far_spots]
        for s, q in [(1, q) for q in range(batches)] + [(0, q) for q in range(batches)]:
            with scope(f"w_F{s}{q}"):
                arrived(s, q).wait_recv()

            @pl.when(is_inner)
            def _():
                arrived(s, q).start()

            sideways(s, q).start()
            pass_on(s, q).start()
        with scope("w_G1"):
            whole(slots.at[2], rest_recv.at[1]).wait()
        hidden = hidden_of(slots[2], True)
        for batch_of in batched:
            for p in batch_of:
                first_out[p, upper, :] = down(hidden, p).astype(jnp.bfloat16)
            for p in batch_of:
                back_x(1, p).start()
        with scope("w_G0"):
            whole(slots.at[3], rest_recv.at[0]).wait()
        late_hidden = hidden_of(slots[3], False)
        for batch_of in batched:
            for p in batch_of:
                first_out[p, lower, :] = down(late_hidden, p).astype(jnp.bfloat16)
            for p in batch_of:
                back_x(0, p).start()
        with scope("w_far"):
            whole(far_in, sent.at[6]).wait()
        span = pieces // groups

        def merge(g):
            with scope(f"w_be{g}"):
                if g == 0:
                    whole(own_pair, pair_recv).wait()
                grouped(from_beside.at[:, upper, :], 0, g).wait()
            for i in range(g * span, g * span + span):
                sums = own_pair[i, upper, :].astype(jnp.float32)
                sums = sums + from_beside[i, upper, :].astype(jnp.float32)
                to_cross[i] = sums.astype(jnp.bfloat16)
                cross(i).start()

        for s in (1, 0):
            there = (lower, upper)[s]
            for p in range(pieces):
                with scope(f"w_bx{s}{p}"):
                    back_x(s, p).wait_recv()
                both = far_in[p, there, :].astype(jnp.float32)
                both = both + first_in[p, there, :].astype(jnp.float32)
                second_out[p, there, :] = both.astype(jnp.bfloat16)
                back_z(s, p).start()

            @pl.when((place == 0) == (s == 1))
            def _():
                for g in range(groups):
                    merge(g)

        for p in range(pieces):
            if p % span == 0:
                with scope(f"w_xA{p}"):
                    grouped(from_across, 1, group(p)).wait()
                with scope(f"w_low{p}"):
                    grouped(from_beside.at[:, lower, :], 2, group(p)).wait()
            total = held[:, part(p)].astype(jnp.float32)
            total = total + own_pair[p, lower, :].astype(jnp.float32)
            total = total + from_beside[p, lower, :].astype(jnp.float32)
            total = total + from_across[p].astype(jnp.float32)
            if p % 2 == 0:
                with scope(f"w_bz{p}"):
                    came_z(p).wait()
            for s in range(2):
                total = total + shares[s] * second_in[p, (lower, upper)[s], :].astype(jnp.float32)
            out_ref[:, part(p)] = total.astype(jnp.bfloat16)
            if (p + 1) % span == 0:
                give(group(p)).start()
        whole(slots, sent.at[1]).wait()
        whole(to_cross, sent.at[2]).wait()

        @pl.when(is_inner)
        def _():
            blocks_sent(9)

        @pl.when(is_outer)
        def _():
            blocks_sent(7)

        swaps_sent()
        with scope("w_end"):
            whole(out_ref, sent.at[5]).wait()


def dense_layer(tokens, gain, route_ids, route_weights, w_gate, w_up, w_down):
    rows, features = tokens.shape
    units = 2 * w_gate.shape[2]
    batches = rows // 16
    pieces = 6
    width = features // pieces
    hbm = pl.BlockSpec(memory_space=pltpu.HBM)
    half = jnp.bfloat16
    dma = pltpu.SemaphoreType.DMA
    ids = route_ids.T
    weights = route_weights.T
    operands = (tokens, gain, ids, weights, w_gate, w_up, w_down)
    travel = pltpu.VMEM((pieces, 2 * rows, width), half)
    single = pltpu.VMEM((pieces, rows, width), half)
    return pl.pallas_call(
        dense_kernel,
        out_shape=pltpu.VMEM(tokens.shape, tokens.dtype),
        in_specs=[hbm] * 7,
        out_specs=pl.BlockSpec(memory_space=pltpu.VMEM),
        scratch_shapes=[
            pltpu.VMEM((rows, features), half),
            pltpu.VMEM((features,), jnp.float32),
            pltpu.VMEM(ids.shape, jnp.int32),
            pltpu.VMEM(weights.shape, jnp.float32),
            pltpu.VMEM((features, units), half),
            pltpu.VMEM((features, units), half),
            pltpu.VMEM((units, features), half),
            pltpu.VMEM((rows, features), half),
            pltpu.VMEM((4, rows, features), half),
            pltpu.VMEM((2, rows, features), half),
        ]
        + [travel] * 8
        + [single] * 2
        + [
            pltpu.VMEM(weights.shape, jnp.float32),
            pltpu.VMEM((3, *weights.shape), jnp.float32),
            dma((3,)),
            dma((3,)),
            dma((7,)),
            dma((2, max(batches, pieces))),
            dma((2,)),
            dma((pieces // 2,)),
            dma((3, 2)),
            dma,
        ],
        compiler_params=pltpu.CompilerParams(
            collective_id=0, has_side_effects=True, vmem_limit_bytes=40_000_000
        ),
    )(*(pltpu.with_memory_space_constraint(array, pltpu.HBM) for array in operands))


def route_tables(chosen_ids, chosen_weights, expert_count, slot_room):
    row_count, top_count = chosen_ids.shape
    matches = (chosen_ids[:, :, None] == jnp.arange(expert_count, dtype=jnp.int32)).astype(
        jnp.float32
    )
    flat_match = matches.reshape(row_count * top_count, expert_count)
    order_range = jnp.arange(row_count * top_count, dtype=jnp.int32)
    earlier = (order_range[:, None] > order_range[None, :]).astype(jnp.float32)
    before = jnp.dot(
        earlier, flat_match, precision=lax.Precision.HIGHEST, preferred_element_type=jnp.float32
    )
    position = jnp.sum(before * flat_match, axis=1).reshape(row_count, top_count).astype(jnp.int32)
    slot_index = chosen_ids * slot_room + position
    targets = jnp.arange(expert_count * slot_room, dtype=jnp.int32)
    slot_hits = slot_index[None, :, :] == targets[:, None, None]
    send_table = jnp.sum(slot_hits.astype(jnp.float32), axis=2).astype(jnp.bfloat16)
    mix_table = jnp.sum(jnp.where(slot_hits, chosen_weights[None, :, :], 0.0), axis=2)
    return (send_table, mix_table)


def routed_layer(tokens, gain, route_ids, route_weights, w_gate, w_up, w_down):
    expert_axis = lax.axis_size("expert")
    expert_count = expert_axis // 2
    tensor_count = lax.axis_size("tensor")
    own_rows = tokens.shape[0] // tensor_count
    top_count = route_ids.shape[1]
    capacity = max(2, own_rows * top_count // expert_count)
    gate_local = w_gate[0]
    up_local = w_up[0]
    down_local = w_down[0]
    first_row = lax.axis_index("tensor") * own_rows
    own_tokens = lax.dynamic_slice_in_dim(tokens, first_row, own_rows, 0)
    own_ids = lax.dynamic_slice_in_dim(route_ids, first_row, own_rows, 0)
    own_weights = lax.dynamic_slice_in_dim(route_weights, first_row, own_rows, 0)
    resident = own_tokens.astype(jnp.float32)
    inv_rms = lax.rsqrt(jnp.mean(resident * resident, axis=1, keepdims=True) + 1e-05)
    normed = (resident * inv_rms * gain).astype(jnp.bfloat16)
    send_table, mix_table = route_tables(own_ids, own_weights, expert_count, capacity)
    packed = jnp.dot(send_table, normed, preferred_element_type=jnp.float32).astype(jnp.bfloat16)
    features = packed.shape[1]
    by_expert = packed.reshape(expert_count, 1, capacity, features)
    outgoing = jnp.broadcast_to(by_expert, (expert_count, 2, capacity, features)).reshape(
        expert_axis * capacity, features
    )
    arrived = lax.all_to_all(outgoing, "expert", split_axis=0, concat_axis=0, tiled=True)
    row_piece = lax.all_gather(arrived, "tensor", axis=0, tiled=True)
    gate_val = jnp.dot(row_piece, gate_local, preferred_element_type=jnp.float32)
    up_val = jnp.dot(row_piece, up_local, preferred_element_type=jnp.float32)
    hidden = gated_unit(gate_val, up_val).astype(jnp.bfloat16)
    partial_value = lax.psum_scatter(
        jnp.dot(hidden, down_local, preferred_element_type=jnp.float32),
        "tensor",
        scatter_dimension=0,
        tiled=True,
    )
    returned = lax.all_to_all(
        partial_value.astype(jnp.bfloat16), "expert", split_axis=0, concat_axis=0, tiled=True
    ).astype(partial_value.dtype)
    expert_out = (
        returned.reshape(expert_count, 2, capacity, features)
        .sum(axis=1)
        .reshape(expert_count * capacity, features)
    )
    weighted = jnp.dot(
        mix_table.T, expert_out, precision=lax.Precision.HIGHEST, preferred_element_type=jnp.float32
    )
    finished = (resident + weighted).astype(jnp.bfloat16)
    return lax.all_gather(finished, "tensor", axis=0, tiled=True)


def per_device(tokens, gain, route_ids, route_weights, w_gate, w_up, w_down):
    experts = lax.axis_size("expert") // 2
    dense = (
        route_ids.shape[1] == experts
        and experts == 4
        and lax.axis_size("tensor") == 2
        and w_gate.shape[0] == 1
    )
    layer = dense_layer if dense else routed_layer
    return layer(tokens, gain, route_ids, route_weights, w_gate, w_up, w_down)


def solution(mesh):
    placed = (
        P(("groups", "expert"), None),
        P(),
        P(("groups", "expert"), None),
        P(("groups", "expert"), None),
        P("expert", None, "tensor"),
        P("expert", None, "tensor"),
        P("expert", "tensor", None),
    )
    return jax.shard_map(
        per_device,
        mesh=mesh,
        in_specs=placed,
        out_specs=P(("groups", "expert"), None),
        check_vma=False,
    )
```
